32 devices in a mesh: seq: 8 (over y, x, core), tp: 4 (over z).
Axes of the slice: x: 2, y: 2, z: 4, core: 2. Of those that a mesh axis runs over, the one named last changes fastest.
Arguments:
- x_old: bfloat16 [4096, 4608], P('seq', 'tp'), may hold values from -6 to 6
- old_blocks: int32 [8], replicated, may hold values from 1 to 4, 16 in all
- new_blocks: int32 [8], replicated, may hold values from 1 to 4, 16 in all
- order: int32 [8], replicated, may hold values from 0 to 7, as said below
- pre_gain: float32 [4608], replicated, may hold values from 0.25 to 1.75
- post_gain: float32 [4608], replicated, may hold values from 0.25 to 1.75
- w_query: bfloat16 [4608, 4096], P('seq', 'tp'), may hold values from -0.59765625 to 0.59765625
- w_key: bfloat16 [4608, 2048], P('seq', 'tp'), may hold values from -0.09375 to 0.09375
- w_value: bfloat16 [4608, 2048], P('seq', 'tp'), may hold values from -0.09375 to 0.09375
- w_out_t: bfloat16 [4608, 4096], P('seq', 'tp'), may hold values from -0.09375 to 0.09375
Outputs:
- layer_out: bfloat16 [4096, 4608], P(('seq', 'tp'))
The draws below stay inside these ranges and needn't reach their ends.
Inputs may be any that keep to these rules, and one draw needn't show every extreme that they name: `old_blocks`: counts of 128-row blocks, at least one each; they sum to 16, and the largest is exactly 4. `new_blocks`: counts of 128-row blocks, at least one each; they sum to 16, and the largest is exactly 4. A permutation of the seq indices with order[7] = 0 and order[3] = 7; the other indices, taken in increasing order, hold 1 to 6 in increasing order, except that aligned pairs of them (first and second, third and fourth, and so on) are swapped or not, pair by pair.
All inputs are finite; a program needn't handle non-finite values.
Results may differ from the reference program's by a relative error of at most 0.013.
Values may be sent and summed in bfloat16 or wider, within the bound.
A program may use at most 128 MiB of HBM per device.

```python
import math
import jax
import jax.numpy as jnp
import numpy as np
from jax import lax

D = 4608
HEADS = 32
KV_HEADS = 16
HEAD = 128
BLOCK = 128
CAP = 512
TOKENS = 2048
SLOTS = 4096
N_SEQ = 8
N_TP = 4


def draw_order(key, part):
    middle = N_SEQ - 2
    kept = [place for place in range(N_SEQ) if place != N_SEQ - 1 and place != N_SEQ // 2 - 1]
    flips = jax.random.randint(jax.random.fold_in(key, 7), (middle // 2,), 0, 2).astype(jnp.int32)
    ranks = jnp.arange(middle, dtype=jnp.int32)
    shards = (jnp.bitwise_xor(ranks, jnp.repeat(flips, 2)) + 1).astype(jnp.int32)
    result = jnp.zeros((N_SEQ,), jnp.int32)
    result = result.at[jnp.array(kept, dtype=jnp.int32)].set(shards)
    result = result.at[N_SEQ - 1].set(0)
    result = result.at[N_SEQ // 2 - 1].set(N_SEQ - 1)
    return result.astype(jnp.int32)


def block_levels(rng, shape, cuts, least, largest):
    factor_of = 1.0
    for axis_at, shards_of in cuts:
        steps = jax.random.uniform(jax.random.fold_in(jax.random.fold_in(rng, 6), axis_at), (shards_of,), jnp.float32, least / len(cuts), largest / len(cuts))
        factor_of = factor_of * jnp.repeat(jnp.exp(steps), shape[axis_at] // shards_of).reshape((-1,) + (1,) * (len(shape) - 1 - axis_at))
    return factor_of


def split_up(number_of, total, reach, slope):
    portions = [(1 << 20) // math.isqrt(standing ** slope) + 1 for standing in range(2, number_of + 1)]
    rest, holding = total - reach - (number_of - 1), [1] * (number_of - 1)
    while rest > 0:
        movable = [i for i in range(number_of - 1) if holding[i] < reach]
        pool, left = sum([portions[i] for i in movable]), rest
        for i in movable:
            addition = min(reach - holding[i], max(1, left * portions[i] // pool), rest)
            holding[i] = holding[i] + addition
            rest = rest - addition
    return np.array([reach] + holding)


def uneven_parts(rng, number_of, total, reach, skew):
    if number_of == 2:
        one = jax.random.randint(rng, (), max(1, total - reach), min(reach, total - 1) + 1)
        return jnp.stack([one, total - one])
    lengths = jnp.asarray(split_up(number_of, total, reach, skew), jnp.int32)
    twos = (number_of - 1) // 2
    donor, receiver = lengths[1:1 + 2 * twos:2], lengths[2:2 + 2 * twos:2]
    room = jnp.minimum(donor - 1, reach - receiver)
    shifted = jax.random.randint(jax.random.fold_in(rng, 1), (twos,), 0, 1 << 20) % (room + 1)
    lengths = lengths.at[1:1 + 2 * twos:2].set(donor - shifted).at[2:2 + 2 * twos:2].set(receiver + shifted)
    return lengths[jax.random.permutation(jax.random.fold_in(rng, 2), number_of)]


def noise(key, shape, scale, bound, pieces=(), kind=jnp.bfloat16):
    values = jax.random.normal(key, shape, jnp.float32) * scale
    if len(pieces) > 0:
        values = block_levels(key, shape, pieces, -0.22, 0.18) * values
    return jnp.clip(values, min=-bound, max=bound).astype(kind)


def setup_inputs(seed: int = 0) -> dict:
    key_list = jax.random.split(jax.random.key(seed), 11)
    return {
        "x_old": noise(key_list[0], (SLOTS, D), 1.0, 6.0, ((0, 8), (1, 4))),
        "old_blocks": uneven_parts(key_list[1], N_SEQ, TOKENS // BLOCK, CAP // BLOCK, 1).astype(jnp.int32),
        "new_blocks": uneven_parts(key_list[2], N_SEQ, TOKENS // BLOCK, CAP // BLOCK, 2).astype(jnp.int32),
        "order": draw_order(jax.random.fold_in(key_list[10], 71), 0),
        "pre_gain": jnp.clip(1.0 + 0.15 * jax.random.normal(key_list[4], (D,), jnp.float32), 0.25, 1.75),
        "post_gain": jnp.clip(1.0 + 0.15 * jax.random.normal(key_list[5], (D,), jnp.float32), 0.25, 1.75),
        "w_query": noise(key_list[6], (D, HEADS * HEAD), 0.1, 0.59765625, ((0, 8), (1, 4))),
        "w_key": noise(key_list[7], (D, KV_HEADS * HEAD), D ** -0.5, 0.09375, ((0, 8), (1, 4))),
        "w_value": noise(key_list[8], (D, KV_HEADS * HEAD), D ** -0.5, 0.09375, ((0, 8), (1, 4))),
        "w_out_t": noise(key_list[9], (D, HEADS * HEAD), (HEADS * HEAD) ** -0.5, 0.09375, ((0, 8), (1, 4))),
    }


EPS = 1e-06

def offsets(blocks):
    return ((jnp.cumsum(blocks) - blocks) * BLOCK).astype(jnp.int32)

def rotate(values, places):
    half = values.shape[-1] // 2
    inverse = jnp.exp(jnp.arange(half, dtype=jnp.float32) * (-2.0 * math.log(10000.0) / values.shape[-1]))
    angles = places.astype(jnp.float32)[:, None] * inverse[None, :]
    cosine = jnp.cos(angles)[:, None, :]
    sine = jnp.sin(angles)[:, None, :]
    first = values[..., :half]
    second = values[..., half:]
    return jnp.concatenate([first * cosine - second * sine, second * cosine + first * sine], axis=-1)

def rms_scale(values, gain):
    return values * lax.rsqrt(lax.optimization_barrier(jnp.mean(values * values, axis=-1, keepdims=True)) + EPS) * gain

def reference(x_old, old_blocks, new_blocks, order, pre_gain, post_gain, w_query, w_key, w_value, w_out_t):
    old_start = offsets(old_blocks)
    new_start = offsets(new_blocks)
    seq_rows = jnp.arange(TOKENS, dtype=jnp.int32)
    shard = (lax.optimization_barrier(jnp.sum((old_start[None, :] <= seq_rows[:, None]).astype(jnp.int32), axis=1)) - 1).astype(jnp.int32)
    devices = jnp.arange(N_SEQ, dtype=jnp.int32)
    holder = lax.optimization_barrier(jnp.sum(devices[None, :] * (order[None, :] == shard[:, None]).astype(jnp.int32), axis=1)).astype(jnp.int32)
    source = (holder * CAP + seq_rows - old_start[shard]).astype(jnp.int32)
    resident = x_old[source]
    resident_f = resident.astype(jnp.float32)
    normed = rms_scale(resident_f, pre_gain).astype(jnp.bfloat16)
    query = jnp.dot(normed, w_query, preferred_element_type=jnp.float32).reshape(TOKENS, HEADS, HEAD)
    query = (rotate(query, seq_rows) * (D // HEADS) ** (-0.5)).astype(jnp.bfloat16)
    key = jnp.dot(normed, w_key, preferred_element_type=jnp.float32).reshape(TOKENS, KV_HEADS, HEAD)
    key = rotate(key, seq_rows).astype(jnp.bfloat16)
    value = jnp.dot(normed, w_value, preferred_element_type=jnp.float32).reshape(TOKENS, KV_HEADS, HEAD).astype(jnp.bfloat16)
    group = HEADS // KV_HEADS
    query_heads = jnp.transpose(query, (1, 0, 2)).astype(jnp.float32)
    key_heads = jnp.repeat(jnp.transpose(key, (1, 0, 2)), group, axis=0).astype(jnp.float32)
    value_heads = jnp.repeat(jnp.transpose(value, (1, 0, 2)), group, axis=0).astype(jnp.float32)
    causal = seq_rows[None, :] <= seq_rows[:, None]

    def one_head(operands):
        query_one, key_one, value_one = operands
        score = jnp.dot(query_one, key_one.T)
        capped = 50.0 * jnp.tanh(score / 50.0)
        weight = jnp.where(causal, jnp.exp(capped), 0.0)
        total = lax.optimization_barrier(jnp.sum(weight, axis=1))
        weight_b = weight.astype(jnp.bfloat16).astype(jnp.float32)
        numer = jnp.dot(weight_b, value_one)
        return (numer / total[:, None]).astype(jnp.bfloat16)
    context = lax.map(one_head, (query_heads, key_heads, value_heads))
    context = jnp.transpose(context, (1, 0, 2)).reshape(TOKENS, HEADS * HEAD)
    span = HEADS * HEAD // N_TP
    projected = jnp.zeros((TOKENS, D), jnp.float32)
    for group_index in range(N_TP):
        columns = context[:, group_index * span:(group_index + 1) * span]
        weights_part = w_out_t[:, group_index * span:(group_index + 1) * span]
        partial_sum = lax.dot_general(columns, weights_part, (((1,), (1,)), ((), ())), preferred_element_type=jnp.float32)
        projected = projected + lax.optimization_barrier(partial_sum.astype(jnp.bfloat16)).astype(jnp.float32)
    refreshed = (resident_f + rms_scale(projected, post_gain)).astype(jnp.bfloat16)
    slots = jnp.arange(N_SEQ * CAP, dtype=jnp.int32)
    owner = (slots // CAP).astype(jnp.int32)
    within = (slots - owner * CAP).astype(jnp.int32)
    valid = within < new_blocks[owner] * BLOCK
    target = jnp.clip(new_start[owner] + within, 0, TOKENS - 1).astype(jnp.int32)
    return jnp.where(valid[:, None], refreshed[target], jnp.zeros((), jnp.bfloat16)).astype(jnp.bfloat16)
```

```python
import functools
import math

import jax
import jax.numpy as jnp
from jax import lax
from jax.experimental import pallas as pl
from jax.experimental.pallas import tpu as pltpu
from jax.sharding import PartitionSpec as P

HEAD = 128
BLOCK = 128
EPS = 1e-06


def offsets(blocks):
    return (jnp.cumsum(blocks) - blocks) * BLOCK


def rms_scale(values, gain):
    return values * lax.rsqrt(jnp.mean(values * values, axis=-1, keepdims=True) + EPS) * gain


def attention_kernel(rows, span, q_ref, k_ref, v_ref, out_ref):
    first = pl.program_id(0) * rows
    query = q_ref[...]

    def step(at, carry, masked):
        numer, denom = carry
        start = pl.multiple_of(at * span, span)
        score = lax.dot_general(
            query,
            k_ref[pl.ds(start, span), :],
            (((1,), (1,)), ((), ())),
            preferred_element_type=jnp.float32,
        )
        weight = jnp.exp(50.0 * jnp.tanh(score * (1.0 / 50.0)))
        if masked:
            places = first + lax.broadcasted_iota(jnp.int32, weight.shape, 0)
            keys = start + lax.broadcasted_iota(jnp.int32, weight.shape, 1)
            weight = jnp.where(keys <= places, weight, 0.0)
        denom = denom + jnp.sum(weight, axis=1, keepdims=True)
        numer = numer + jnp.dot(
            weight.astype(jnp.bfloat16),
            v_ref[pl.ds(start, span), :],
            preferred_element_type=jnp.float32,
        )
        return numer, denom

    whole = first // span
    state = (jnp.zeros((rows, HEAD), jnp.float32), jnp.zeros((rows, 1), jnp.float32))
    state = lax.fori_loop(0, whole, lambda at, c: step(at, c, False), state)
    numer, denom = step(whole, state, True)
    out_ref[...] = (numer / denom).astype(out_ref.dtype)


def attention(query, key, value):
    tokens = query.shape[0]
    rows, span = 256, 512
    return pl.pallas_call(
        functools.partial(attention_kernel, rows, span),
        grid=(tokens // rows,),
        in_specs=[
            pl.BlockSpec((rows, HEAD), lambda i: (i, 0)),
            pl.BlockSpec((tokens, HEAD), lambda i: (0, 0)),
            pl.BlockSpec((tokens, HEAD), lambda i: (0, 0)),
        ],
        out_specs=pl.BlockSpec((rows, HEAD), lambda i: (i, 0)),
        out_shape=jax.ShapeDtypeStruct((tokens, HEAD), jnp.bfloat16),
        cost_estimate=pl.CostEstimate(
            flops=3 * tokens * tokens * HEAD,
            bytes_accessed=8 * tokens * HEAD,
            transcendentals=tokens * tokens,
        ),
    )(query, key, value)


MESH = pl.DeviceIdType.MESH


def arrangements(seq_count):
    found = []
    for second in range(1, seq_count + 1):
        for third in range(1, second + 1):
            fourth = seq_count - second - third
            if 1 <= fourth <= third:
                found.append((seq_count, second, third, fourth))
    return found


def layer_windows(seq_count, tp_count, per_block):
    first, last = [], []
    for layer in range(tp_count):
        starts, ends = [], []
        for counts in arrangements(seq_count):
            begin = sum(counts[u // per_block] for u in range(layer))
            starts.append(begin)
            ends.append(begin + counts[layer // per_block])
        first.append(min(starts))
        last.append(max(ends))
    return first, last


def pick(index, values):
    result = jnp.int32(values[0])
    for k in range(1, len(values)):
        result = jnp.where(index == k, jnp.int32(values[k]), result)
    return result


def flipped(index, mask):
    result = index
    bit = 1
    while bit <= mask:
        if mask & bit:
            result = result + bit - 2 * bit * lax.rem(index // bit, 2)
        bit *= 2
    return result


def output_kernel(
    heads,
    copies,
    seq_count,
    tp_count,
    share,
    first,
    last,
    perm_ref,
    place_ref,
    context_ref,
    weight_ref,
    residual_ref,
    gain_ref,
    out_ref,
    full,
    partial,
    left_in,
    right_in,
    left_out,
    right_out,
    total,
    sent,
    came,
    gather_send,
    gather_recv,
    left_send,
    left_recv,
    right_send,
    right_recv,
    swap_send,
    swap_recv,
):
    seq_index = lax.axis_index("seq")
    tp_index = lax.axis_index("tp")
    places = partial.shape[0]
    depth = weight_ref.shape[0]
    head = seq_index // copies
    chunks = full.shape[0]
    per_chunk = places // chunks
    chunk_rows = full.shape[1]

    barrier = pltpu.get_barrier_semaphore()
    for k in range(1, seq_count):
        pl.semaphore_signal(
            barrier,
            inc=1,
            device_id=(lax.rem(seq_index + k, seq_count), tp_index),
            device_id_type=MESH,
        )

    @pl.when(tp_index > 0)
    def _():
        pl.semaphore_signal(
            barrier, inc=1, device_id=(seq_index, tp_index - 1), device_id_type=MESH
        )

    @pl.when(tp_index < tp_count - 1)
    def _():
        pl.semaphore_signal(
            barrier, inc=1, device_id=(seq_index, tp_index + 1), device_id_type=MESH
        )

    own_columns = pl.ds(pl.multiple_of(head * HEAD, HEAD), HEAD)
    for chunk in range(chunks):
        for at in range(per_chunk):
            full[chunk, at * share : (at + 1) * share, own_columns] = context_ref[
                perm_ref[chunk * per_chunk + at]
            ]

    neighbours = jnp.where(tp_index > 0, 1, 0) + jnp.where(tp_index < tp_count - 1, 1, 0)
    pl.semaphore_wait(barrier, seq_count - 1 + neighbours)

    bits = heads.bit_length() - 1
    order = [0, chunks - 1] + list(range(1, chunks - 1))

    def dims(chunk):
        outer = list(range(1, bits))
        if chunk >= chunks // 2:
            outer = outer[::-1]
        return outer + [0] if bits > 0 else []

    def gather_copy(chunk, bit, combo, to_me):
        slot = flipped(head, (combo ^ (1 << bit)) if to_me else combo)
        columns = pl.ds(pl.multiple_of(slot * HEAD, HEAD), HEAD)
        partner = flipped(seq_index, copies << bit)
        view = full.at[chunk, :, columns]
        return pltpu.make_async_remote_copy(
            src_ref=view,
            dst_ref=view,
            send_sem=gather_send.at[chunk, bit, combo],
            recv_sem=gather_recv.at[chunk, bit, combo],
            device_id=(partner, tp_index),
            device_id_type=MESH,
        )

    def steps(chunk):
        held = [0]
        for bit in dims(chunk):
            yield bit, list(held)
            held = held + [c ^ (1 << bit) for c in held]

    for chunk in order:
        for bit, held in steps(chunk):
            gather_copy(chunk, bit, 0, False).start()
    for level in range(bits):
        for chunk in order:
            stages = list(steps(chunk))
            bit, held = stages[level]
            for combo in held:
                gather_copy(chunk, bit, combo, True).wait_recv()
                for later, _ in stages[level + 1 :]:
                    gather_copy(chunk, later, combo ^ (1 << bit), False).start()

    for chunk in range(chunks):
        for bit, held in steps(chunk):
            for combo in held:
                gather_copy(chunk, bit, combo, False).wait_send()
    for chunk in range(chunks):
        product = lax.dot_general(
            full[chunk],
            weight_ref[...],
            (((1,), (1,)), ((), ())),
            preferred_element_type=jnp.float32,
        ).astype(jnp.bfloat16)
        for at in range(per_chunk):
            partial[chunk * per_chunk + at] = product[at * share : (at + 1) * share]

    left_has = jnp.where(tp_index < tp_count - 1, pick(tp_index, last), 0)
    left_gives = pick(tp_index, [0] + last[:-1])
    right_has = jnp.where(tp_index > 0, pick(tp_index, first), places)
    right_gives = pick(tp_index, first[1:] + [places])

    def line_copy(place, source, landing, send, recv, step):
        return pltpu.make_async_remote_copy(
            src_ref=source.at[place],
            dst_ref=landing.at[place],
            send_sem=send.at[place],
            recv_sem=recv.at[place],
            device_id=(seq_index, tp_index + step),
            device_id_type=MESH,
        )

    def flow(place, has, gives, source, landing, send, recv, step):
        copy = line_copy(place, source, landing, send, recv, step)

        @pl.when(has)
        def _():
            copy.wait_recv()

        @pl.when(jnp.logical_and(has, gives))
        def _():
            source[place] = (
                partial[place].astype(jnp.float32) + landing[place].astype(jnp.float32)
            ).astype(jnp.bfloat16)

        @pl.when(jnp.logical_and(jnp.logical_not(has), gives))
        def _():
            source[place] = partial[place]

        @pl.when(gives)
        def _():
            copy.start()

    def line_step(at, carry):
        flow(at, at < left_has, at < left_gives, left_out, left_in, left_send, left_recv, -1)
        back = places - 1 - at
        flow(
            back,
            back >= right_has,
            back >= right_gives,
            right_out,
            right_in,
            right_send,
            right_recv,
            1,
        )
        return carry

    lax.fori_loop(0, places, line_step, 0)

    def sum_step(place, carry):
        total[place] = partial[place].astype(jnp.float32)

        @pl.when(place < left_has)
        def _():
            total[place] = total[place] + left_in[place].astype(jnp.float32)

        @pl.when(place >= right_has)
        def _():
            total[place] = total[place] + right_in[place].astype(jnp.float32)

        return carry

    lax.fori_loop(0, places, sum_step, 0)

    def swap_copy(k, to_me):
        other = lax.rem(seq_index + k, seq_count)
        mine = lax.rem(seq_index + seq_count - k, seq_count) if to_me else seq_index
        return pltpu.make_async_remote_copy(
            src_ref=sent.at[other],
            dst_ref=came.at[mine],
            send_sem=swap_send.at[k],
            recv_sem=swap_recv.at[k],
            device_id=(other, tp_index),
            device_id_type=MESH,
        )

    for j in range(seq_count):
        sent[j] = total[place_ref[j]].astype(jnp.bfloat16)
    for k in range(1, seq_count):
        swap_copy(k, False).start()
    came[seq_index] = sent[seq_index]
    for k in range(1, seq_count):
        swap_copy(k, True).wait_recv()

    square = jnp.zeros((share, 1), jnp.float32)
    for s in range(seq_count):
        piece = came[s].astype(jnp.float32)
        square = square + jnp.sum(piece * piece, axis=1, keepdims=True)
    factor = lax.rsqrt(square * (1.0 / (depth * seq_count)) + EPS)
    for s in range(seq_count // 2):
        piece = jnp.concatenate([came[2 * s], came[2 * s + 1]], axis=1).astype(jnp.float32)
        columns = slice(2 * s * depth, (2 * s + 2) * depth)
        value = residual_ref[:, columns].astype(jnp.float32) + (
            piece * factor * gain_ref[:, columns]
        )
        out_ref[:, columns] = value.astype(jnp.bfloat16)

    for k in range(1, seq_count):
        swap_copy(k, False).wait_send()

    def drain(place, carry):
        @pl.when(place < left_gives)
        def _():
            line_copy(place, left_out, left_in, left_send, left_recv, -1).wait_send()

        @pl.when(place >= right_gives)
        def _():
            line_copy(place, right_out, right_in, right_send, right_recv, 1).wait_send()

        return carry

    lax.fori_loop(0, places, drain, 0)


def output_phase(context, w_out_t, residual, post_gain, new_blocks, seq_count, tp_count, heads):
    tokens = context.shape[0]
    depth = w_out_t.shape[0]
    share, width = residual.shape
    places = tokens // share
    per_block = BLOCK // share
    copies = seq_count // heads
    bits = heads.bit_length() - 1
    first, last = layer_windows(seq_count, tp_count, per_block)
    seq_index = lax.axis_index("seq")
    tp_index = lax.axis_index("tp")
    blocks = new_blocks * per_block
    new_start = jnp.sum(
        jnp.where(
            jnp.arange(seq_count)[None, :] < jnp.arange(seq_count)[:, None], blocks[None, :], 0
        ),
        axis=1,
    )
    slots = jnp.arange(tp_count * seq_count, dtype=jnp.int32)
    layer = jnp.arange(tp_count, dtype=jnp.int32)[:, None]
    valid = (blocks[None, :] > layer).astype(jnp.int32).reshape(-1)
    source = (new_start[None, :] + layer).reshape(-1)
    rank = jnp.sum(jnp.where(slots[None, :] < slots[:, None], valid[None, :], 0), axis=1)
    perm = jnp.sum(
        jnp.where(
            (jnp.arange(places)[:, None] == rank[None, :]) & (valid[None, :] > 0),
            source[None, :],
            0,
        ),
        axis=1,
    ).astype(jnp.int32)
    in_layer = (jnp.arange(tp_count) == tp_index)[:, None]
    place = jnp.sum(jnp.where(in_layer, rank.reshape(tp_count, seq_count), 0), axis=0)
    place = jnp.minimum(place, places - 1).astype(jnp.int32)
    mine = jnp.sum(jnp.where(jnp.arange(seq_count) == seq_index, blocks, 0))
    chunks = 4
    rows = tokens // chunks
    scratch_block = pltpu.VMEM((places, share, depth), jnp.bfloat16)
    swap_block = pltpu.VMEM((seq_count, share, depth), jnp.bfloat16)
    line_sem = pltpu.SemaphoreType.DMA((places,))
    gather_sem = pltpu.SemaphoreType.DMA((chunks, bits, heads))
    swap_sem = pltpu.SemaphoreType.DMA((seq_count,))
    result = pl.pallas_call(
        functools.partial(
            output_kernel, heads, copies, seq_count, tp_count, share, first, last
        ),
        out_shape=jax.ShapeDtypeStruct((share, width), jnp.bfloat16),
        in_specs=[pl.BlockSpec(memory_space=pltpu.SMEM)] * 2
        + [pl.BlockSpec(memory_space=pltpu.VMEM)] * 4,
        out_specs=pl.BlockSpec(memory_space=pltpu.VMEM),
        scratch_shapes=[
            pltpu.VMEM((chunks, rows, heads * HEAD), jnp.bfloat16),
            scratch_block,
            scratch_block,
            scratch_block,
            scratch_block,
            scratch_block,
            pltpu.VMEM((places, share, depth), jnp.float32),
            swap_block,
            swap_block,
            gather_sem,
            gather_sem,
            line_sem,
            line_sem,
            line_sem,
            line_sem,
            swap_sem,
            swap_sem,
        ],
        compiler_params=pltpu.CompilerParams(
            collective_id=0, has_side_effects=True, vmem_limit_bytes=56 * 2**20
        ),
        cost_estimate=pl.CostEstimate(
            flops=60_000_000_000, bytes_accessed=4 * tokens * depth, transcendentals=0
        ),
    )(perm, place, context.reshape(places, share, HEAD), w_out_t, residual, post_gain.reshape(1, -1))
    return jnp.where(tp_index < mine, result, jnp.zeros_like(result))


def per_device(
    x_old, old_blocks, new_blocks, order, pre_gain, post_gain, w_query, w_key, w_value, w_out_t
):
    seq_count = lax.axis_size("seq")
    tp_count = lax.axis_size("tp")
    capacity, quarter = x_old.shape
    width = quarter * tp_count
    tokens = seq_count * capacity // 2
    own = tokens // seq_count
    share = capacity // tp_count
    seq_index = lax.axis_index("seq")
    tp_index = lax.axis_index("tp")
    old_start = offsets(old_blocks)
    new_start = offsets(new_blocks)
    device_ids = jnp.arange(seq_count, dtype=jnp.int32)

    gathered = lax.all_gather(x_old, "seq", axis=0, tiled=True)

    def stored(row, count):
        row = jnp.minimum(row, tokens - count)
        shard = jnp.sum((old_start <= row).astype(jnp.int32)) - 1
        holder = jnp.sum(jnp.where(order == shard, device_ids, 0))
        begin = jnp.sum(jnp.where(device_ids == shard, old_start, 0))
        return lax.dynamic_slice_in_dim(gathered, holder * capacity + row - begin, count, 0)

    def shift(k):
        return [(i, (i + k) % tp_count) for i in range(tp_count)]

    def by_source(received):
        stack = jnp.stack(received)
        pieces = [
            lax.dynamic_index_in_dim(stack, lax.rem(tp_index - u + tp_count, tp_count), 0, False)
            for u in range(tp_count)
        ]
        return jnp.concatenate(pieces, axis=1)

    mine = jnp.concatenate(
        [stored(seq_index * own + at, BLOCK) for at in range(0, own, BLOCK)], axis=0
    )
    full_rows = by_source(
        [mine] + [lax.ppermute(mine, "tp", shift(k)) for k in range(1, tp_count)]
    )
    my_start = jnp.sum(jnp.where(device_ids == seq_index, new_start, 0))

    def slot_rows(place):
        return stored(my_start + place * share, share)

    residual = by_source(
        [slot_rows(tp_index)]
        + [
            lax.ppermute(slot_rows(lax.rem(tp_index + k, tp_count)), "tp", shift(k))
            for k in range(1, tp_count)
        ]
    )

    weights = lax.all_gather(
        jnp.concatenate([w_query, w_key, w_value], axis=1), "seq", axis=0, tiled=True
    )

    normed = rms_scale(full_rows.astype(jnp.float32), pre_gain).astype(jnp.bfloat16)
    normed, residual = lax.optimization_barrier((normed, residual))
    heads = w_query.shape[1] // HEAD
    kv_heads = w_key.shape[1] // HEAD
    group = heads // kv_heads
    copies = seq_count // heads
    raw = jnp.dot(normed, weights, preferred_element_type=jnp.float32)

    half = HEAD // 2
    inverse = jnp.exp(jnp.arange(half, dtype=jnp.float32) * (-2.0 * math.log(10000.0) / HEAD))
    places = seq_index * own + jnp.arange(own, dtype=jnp.int32)
    angles = places.astype(jnp.float32)[:, None] * inverse[None, :]
    cosine, sine = jnp.cos(angles), jnp.sin(angles)

    def rotate(at):
        first = raw[:, at * HEAD : at * HEAD + half]
        second = raw[:, at * HEAD + half : (at + 1) * HEAD]
        return jnp.concatenate(
            [first * cosine - second * sine, second * cosine + first * sine], axis=-1
        )

    scale = (width // (heads * tp_count)) ** (-0.5)
    queries = [(rotate(h) * scale).astype(jnp.bfloat16) for h in range(heads)]
    keys = [rotate(heads + g).astype(jnp.bfloat16) for g in range(kv_heads)]
    values = [
        raw[:, (heads + kv_heads + g) * HEAD : (heads + kv_heads + g + 1) * HEAD].astype(
            jnp.bfloat16
        )
        for g in range(kv_heads)
    ]
    sent = jnp.stack(
        [
            jnp.stack([queries[s // copies], keys[s // copies // group], values[s // copies // group]])
            for s in range(seq_count)
        ]
    )
    came = lax.all_to_all(sent, "seq", 0, 0, tiled=True)
    context = attention(
        came[:, 0].reshape(tokens, HEAD),
        came[:, 1].reshape(tokens, HEAD),
        came[:, 2].reshape(tokens, HEAD),
    )
    return output_phase(
        context, w_out_t, residual, post_gain, new_blocks, seq_count, tp_count, heads
    )


def solution(mesh):
    placed = (
        P("seq", "tp"),
        P(),
        P(),
        P(),
        P(),
        P(),
        P("seq", "tp"),
        P("seq", "tp"),
        P("seq", "tp"),
        P("seq", "tp"),
    )
    return jax.shard_map(
        per_device, mesh=mesh, in_specs=placed, out_specs=P(("seq", "tp"), None), check_vma=False
    )
```

```python
import functools
import math

import jax
import jax.numpy as jnp
from jax import lax
from jax.experimental import pallas as pl
from jax.experimental.pallas import tpu as pltpu
from jax.sharding import PartitionSpec as P

HEAD = 128
BLOCK = 128
EPS = 1e-06
LAG = 4


def offsets(blocks):
    return (jnp.cumsum(blocks) - blocks) * BLOCK


def rms_scale(values, gain):
    return values * lax.rsqrt(jnp.mean(values * values, axis=-1, keepdims=True) + EPS) * gain


def attention_kernel(rows, span, q_ref, k_ref, v_ref, out_ref):
    first = pl.program_id(0) * rows
    query = q_ref[...]

    def step(at, carry, masked):
        numer, denom = carry
        start = pl.multiple_of(at * span, span)
        score = lax.dot_general(
            query,
            k_ref[pl.ds(start, span), :],
            (((1,), (1,)), ((), ())),
            preferred_element_type=jnp.float32,
        )
        weight = jnp.exp(50.0 * jnp.tanh(score * (1.0 / 50.0)))
        if masked:
            places = first + lax.broadcasted_iota(jnp.int32, weight.shape, 0)
            keys = start + lax.broadcasted_iota(jnp.int32, weight.shape, 1)
            weight = jnp.where(keys <= places, weight, 0.0)
        denom = denom + jnp.sum(weight, axis=1, keepdims=True)
        numer = numer + jnp.dot(
            weight.astype(jnp.bfloat16),
            v_ref[pl.ds(start, span), :],
            preferred_element_type=jnp.float32,
        )
        return numer, denom

    whole = first // span
    state = (jnp.zeros((rows, HEAD), jnp.float32), jnp.zeros((rows, 1), jnp.float32))
    state = lax.fori_loop(0, whole, lambda at, c: step(at, c, False), state)
    numer, denom = step(whole, state, True)
    out_ref[...] = (numer / denom).astype(out_ref.dtype)


def attention(query, key, value):
    tokens = query.shape[0]
    rows, span = 256, 512
    return pl.pallas_call(
        functools.partial(attention_kernel, rows, span),
        grid=(tokens // rows,),
        in_specs=[
            pl.BlockSpec((rows, HEAD), lambda i: (i, 0)),
            pl.BlockSpec((tokens, HEAD), lambda i: (0, 0)),
            pl.BlockSpec((tokens, HEAD), lambda i: (0, 0)),
        ],
        out_specs=pl.BlockSpec((rows, HEAD), lambda i: (i, 0)),
        out_shape=jax.ShapeDtypeStruct((tokens, HEAD), jnp.bfloat16),
        cost_estimate=pl.CostEstimate(
            flops=3 * tokens * tokens * HEAD,
            bytes_accessed=8 * tokens * HEAD,
            transcendentals=tokens * tokens,
        ),
    )(query, key, value)


MESH = pl.DeviceIdType.MESH


def arrangements(seq_count):
    found = []
    for second in range(1, seq_count + 1):
        for third in range(1, second + 1):
            fourth = seq_count - second - third
            if 1 <= fourth <= third:
                found.append((seq_count, second, third, fourth))
    return found


def layer_windows(seq_count, tp_count, per_block):
    first, last = [], []
    for layer in range(tp_count):
        starts, ends = [], []
        for counts in arrangements(seq_count):
            begin = sum(counts[u // per_block] for u in range(layer))
            starts.append(begin)
            ends.append(begin + counts[layer // per_block])
        first.append(min(starts))
        last.append(max(ends))
    return first, last


def pick(index, values):
    result = jnp.int32(values[0])
    for k in range(1, len(values)):
        result = jnp.where(index == k, jnp.int32(values[k]), result)
    return result


def flipped(index, mask):
    result = index
    bit = 1
    while bit <= mask:
        if mask & bit:
            result = result + bit - 2 * bit * lax.rem(index // bit, 2)
        bit *= 2
    return result


def output_kernel(
    heads,
    copies,
    seq_count,
    tp_count,
    share,
    first,
    last,
    perm_ref,
    place_ref,
    context_ref,
    weight_ref,
    residual_ref,
    gain_ref,
    out_ref,
    full,
    partial,
    left_in,
    right_in,
    left_out,
    right_out,
    total,
    sent,
    came,
    gather_send,
    gather_recv,
    left_send,
    left_recv,
    right_send,
    right_recv,
    swap_send,
    swap_recv,
):
    seq_index = lax.axis_index("seq")
    tp_index = lax.axis_index("tp")
    places = partial.shape[0]
    depth = weight_ref.shape[0]
    head = seq_index // copies
    chunks = full.shape[0]
    per_chunk = places // chunks
    chunk_rows = full.shape[1]

    barrier = pltpu.get_barrier_semaphore()
    for k in range(1, seq_count):
        pl.semaphore_signal(
            barrier,
            inc=1,
            device_id=(lax.rem(seq_index + k, seq_count), tp_index),
            device_id_type=MESH,
        )

    @pl.when(tp_index > 0)
    def _():
        pl.semaphore_signal(
            barrier, inc=1, device_id=(seq_index, tp_index - 1), device_id_type=MESH
        )

    @pl.when(tp_index < tp_count - 1)
    def _():
        pl.semaphore_signal(
            barrier, inc=1, device_id=(seq_index, tp_index + 1), device_id_type=MESH
        )

    own_columns = pl.ds(pl.multiple_of(head * HEAD, HEAD), HEAD)
    for chunk in range(chunks):
        for at in range(per_chunk):
            full[chunk, at * share : (at + 1) * share, own_columns] = context_ref[
                perm_ref[chunk * per_chunk + at]
            ]

    neighbours = jnp.where(tp_index > 0, 1, 0) + jnp.where(tp_index < tp_count - 1, 1, 0)
    pl.semaphore_wait(barrier, seq_count - 1 + neighbours)

    bits = heads.bit_length() - 1
    order = list(range(chunks))[::-1]

    def dims(chunk):
        outer = list(range(1, bits))
        return (outer[::-1] if chunk % 2 else outer) + ([0] if bits > 0 else [])

    def gather_copy(chunk, bit, combo, to_me):
        slot = flipped(head, (combo ^ (1 << bit)) if to_me else combo)
        columns = pl.ds(pl.multiple_of(slot * HEAD, HEAD), HEAD)
        partner = flipped(seq_index, copies << bit)
        view = full.at[chunk, :, columns]
        return pltpu.make_async_remote_copy(
            src_ref=view,
            dst_ref=view,
            send_sem=gather_send.at[chunk, bit, combo],
            recv_sem=gather_recv.at[chunk, bit, combo],
            device_id=(partner, tp_index),
            device_id_type=MESH,
        )

    def steps(chunk):
        held = [0]
        for bit in dims(chunk):
            yield bit, list(held)
            held = held + [c ^ (1 << bit) for c in held]

    def offer(at):
        if at < chunks:
            for bit, _ in steps(order[at]):
                gather_copy(order[at], bit, 0, False).start()

    offer(0)
    total[...] = jnp.zeros_like(total)

    def relay(at):
        chunk = order[at]
        stages = list(steps(chunk))
        for level, (bit, held) in enumerate(stages):
            for combo in held:
                gather_copy(chunk, bit, combo, True).wait_recv()
                for later, _ in stages[level + 1 :]:
                    gather_copy(chunk, later, combo ^ (1 << bit), False).start()
            if level == 0:
                offer(at + 1)

    def multiply(chunk):
        product = lax.dot_general(
            full[chunk],
            weight_ref[...],
            (((1,), (1,)), ((), ())),
            preferred_element_type=jnp.float32,
        ).astype(jnp.bfloat16)
        for at in range(per_chunk):
            partial[chunk * per_chunk + at] = product[at * share : (at + 1) * share]

    left_has = jnp.where(tp_index < tp_count - 1, pick(tp_index, last), 0)
    left_gives = pick(tp_index, [0] + last[:-1])
    right_has = jnp.where(tp_index > 0, pick(tp_index, first), places)
    right_gives = pick(tp_index, first[1:] + [places])

    def line_copy(place, source, landing, send, recv, step):
        return pltpu.make_async_remote_copy(
            src_ref=source.at[place],
            dst_ref=landing.at[place],
            send_sem=send.at[place],
            recv_sem=recv.at[place],
            device_id=(seq_index, tp_index + step),
            device_id_type=MESH,
        )

    def flow(place, has, gives, source, landing, send, recv, step):
        @pl.when(has)
        def _():
            line_copy(place, source, landing, send, recv, step).wait_recv()

        @pl.when(jnp.logical_and(has, gives))
        def _():
            source[place] = (
                partial[place].astype(jnp.float32) + landing[place].astype(jnp.float32)
            ).astype(jnp.bfloat16)

        @pl.when(jnp.logical_and(jnp.logical_not(has), gives))
        def _():
            source[place] = partial[place]

        @pl.when(gives)
        def _():
            line_copy(place, source, landing, send, recv, step).start()

    def swap_copy(other, mine, at):
        return pltpu.make_async_remote_copy(
            src_ref=sent.at[other],
            dst_ref=came.at[mine],
            send_sem=swap_send.at[at],
            recv_sem=swap_recv.at[at],
            device_id=(other, tp_index),
            device_id_type=MESH,
        )

    def line_step(at, carry):
        passed = at - LAG * (tp_count - 1 - tp_index)
        place = places - 1 - passed
        valid = jnp.logical_and(passed >= 0, passed < places)
        has = jnp.logical_and(valid, place < left_has)
        gives = jnp.logical_and(valid, place < left_gives)
        flow(place, has, gives, left_out, left_in, left_send, left_recv, -1)
        ends = jnp.logical_and(
            jnp.logical_and(valid, tp_index == 0), place < seq_count
        )

        @pl.when(ends)
        def _():
            sent[place] = (
                partial[place].astype(jnp.float32) + left_in[place].astype(jnp.float32)
            ).astype(jnp.bfloat16)

            @pl.when(place == seq_index)
            def _():
                came[place] = sent[place]

            @pl.when(place != seq_index)
            def _():
                swap_copy(
                    place, seq_index, lax.rem(place + seq_count - seq_index, seq_count)
                ).start()

        passed = at - LAG * tp_index
        place = places - 1 - passed
        valid = jnp.logical_and(passed >= 0, passed < places)
        has = jnp.logical_and(valid, place >= right_has)
        gives = jnp.logical_and(valid, place >= right_gives)
        flow(place, has, gives, right_out, right_in, right_send, right_recv, 1)
        return carry

    for at, chunk in enumerate(order):
        relay(at)
        multiply(chunk)
        lax.fori_loop(at * per_chunk, (at + 1) * per_chunk, line_step, 0)
    lax.fori_loop(places, places + LAG * (tp_count - 1), line_step, 0)

    def sum_step(place, carry):
        value = partial[place].astype(jnp.float32) + right_in[place].astype(jnp.float32)

        @pl.when(place < left_has)
        def _():
            total[place] = (value + left_in[place].astype(jnp.float32)).astype(jnp.bfloat16)

        @pl.when(place >= left_has)
        def _():
            total[place] = value.astype(jnp.bfloat16)

        return carry

    @pl.when(tp_index > 0)
    def _():
        lax.fori_loop(pick(tp_index, first), pick(tp_index, last), sum_step, 0)
        for j in range(seq_count):
            sent[j] = total[place_ref[j]]
        for k in range(1, seq_count):
            swap_copy(lax.rem(seq_index + k, seq_count), seq_index, k).start()
        came[seq_index] = sent[seq_index]

    for k in range(1, seq_count):
        swap_copy(
            lax.rem(seq_index + k, seq_count),
            lax.rem(seq_index + seq_count - k, seq_count),
            k,
        ).wait_recv()

    square = jnp.zeros((share, 1), jnp.float32)
    for s in range(seq_count):
        piece = came[s].astype(jnp.float32)
        square = square + jnp.sum(piece * piece, axis=1, keepdims=True)
    factor = lax.rsqrt(square * (1.0 / (depth * seq_count)) + EPS)
    for s in range(seq_count // 2):
        piece = jnp.concatenate([came[2 * s], came[2 * s + 1]], axis=1).astype(jnp.float32)
        columns = slice(2 * s * depth, (2 * s + 2) * depth)
        value = residual_ref[:, columns].astype(jnp.float32) + (
            piece * factor * gain_ref[:, columns]
        )
        out_ref[:, columns] = value.astype(jnp.bfloat16)

    for k in range(1, seq_count):
        swap_copy(lax.rem(seq_index + k, seq_count), seq_index, k).wait_send()
    for chunk in range(chunks):
        for bit, held in steps(chunk):
            for combo in held:
                gather_copy(chunk, bit, combo, False).wait_send()

    def drain(place, carry):
        @pl.when(place < left_gives)
        def _():
            line_copy(place, left_out, left_in, left_send, left_recv, -1).wait_send()

        @pl.when(place >= right_gives)
        def _():
            line_copy(place, right_out, right_in, right_send, right_recv, 1).wait_send()

        return carry

    lax.fori_loop(0, places, drain, 0)


def output_phase(context, w_out_t, residual, post_gain, new_blocks, seq_count, tp_count, heads):
    tokens = context.shape[0]
    depth = w_out_t.shape[0]
    share, width = residual.shape
    places = tokens // share
    per_block = BLOCK // share
    copies = seq_count // heads
    bits = heads.bit_length() - 1
    first, last = layer_windows(seq_count, tp_count, per_block)
    seq_index = lax.axis_index("seq")
    tp_index = lax.axis_index("tp")
    blocks = new_blocks * per_block
    new_start = jnp.sum(
        jnp.where(
            jnp.arange(seq_count)[None, :] < jnp.arange(seq_count)[:, None], blocks[None, :], 0
        ),
        axis=1,
    )
    slots = jnp.arange(tp_count * seq_count, dtype=jnp.int32)
    layer = jnp.arange(tp_count, dtype=jnp.int32)[:, None]
    valid = (blocks[None, :] > layer).astype(jnp.int32).reshape(-1)
    source = (new_start[None, :] + layer).reshape(-1)
    rank = jnp.sum(jnp.where(slots[None, :] < slots[:, None], valid[None, :], 0), axis=1)
    perm = jnp.sum(
        jnp.where(
            (jnp.arange(places)[:, None] == rank[None, :]) & (valid[None, :] > 0),
            source[None, :],
            0,
        ),
        axis=1,
    ).astype(jnp.int32)
    in_layer = (jnp.arange(tp_count) == tp_index)[:, None]
    place = jnp.sum(jnp.where(in_layer, rank.reshape(tp_count, seq_count), 0), axis=0)
    place = jnp.minimum(place, places - 1).astype(jnp.int32)
    mine = jnp.sum(jnp.where(jnp.arange(seq_count) == seq_index, blocks, 0))
    chunks = 4
    rows = tokens // chunks
    scratch_block = pltpu.VMEM((places, share, depth), jnp.bfloat16)
    swap_block = pltpu.VMEM((seq_count, share, depth), jnp.bfloat16)
    line_sem = pltpu.SemaphoreType.DMA((places,))
    gather_sem = pltpu.SemaphoreType.DMA((chunks, bits, heads))
    swap_sem = pltpu.SemaphoreType.DMA((seq_count,))
    result = pl.pallas_call(
        functools.partial(
            output_kernel, heads, copies, seq_count, tp_count, share, first, last
        ),
        out_shape=jax.ShapeDtypeStruct((share, width), jnp.bfloat16),
        in_specs=[pl.BlockSpec(memory_space=pltpu.SMEM)] * 2
        + [pl.BlockSpec(memory_space=pltpu.VMEM)] * 4,
        out_specs=pl.BlockSpec(memory_space=pltpu.VMEM),
        scratch_shapes=[
            pltpu.VMEM((chunks, rows, heads * HEAD), jnp.bfloat16),
            scratch_block,
            scratch_block,
            scratch_block,
            scratch_block,
            scratch_block,
            scratch_block,
            swap_block,
            swap_block,
            gather_sem,
            gather_sem,
            line_sem,
            line_sem,
            line_sem,
            line_sem,
            swap_sem,
            swap_sem,
        ],
        compiler_params=pltpu.CompilerParams(
            collective_id=0, has_side_effects=True, vmem_limit_bytes=56 * 2**20
        ),
        cost_estimate=pl.CostEstimate(
            flops=60_000_000_000, bytes_accessed=4 * tokens * depth, transcendentals=0
        ),
    )(perm, place, context.reshape(places, share, HEAD), w_out_t, residual, post_gain.reshape(1, -1))
    return jnp.where(tp_index < mine, result, jnp.zeros_like(result))


def per_device(
    x_old, old_blocks, new_blocks, order, pre_gain, post_gain, w_query, w_key, w_value, w_out_t
):
    seq_count = lax.axis_size("seq")
    tp_count = lax.axis_size("tp")
    capacity, quarter = x_old.shape
    width = quarter * tp_count
    tokens = seq_count * capacity // 2
    own = tokens // seq_count
    share = capacity // tp_count
    seq_index = lax.axis_index("seq")
    tp_index = lax.axis_index("tp")
    old_start = offsets(old_blocks)
    new_start = offsets(new_blocks)
    device_ids = jnp.arange(seq_count, dtype=jnp.int32)

    gathered = lax.all_gather(x_old, "seq", axis=0, tiled=True)

    def stored(row, count):
        row = jnp.minimum(row, tokens - count)
        shard = jnp.sum((old_start <= row).astype(jnp.int32)) - 1
        holder = jnp.sum(jnp.where(order == shard, device_ids, 0))
        begin = jnp.sum(jnp.where(device_ids == shard, old_start, 0))
        return lax.dynamic_slice_in_dim(gathered, holder * capacity + row - begin, count, 0)

    def shift(k):
        return [(i, (i + k) % tp_count) for i in range(tp_count)]

    def by_source(received):
        stack = jnp.stack(received)
        pieces = [
            lax.dynamic_index_in_dim(stack, lax.rem(tp_index - u + tp_count, tp_count), 0, False)
            for u in range(tp_count)
        ]
        return jnp.concatenate(pieces, axis=1)

    mine = jnp.concatenate(
        [stored(seq_index * own + at, BLOCK) for at in range(0, own, BLOCK)], axis=0
    )
    full_rows = by_source(
        [mine] + [lax.ppermute(mine, "tp", shift(k)) for k in range(1, tp_count)]
    )
    my_start = jnp.sum(jnp.where(device_ids == seq_index, new_start, 0))

    def slot_rows(place):
        return stored(my_start + place * share, share)

    residual = by_source(
        [slot_rows(tp_index)]
        + [
            lax.ppermute(slot_rows(lax.rem(tp_index + k, tp_count)), "tp", shift(k))
            for k in range(1, tp_count)
        ]
    )

    weights = lax.all_gather(
        jnp.concatenate([w_query, w_key, w_value], axis=1), "seq", axis=0, tiled=True
    )

    normed = rms_scale(full_rows.astype(jnp.float32), pre_gain).astype(jnp.bfloat16)
    normed, residual = lax.optimization_barrier((normed, residual))
    heads = w_query.shape[1] // HEAD
    kv_heads = w_key.shape[1] // HEAD
    group = heads // kv_heads
    copies = seq_count // heads
    raw = jnp.dot(normed, weights, preferred_element_type=jnp.float32)

    half = HEAD // 2
    inverse = jnp.exp(jnp.arange(half, dtype=jnp.float32) * (-2.0 * math.log(10000.0) / HEAD))
    places = seq_index * own + jnp.arange(own, dtype=jnp.int32)
    angles = places.astype(jnp.float32)[:, None] * inverse[None, :]
    cosine, sine = jnp.cos(angles), jnp.sin(angles)

    def rotate(at):
        first = raw[:, at * HEAD : at * HEAD + half]
        second = raw[:, at * HEAD + half : (at + 1) * HEAD]
        return jnp.concatenate(
            [first * cosine - second * sine, second * cosine + first * sine], axis=-1
        )

    scale = (width // (heads * tp_count)) ** (-0.5)
    queries = [(rotate(h) * scale).astype(jnp.bfloat16) for h in range(heads)]
    keys = [rotate(heads + g).astype(jnp.bfloat16) for g in range(kv_heads)]
    values = [
        raw[:, (heads + kv_heads + g) * HEAD : (heads + kv_heads + g + 1) * HEAD].astype(
            jnp.bfloat16
        )
        for g in range(kv_heads)
    ]
    sent = jnp.stack(
        [
            jnp.stack([queries[s // copies], keys[s // copies // group], values[s // copies // group]])
            for s in range(seq_count)
        ]
    )
    came = lax.all_to_all(sent, "seq", 0, 0, tiled=True)
    context = attention(
        came[:, 0].reshape(tokens, HEAD),
        came[:, 1].reshape(tokens, HEAD),
        came[:, 2].reshape(tokens, HEAD),
    )
    return output_phase(
        context, w_out_t, residual, post_gain, new_blocks, seq_count, tp_count, heads
    )


def solution(mesh):
    placed = (
        P("seq", "tp"),
        P(),
        P(),
        P(),
        P(),
        P(),
        P("seq", "tp"),
        P("seq", "tp"),
        P("seq", "tp"),
        P("seq", "tp"),
    )
    return jax.shard_map(
        per_device, mesh=mesh, in_specs=placed, out_specs=P(("seq", "tp"), None), check_vma=False
    )
```

```python
import functools
import math

import jax
import jax.numpy as jnp
import numpy as np
from jax import lax
from jax.experimental import pallas as pl
from jax.experimental.pallas import tpu as pltpu
from jax.sharding import PartitionSpec as P

HEAD = 128
BLOCK = 128
EPS = 1e-06
LAG = 4


def offsets(blocks):
    return (jnp.cumsum(blocks) - blocks) * BLOCK


def rms_scale(values, gain):
    return values * lax.rsqrt(jnp.mean(values * values, axis=-1, keepdims=True) + EPS) * gain


def attention_kernel(rows, span, q_ref, k_ref, v_ref, out_ref):
    first = pl.program_id(0) * rows
    query = q_ref[...]

    def step(at, carry, masked):
        numer, denom = carry
        start = pl.multiple_of(at * span, span)
        score = lax.dot_general(
            query,
            k_ref[pl.ds(start, span), :],
            (((1,), (1,)), ((), ())),
            preferred_element_type=jnp.float32,
        )
        weight = jnp.exp(50.0 * jnp.tanh(score * (1.0 / 50.0)))
        if masked:
            places = first + lax.broadcasted_iota(jnp.int32, weight.shape, 0)
            keys = start + lax.broadcasted_iota(jnp.int32, weight.shape, 1)
            weight = jnp.where(keys <= places, weight, 0.0)
        denom = denom + jnp.sum(weight, axis=1, keepdims=True)
        numer = numer + jnp.dot(
            weight.astype(jnp.bfloat16),
            v_ref[pl.ds(start, span), :],
            preferred_element_type=jnp.float32,
        )
        return numer, denom

    whole = first // span
    state = (jnp.zeros((rows, HEAD), jnp.float32), jnp.zeros((rows, 1), jnp.float32))
    state = lax.fori_loop(0, whole, lambda at, c: step(at, c, False), state)
    numer, denom = step(whole, state, True)
    out_ref[...] = (numer / denom).astype(out_ref.dtype)


def attention(query, key, value):
    tokens = query.shape[0]
    rows, span = 256, 512
    return pl.pallas_call(
        functools.partial(attention_kernel, rows, span),
        grid=(tokens // rows,),
        in_specs=[
            pl.BlockSpec((rows, HEAD), lambda i: (i, 0)),
            pl.BlockSpec((tokens, HEAD), lambda i: (0, 0)),
            pl.BlockSpec((tokens, HEAD), lambda i: (0, 0)),
        ],
        out_specs=pl.BlockSpec((rows, HEAD), lambda i: (i, 0)),
        out_shape=jax.ShapeDtypeStruct((tokens, HEAD), jnp.bfloat16),
        cost_estimate=pl.CostEstimate(
            flops=3 * tokens * tokens * HEAD,
            bytes_accessed=8 * tokens * HEAD,
            transcendentals=tokens * tokens,
        ),
    )(query, key, value)


MESH = pl.DeviceIdType.MESH


def arrangements(seq_count):
    found = []
    for second in range(1, seq_count + 1):
        for third in range(1, second + 1):
            fourth = seq_count - second - third
            if 1 <= fourth <= third:
                found.append((seq_count, second, third, fourth))
    return found


def layer_windows(seq_count, tp_count, per_block):
    first, last = [], []
    for layer in range(tp_count):
        starts, ends = [], []
        for counts in arrangements(seq_count):
            begin = sum(counts[u // per_block] for u in range(layer))
            starts.append(begin)
            ends.append(begin + counts[layer // per_block])
        first.append(min(starts))
        last.append(max(ends))
    return first, last


def pick(index, values):
    result = jnp.int32(values[0])
    for k in range(1, len(values)):
        result = jnp.where(index == k, jnp.int32(values[k]), result)
    return result


def flipped(index, mask):
    result = index
    bit = 1
    while bit <= mask:
        if mask & bit:
            result = result + bit - 2 * bit * lax.rem(index // bit, 2)
        bit *= 2
    return result


def output_kernel(
    heads,
    copies,
    seq_count,
    tp_count,
    share,
    first,
    last,
    scattered,
    perm_ref,
    place_ref,
    block_ref,
    context_ref,
    weight_ref,
    residual_ref,
    gain_ref,
    out_ref,
    full,
    partial,
    left_in,
    right_in,
    left_out,
    right_out,
    total,
    sent,
    came,
    gather_send,
    gather_recv,
    left_send,
    left_recv,
    right_send,
    right_recv,
    swap_send,
    swap_recv,
    old_sent,
    old_came,
    old_send,
    old_recv,
):
    seq_index = lax.axis_index("seq")
    tp_index = lax.axis_index("tp")
    places = partial.shape[0]
    depth = weight_ref.shape[0]
    head = seq_index // copies
    chunks = full.shape[0]
    per_chunk = places // chunks
    chunk_rows = full.shape[1]

    barrier = pltpu.get_barrier_semaphore()
    for k in range(1, seq_count):
        pl.semaphore_signal(
            barrier,
            inc=1,
            device_id=(lax.rem(seq_index + k, seq_count), tp_index),
            device_id_type=MESH,
        )

    @pl.when(tp_index > 0)
    def _():
        pl.semaphore_signal(
            barrier, inc=1, device_id=(seq_index, tp_index - 1), device_id_type=MESH
        )

    @pl.when(tp_index < tp_count - 1)
    def _():
        pl.semaphore_signal(
            barrier, inc=1, device_id=(seq_index, tp_index + 1), device_id_type=MESH
        )

    own_columns = pl.ds(pl.multiple_of(head * HEAD, HEAD), HEAD)
    for chunk in range(chunks):
        for at in range(per_chunk):
            full[chunk, at * share : (at + 1) * share, own_columns] = context_ref[
                perm_ref[chunk * per_chunk + at]
            ]

    neighbours = jnp.where(tp_index > 0, 1, 0) + jnp.where(tp_index < tp_count - 1, 1, 0)
    pl.semaphore_wait(barrier, seq_count - 1 + neighbours)

    bits = heads.bit_length() - 1
    order = list(range(chunks))[::-1]

    def dims(chunk):
        outer = list(range(1, bits))
        return (outer[::-1] if chunk % 2 else outer) + ([0] if bits > 0 else [])

    def gather_copy(chunk, bit, combo, to_me):
        slot = flipped(head, (combo ^ (1 << bit)) if to_me else combo)
        columns = pl.ds(pl.multiple_of(slot * HEAD, HEAD), HEAD)
        partner = flipped(seq_index, copies << bit)
        view = full.at[chunk, :, columns]
        return pltpu.make_async_remote_copy(
            src_ref=view,
            dst_ref=view,
            send_sem=gather_send.at[chunk, bit, combo],
            recv_sem=gather_recv.at[chunk, bit, combo],
            device_id=(partner, tp_index),
            device_id_type=MESH,
        )

    def steps(chunk):
        held = [0]
        for bit in dims(chunk):
            yield bit, list(held)
            held = held + [c ^ (1 << bit) for c in held]

    def offer(at):
        if at < chunks:
            for bit, _ in steps(order[at]):
                gather_copy(order[at], bit, 0, False).start()

    offer(0)
    total[...] = jnp.zeros_like(total)

    def relay(at):
        chunk = order[at]
        stages = list(steps(chunk))
        for level, (bit, held) in enumerate(stages):
            for combo in held:
                gather_copy(chunk, bit, combo, True).wait_recv()
                for later, _ in stages[level + 1 :]:
                    gather_copy(chunk, later, combo ^ (1 << bit), False).start()
            if level == 0:
                offer(at + 1)

    def multiply(chunk):
        product = lax.dot_general(
            full[chunk],
            weight_ref[...],
            (((1,), (1,)), ((), ())),
            preferred_element_type=jnp.float32,
        ).astype(jnp.bfloat16)
        for at in range(per_chunk):
            partial[chunk * per_chunk + at] = product[at * share : (at + 1) * share]

    left_has = jnp.where(tp_index < tp_count - 1, pick(tp_index, last), 0)
    left_gives = pick(tp_index, [0] + last[:-1])
    right_has = jnp.where(tp_index > 0, pick(tp_index, first), places)
    right_gives = pick(tp_index, first[1:] + [places])

    def line_copy(place, source, landing, send, recv, step):
        return pltpu.make_async_remote_copy(
            src_ref=source.at[place],
            dst_ref=landing.at[place],
            send_sem=send.at[place],
            recv_sem=recv.at[place],
            device_id=(seq_index, tp_index + step),
            device_id_type=MESH,
        )

    def flow(place, has, gives, source, landing, send, recv, step):
        @pl.when(has)
        def _():
            line_copy(place, source, landing, send, recv, step).wait_recv()

        @pl.when(jnp.logical_and(has, gives))
        def _():
            source[place] = (
                partial[place].astype(jnp.float32) + landing[place].astype(jnp.float32)
            ).astype(jnp.bfloat16)

        @pl.when(jnp.logical_and(jnp.logical_not(has), gives))
        def _():
            source[place] = partial[place]

        @pl.when(gives)
        def _():
            line_copy(place, source, landing, send, recv, step).start()

    def swap_copy(other, mine, at):
        return pltpu.make_async_remote_copy(
            src_ref=sent.at[other],
            dst_ref=came.at[mine],
            send_sem=swap_send.at[at],
            recv_sem=swap_recv.at[at],
            device_id=(other, tp_index),
            device_id_type=MESH,
        )

    def line_step(at, carry):
        passed = at - LAG * (tp_count - 1 - tp_index)
        place = places - 1 - passed
        valid = jnp.logical_and(passed >= 0, passed < places)
        has = jnp.logical_and(valid, place < left_has)
        gives = jnp.logical_and(valid, place < left_gives)
        flow(place, has, gives, left_out, left_in, left_send, left_recv, -1)
        ends = jnp.logical_and(
            jnp.logical_and(valid, tp_index == 0), place < seq_count
        )

        @pl.when(ends)
        def _():
            sent[place] = (
                partial[place].astype(jnp.float32) + left_in[place].astype(jnp.float32)
            ).astype(jnp.bfloat16)

            @pl.when(place == seq_index)
            def _():
                came[place] = sent[place]

            @pl.when(place != seq_index)
            def _():
                swap_copy(
                    place, seq_index, lax.rem(place + seq_count - seq_index, seq_count)
                ).start()

        passed = at - LAG * tp_index
        place = places - 1 - passed
        valid = jnp.logical_and(passed >= 0, passed < places)
        has = jnp.logical_and(valid, place >= right_has)
        gives = jnp.logical_and(valid, place >= right_gives)
        flow(place, has, gives, right_out, right_in, right_send, right_recv, 1)
        return carry

    for at, chunk in enumerate(order):
        relay(at)
        multiply(chunk)
        lax.fori_loop(at * per_chunk, (at + 1) * per_chunk, line_step, 0)

    def old_copy(other, mine, at):
        return pltpu.make_async_remote_copy(
            src_ref=old_sent.at[other],
            dst_ref=old_came.at[mine],
            send_sem=old_send.at[at],
            recv_sem=old_recv.at[at],
            device_id=(other, tp_index),
            device_id_type=MESH,
        )

    if scattered:
        for j in range(seq_count):
            old_sent[j] = residual_ref[block_ref[j]]
        for k in range(1, seq_count):
            old_copy(lax.rem(seq_index + k, seq_count), seq_index, k).start()
        old_came[seq_index] = old_sent[seq_index]
    lax.fori_loop(places, places + LAG * (tp_count - 1), line_step, 0)

    def sum_step(place, carry):
        value = partial[place].astype(jnp.float32) + right_in[place].astype(jnp.float32)

        @pl.when(place < left_has)
        def _():
            total[place] = (value + left_in[place].astype(jnp.float32)).astype(jnp.bfloat16)

        @pl.when(place >= left_has)
        def _():
            total[place] = value.astype(jnp.bfloat16)

        return carry

    @pl.when(tp_index > 0)
    def _():
        lax.fori_loop(pick(tp_index, first), pick(tp_index, last), sum_step, 0)
        for j in range(seq_count):
            sent[j] = total[place_ref[j]]
        for k in range(1, seq_count):
            swap_copy(lax.rem(seq_index + k, seq_count), seq_index, k).start()
        came[seq_index] = sent[seq_index]

    for k in range(1, seq_count):
        swap_copy(
            lax.rem(seq_index + k, seq_count),
            lax.rem(seq_index + seq_count - k, seq_count),
            k,
        ).wait_recv()

    if scattered:
        for k in range(1, seq_count):
            old_copy(
                lax.rem(seq_index + k, seq_count),
                lax.rem(seq_index + seq_count - k, seq_count),
                k,
            ).wait_recv()
    square = jnp.zeros((share, 1), jnp.float32)
    for s in range(seq_count):
        piece = came[s].astype(jnp.float32)
        square = square + jnp.sum(piece * piece, axis=1, keepdims=True)
    factor = lax.rsqrt(square * (1.0 / (depth * seq_count)) + EPS)
    for s in range(seq_count // 2):
        piece = jnp.concatenate([came[2 * s], came[2 * s + 1]], axis=1).astype(jnp.float32)
        columns = slice(2 * s * depth, (2 * s + 2) * depth)
        if scattered:
            old = jnp.concatenate([old_came[2 * s], old_came[2 * s + 1]], axis=0)
        else:
            old = residual_ref[:, columns]
        value = old.astype(jnp.float32) + (
            piece * factor * gain_ref[:, columns]
        )
        out_ref[:, columns] = value.astype(jnp.bfloat16)

    for k in range(1, seq_count):
        swap_copy(lax.rem(seq_index + k, seq_count), seq_index, k).wait_send()
    if scattered:
        for k in range(1, seq_count):
            old_copy(lax.rem(seq_index + k, seq_count), seq_index, k).wait_send()
    for chunk in range(chunks):
        for bit, held in steps(chunk):
            for combo in held:
                gather_copy(chunk, bit, combo, False).wait_send()

    def drain(place, carry):
        @pl.when(place < left_gives)
        def _():
            line_copy(place, left_out, left_in, left_send, left_recv, -1).wait_send()

        @pl.when(place >= right_gives)
        def _():
            line_copy(place, right_out, right_in, right_send, right_recv, 1).wait_send()

        return carry

    lax.fori_loop(0, places, drain, 0)


def front_kernel(
    seq_count,
    tp_count,
    group,
    scale,
    blocks_ref,
    order_ref,
    x_ref,
    gain_ref,
    query_ref,
    key_ref,
    value_ref,
    angle_ref,
    q_out,
    kv_out,
    x_out,
    near,
    send_a,
    send_b,
    far,
    line,
    twin,
    weight,
    normed,
    scale_row,
    scale_all,
    scale_column,
    first_out,
    first_in,
    second_out,
    second_in,
    kept,
    core_sem,
    weight_sem,
    stage_sem,
    line_send,
    line_recv,
    plane_send,
    plane_recv,
    twin_sem,
    stat_sem,
    factor_sem,
    first_sem,
    second_sem,
    kv_sem,
):
    seq_index = lax.axis_index("seq")
    tp_index = lax.axis_index("tp")
    chip = seq_index // 2
    core = lax.rem(seq_index, 2)
    partner = seq_index + 1 - 2 * core
    slots = x_ref.shape[0]
    chips = seq_count // 2
    each = line.shape[1]
    half = line.shape[2]
    quarter = line.shape[3]
    depth = query_ref.shape[0]
    pair = 2 * HEAD

    barrier = pltpu.get_barrier_semaphore()
    for k in range(1, seq_count):
        other = lax.rem(seq_index + k, seq_count)
        pl.semaphore_signal(barrier, inc=1, device_id=(other, tp_index), device_id_type=MESH)
    for k in range(1, tp_count):
        other = lax.rem(tp_index + k, tp_count)
        pl.semaphore_signal(barrier, inc=1, device_id=(seq_index, other), device_id_type=MESH)

    def remote(source, target, sems, at, seq, tp):
        return pltpu.make_async_remote_copy(
            src_ref=source,
            dst_ref=target,
            send_sem=sems[0].at[at],
            recv_sem=sems[1].at[at],
            device_id=(seq, tp),
            device_id_type=MESH,
        )

    core_sems = (core_sem.at[0], core_sem.at[1])

    def swap_slots(holder):
        return remote(
            x_ref.at[:, 1 - core],
            near.at[pl.ds(slots * holder, slots)],
            core_sems,
            0,
            partner,
            tp_index,
        )

    def lanes(head, count=1):
        return pl.ds(pl.multiple_of(head * HEAD, HEAD), count * HEAD)

    def weight_copy(source, column, target, at, holder):
        return remote(
            source.at[:, lanes(column)],
            weight.at[pl.ds(pl.multiple_of(holder * depth, depth), depth), lanes(target)],
            (weight_sem.at[0], weight_sem.at[1]),
            at,
            partner,
            tp_index,
        )

    pl.semaphore_wait(barrier, seq_count - 1 + tp_count - 1)
    swap_slots(core).start()
    for slot in range(slots):
        near[slots * core + slot] = x_ref[slot, core]

    starts, counts, holders = [], [], []
    begin = jnp.int32(0)
    for k in range(seq_count):
        starts.append(begin)
        counts.append(blocks_ref[k])
        begin = begin + blocks_ref[k]
        holder = jnp.int32(0)
        for place in range(1, seq_count):
            holder = holder + jnp.where(order_ref[place] == k, jnp.int32(place), jnp.int32(0))
        holders.append(holder)

    def found(block):
        at = jnp.int32(0)
        for k in range(seq_count):
            inside = jnp.logical_and(starts[k] <= block, block < starts[k] + counts[k])
            at = at + jnp.where(inside, holders[k] * slots + block - starts[k], jnp.int32(0))
        return at // (2 * slots), lax.rem(at, 2 * slots)

    first_chip = jnp.where(core == 0, flipped(chip, 1), flipped(chip, 2))
    second_chip = jnp.where(core == 0, flipped(chip, 2), flipped(chip, 1))
    cross_chip = flipped(chip, 3)
    swap_slots(1 - core).wait_recv()

    stage_sems = (stage_sem.at[0], stage_sem.at[1])
    table_a = []
    for at in range(2 * each):
        target = first_chip if at < each else cross_chip
        owner, index = found(each * target + at % each)
        table_a.append(jnp.where(owner == chip, index, 0))
    across_first = list(range(each, 2 * each)) + list(range(each))
    for at in across_first:
        send_a[at] = near[table_a[at]]
        remote(
            send_a.at[at], far.at[at], stage_sems, at, 2 * first_chip + core, tp_index
        ).start()

    for c in range(chips):
        weight_copy(query_ref, 2 * c + 1 - core, 2 * c, 2 * c, core).start()

        @pl.when(core == 0)
        def _():
            weight_copy(value_ref, c, 2 * c + 1, 2 * c + 1, core).start()

        @pl.when(core == 1)
        def _():
            weight_copy(key_ref, c, 2 * c + 1, 2 * c + 1, core).start()

    own_rows = pl.ds(pl.multiple_of(core * depth, depth), depth)
    for c in range(chips):
        weight[own_rows, pl.ds(2 * c * HEAD, HEAD)] = query_ref[:, lanes(2 * c + core)]

        @pl.when(core == 0)
        def _():
            weight[own_rows, pl.ds((2 * c + 1) * HEAD, HEAD)] = key_ref[
                :, pl.ds(c * HEAD, HEAD)
            ]

        @pl.when(core == 1)
        def _():
            weight[own_rows, pl.ds((2 * c + 1) * HEAD, HEAD)] = value_ref[
                :, pl.ds(c * HEAD, HEAD)
            ]

    def arrive_a(at):
        remote(
            send_a.at[at], far.at[at], stage_sems, at, 2 * first_chip + core, tp_index
        ).wait_recv()

    both = 2 * slots
    for at in range(each, 2 * each):
        arrive_a(at)
        near[both + at] = far[at]
    for at in range(each):
        owner, index = found(each * second_chip + at)
        send_b[at] = near[jnp.where(owner == chip, index, both + each + at)]
        remote(
            send_b.at[at],
            far.at[2 * each + at],
            stage_sems,
            2 * each + at,
            2 * second_chip + core,
            tp_index,
        ).start()
    for at in range(each):
        arrive_a(at)
        near[both + at] = far[at]
    for at in range(each):
        owner, index = found(each * chip + at)
        near[both + 2 * each + at] = near[jnp.where(owner == chip, index, both + at)]
    for at in range(each):
        remote(
            send_b.at[at],
            far.at[2 * each + at],
            stage_sems,
            2 * each + at,
            2 * second_chip + core,
            tp_index,
        ).wait_recv()
        near[both + 3 * each + at] = far[2 * each + at]
    for at in range(each):
        owner, _ = found(each * chip + at)
        local = jnp.logical_or(owner == chip, owner == first_chip)
        line[tp_index, at] = near[
            jnp.where(local, both + 2 * each + at, both + 3 * each + at)
        ]

    def line_copy(layer, at, step):
        view = line.at[layer, at]
        return pltpu.make_async_remote_copy(
            src_ref=view,
            dst_ref=view,
            send_sem=line_send.at[(step + 1) // 2, layer, at],
            recv_sem=line_recv.at[layer, at],
            device_id=(seq_index, tp_index + step),
            device_id_type=MESH,
        )

    def plane_copy(layer, at, holder):
        return pltpu.make_async_remote_copy(
            src_ref=line.at[layer, at],
            dst_ref=x_out.at[each * holder + at],
            send_sem=plane_send.at[layer, at],
            recv_sem=plane_recv.at[each * holder + at],
            device_id=(2 * layer + core, tp_index),
            device_id_type=MESH,
        )

    def twin_copy(block):
        return remote(
            x_out.at[block],
            twin.at[block],
            (twin_sem.at[0], twin_sem.at[1]),
            block,
            partner,
            tp_index,
        )

    def guarded(condition, action):
        @pl.when(condition)
        def _():
            action()

    def forward(layer, at):
        @pl.when(layer == chip)
        def _():
            x_out[each * chip + at] = line[layer, at]

        @pl.when(layer != chip)
        def _():
            plane_copy(layer, at, chip).start()

    def own_step(at):
        guarded(tp_index > 0, lambda: line_copy(tp_index, at, -1).start())
        guarded(tp_index < tp_count - 1, lambda: line_copy(tp_index, at, 1).start())
        forward(tp_index, at)

    def hop_step(at, distance):
        @pl.when(tp_index >= distance)
        def _():
            layer = tp_index - distance
            line_copy(layer, at, 1).wait_recv()
            guarded(tp_index < tp_count - 1, lambda: line_copy(layer, at, 1).start())
            forward(layer, at)

        @pl.when(tp_index + distance < tp_count)
        def _():
            layer = tp_index + distance
            line_copy(layer, at, -1).wait_recv()
            guarded(tp_index > 0, lambda: line_copy(layer, at, -1).start())
            forward(layer, at)

    def plane_step(at):
        for c in range(chips):

            @pl.when(chip != c)
            def _():
                plane_copy(chip, at, c).wait_recv()

        for c in range(chips):
            twin_copy(each * c + at).start()

    tiles = quarter // HEAD
    gain_at = pl.multiple_of(chip * quarter, HEAD)

    def normalize(source, block, holder, target):
        rows = pl.ds(pl.multiple_of(lax.rem(block, each) * half, half), half)
        factor = scale_column[holder, rows, :]
        for tile in range(tiles):
            columns = slice(tile * HEAD, (tile + 1) * HEAD)
            values = source[block, :, columns].astype(jnp.float32)
            gains = gain_ref[:, pl.ds(pl.multiple_of(gain_at + tile * HEAD, HEAD), HEAD)]
            normed[target[0], target[1], target[2], :, columns] = (
                values * factor * gains
            ).astype(jnp.bfloat16)

    bits = (1, 2)

    def first_copy(at, side):
        bit = bits[side]
        return pltpu.make_async_remote_copy(
            src_ref=first_out.at[at, side],
            dst_ref=first_in.at[at, side],
            send_sem=first_sem.at[0, at, side],
            recv_sem=first_sem.at[1, at, side],
            device_id=(2 * flipped(chip, bit) + core, tp_index),
            device_id_type=MESH,
        )

    def second_copy(at, side):
        bit = bits[1 - side]
        return pltpu.make_async_remote_copy(
            src_ref=second_out.at[at, side],
            dst_ref=second_in.at[at, side],
            send_sem=second_sem.at[0, at, side],
            recv_sem=second_sem.at[1, at, side],
            device_id=(2 * flipped(chip, bit) + core, tp_index),
            device_id_type=MESH,
        )

    def multiply_step(at):
        for side in range(2):
            for u in range(2):
                c = 2 * side + u
                block = each * c + at
                twin_copy(block).wait_recv()
                normalize(x_out, block, 2 * c + core, (side, u, core))
                normalize(twin, block, 2 * c + 1 - core, (side, u, 1 - core))
            rows = normed[side].reshape(4 * half, quarter)

            def part(mask):
                target = flipped(chip, mask)
                return jnp.dot(
                    rows,
                    weight[:, lanes(2 * target, 2)],
                    preferred_element_type=jnp.float32,
                )

            first, second = bits[side], bits[1 - side]
            first_out[at, side, 0] = part(first).astype(jnp.bfloat16)
            first_out[at, side, 1] = part(3).astype(jnp.bfloat16)
            first_copy(at, side).start()
            kept[at, side, 0] = part(0)
            kept[at, side, 1] = part(second)

    def add_step(at):
        for side in range(2):
            first_copy(at, side).wait_recv()
            second_out[at, side] = (
                kept[at, side, 1] + first_in[at, side, 1].astype(jnp.float32)
            ).astype(jnp.bfloat16)
            second_copy(at, side).start()

    def kv_copy(kind, block):
        rows = pl.ds(pl.multiple_of(block * BLOCK, BLOCK), BLOCK)
        view = kv_out.at[kind, rows, :]
        return remote(
            view, view, (kv_sem.at[0], kv_sem.at[1]), block, partner, tp_index
        )

    lane = lax.broadcasted_iota(jnp.int32, (BLOCK, HEAD), 1)

    def turned(values, rows):
        angles = angle_ref[rows, :]
        swapped = pltpu.roll(angles, HEAD // 2, 1)
        low = lane < HEAD // 2
        cosine = jnp.where(low, angles, swapped)
        sine = jnp.where(low, -swapped, angles)
        return values * cosine + pltpu.roll(values, HEAD // 2, 1) * sine

    def finish_step(at):
        for side in range(2):
            second_copy(at, side).wait_recv()
            for u in range(2):
                block = each * (2 * side + u) + at
                part = slice(u * BLOCK, (u + 1) * BLOCK)
                value = (
                    kept[at, side, 0, part]
                    + first_in[at, side, 0, part].astype(jnp.float32)
                    + second_in[at, side, part].astype(jnp.float32)
                )
                rows = pl.ds(pl.multiple_of(block * BLOCK, BLOCK), BLOCK)
                q_out[rows, :] = (turned(value[:, :HEAD], rows) * scale).astype(jnp.bfloat16)

                @pl.when(core == 0)
                def _():
                    kv_out[0, rows, :] = turned(value[:, HEAD:], rows).astype(jnp.bfloat16)

                @pl.when(core == 1)
                def _():
                    kv_out[1, rows, :] = value[:, HEAD:].astype(jnp.bfloat16)

                kv_copy(core, block).start()

    def stat_copy(layer_from, layer_to):
        return pltpu.make_async_remote_copy(
            src_ref=scale_row.at[layer_from],
            dst_ref=scale_row.at[layer_from],
            send_sem=stat_sem.at[0, layer_to],
            recv_sem=stat_sem.at[1, layer_from],
            device_id=(seq_index, layer_to),
            device_id_type=MESH,
        )

    def factor_copy(holder, other):
        return pltpu.make_async_remote_copy(
            src_ref=scale_all.at[holder],
            dst_ref=scale_all.at[holder],
            send_sem=factor_sem.at[0, other],
            recv_sem=factor_sem.at[1, holder],
            device_id=(other, tp_index),
            device_id_type=MESH,
        )

    own_step(0)
    squares = []
    for at in range(each):
        values = line[tp_index, at].astype(jnp.float32)
        squares.append(jnp.sum(values * values, axis=1, keepdims=True))
    column = jnp.broadcast_to(jnp.concatenate(squares, axis=0), (each * half, HEAD))
    scale_row[tp_index] = jnp.transpose(column)[:8, :]
    for k in range(1, tp_count):
        stat_copy(tp_index, lax.rem(tp_index + k, tp_count)).start()
    for c in range(2 * chips):
        weight_copy(query_ref, 0, 0, c, 1 - core).wait_recv()
    for k in range(1, tp_count):
        other = lax.rem(tp_index + k, tp_count)
        stat_copy(other, tp_index).wait_recv()
    square = scale_row[0]
    for k in range(1, tp_count):
        square = square + scale_row[k]
    scale_all[seq_index] = lax.rsqrt(square * (1.0 / (quarter * tp_count)) + EPS)
    for k in range(1, seq_count):
        factor_copy(seq_index, lax.rem(seq_index + k, seq_count)).start()

    def steps(i, carry):
        for lag, action in (
            (0, lambda at: guarded(at > 0, lambda: own_step(at))),
            (1, lambda at: hop_step(at, 1)),
            (2, lambda at: hop_step(at, 2)),
            (3, lambda at: hop_step(at, 3)),
            (4, plane_step),
            (5, multiply_step),
            (6, add_step),
            (7, finish_step),
        ):
            at = i - lag

            @pl.when(jnp.logical_and(at >= 0, at < each))
            def _():
                action(at)

        return carry

    lax.fori_loop(0, 5, steps, 0)
    for k in range(1, seq_count):
        other = lax.rem(seq_index + k, seq_count)
        factor_copy(other, seq_index).wait_recv()
    for s in range(seq_count):
        scale_column[s] = jnp.transpose(
            jnp.broadcast_to(scale_all[s, :1, :], (HEAD, each * half))
        )
    lax.fori_loop(5, each + 7, steps, 0)

    def last(block, carry):
        kv_copy(1 - core, block).wait_recv()
        return carry

    lax.fori_loop(0, each * chips, last, 0)

    swap_slots(core).wait_send()
    for c in range(2 * chips):
        weight_copy(query_ref, 0, 0, c, core).wait_send()
    for at in range(2 * each):
        remote(
            send_a.at[at], far.at[at], stage_sems, at, 2 * first_chip + core, tp_index
        ).wait_send()
    for at in range(each):
        remote(
            send_b.at[at],
            far.at[2 * each + at],
            stage_sems,
            2 * each + at,
            2 * second_chip + core,
            tp_index,
        ).wait_send()
    for k in range(1, tp_count):
        stat_copy(tp_index, lax.rem(tp_index + k, tp_count)).wait_send()
    for k in range(1, seq_count):
        factor_copy(seq_index, lax.rem(seq_index + k, seq_count)).wait_send()

    def drain(at, carry):
        for layer in range(tp_count):
            right = jnp.logical_and(tp_index >= layer, tp_index < tp_count - 1)
            guarded(right, lambda: line_copy(layer, at, 1).wait_send())
            left = jnp.logical_and(tp_index <= layer, tp_index > 0)
            guarded(left, lambda: line_copy(layer, at, -1).wait_send())
            guarded(chip != layer, lambda: plane_copy(layer, at, chip).wait_send())
        for side in range(2):
            first_copy(at, side).wait_send()
            second_copy(at, side).wait_send()
        for c in range(chips):
            twin_copy(each * c + at).wait_send()
            kv_copy(core, each * c + at).wait_send()
        return carry

    lax.fori_loop(0, each, drain, 0)


def front_fits(seq_count, tp_count, heads, kv_heads, capacity):
    return (
        heads == seq_count == 8
        and 2 * kv_heads == heads
        and tp_count == 4
        and capacity == 4 * BLOCK
    )


def front_phase(
    x_old, old_blocks, order, pre_gain, w_query, w_key, w_value, seq_count, tp_count, scale
):
    capacity, quarter = x_old.shape
    depth = w_query.shape[0]
    slots = capacity // BLOCK
    half = BLOCK // 2
    tokens = seq_count * capacity // 2
    chips = seq_count // 2
    each = tokens // BLOCK // chips
    group = w_query.shape[1] // w_key.shape[1]
    angles = (
        np.arange(tokens, dtype=np.float32)[:, None]
        * np.exp(
            np.arange(HEAD // 2, dtype=np.float32) * np.float32(-2.0 * math.log(10000.0) / HEAD)
        )[None, :]
    )
    table = np.concatenate([np.cos(angles), np.sin(angles)], axis=1).astype(np.float32)
    bf16, f32 = jnp.bfloat16, jnp.float32
    piece = (half, quarter)
    dma = pltpu.SemaphoreType.DMA
    vmem = pl.BlockSpec(memory_space=pltpu.VMEM)
    smem = pl.BlockSpec(memory_space=pltpu.SMEM)
    square = (2 * BLOCK, 2 * HEAD)
    return pl.pallas_call(
        functools.partial(front_kernel, seq_count, tp_count, group, scale),
        out_shape=(
            jax.ShapeDtypeStruct((tokens, HEAD), bf16),
            jax.ShapeDtypeStruct((2, tokens, HEAD), bf16),
            jax.ShapeDtypeStruct((each * chips,) + piece, bf16),
        ),
        in_specs=[smem] * 2 + [vmem] * 6,
        out_specs=(vmem, vmem, vmem),
        scratch_shapes=[
            pltpu.VMEM((2 * slots + 4 * each,) + piece, bf16),
            pltpu.VMEM((2 * each,) + piece, bf16),
            pltpu.VMEM((each,) + piece, bf16),
            pltpu.VMEM((3 * each,) + piece, bf16),
            pltpu.VMEM((tp_count, each) + piece, bf16),
            pltpu.VMEM((each * chips,) + piece, bf16),
            pltpu.VMEM((2 * depth, 2 * chips * HEAD), bf16),
            pltpu.VMEM((2, 2, 2) + piece, bf16),
            pltpu.VMEM((tp_count, 8, each * half), f32),
            pltpu.VMEM((seq_count, 8, each * half), f32),
            pltpu.VMEM((seq_count, each * half, HEAD), f32),
            pltpu.VMEM((each, 2, 2) + square, bf16),
            pltpu.VMEM((each, 2, 2) + square, bf16),
            pltpu.VMEM((each, 2) + square, bf16),
            pltpu.VMEM((each, 2) + square, bf16),
            pltpu.VMEM((each, 2, 2) + square, f32),
            dma((2, 1)),
            dma((2, 2 * chips)),
            dma((2, 3 * each)),
            dma((2, tp_count, each)),
            dma((tp_count, each)),
            dma((tp_count, each)),
            dma((each * chips,)),
            dma((2, each * chips)),
            dma((2, tp_count)),
            dma((2, seq_count)),
            dma((2, each, 2)),
            dma((2, each, 2)),
            dma((2, each * chips)),
        ],
        compiler_params=pltpu.CompilerParams(
            collective_id=1, has_side_effects=True, vmem_limit_bytes=60 * 2**20
        ),
        cost_estimate=pl.CostEstimate(
            flops=60_000_000_000, bytes_accessed=8 * tokens * depth, transcendentals=0
        ),
    )(
        old_blocks,
        order,
        x_old.reshape(slots, 2, half, quarter),
        pre_gain.reshape(1, -1),
        w_query,
        w_key,
        w_value,
        jnp.asarray(table),
    )


def output_phase(context, w_out_t, residual, post_gain, new_blocks, seq_count, tp_count, heads):
    tokens = context.shape[0]
    depth = w_out_t.shape[0]
    width = depth * seq_count
    share = 2 * tokens // (seq_count * tp_count)
    scattered = residual.ndim == 3
    places = tokens // share
    per_block = BLOCK // share
    copies = seq_count // heads
    bits = heads.bit_length() - 1
    first, last = layer_windows(seq_count, tp_count, per_block)
    seq_index = lax.axis_index("seq")
    tp_index = lax.axis_index("tp")
    blocks = new_blocks * per_block
    new_start = jnp.sum(
        jnp.where(
            jnp.arange(seq_count)[None, :] < jnp.arange(seq_count)[:, None], blocks[None, :], 0
        ),
        axis=1,
    )
    slots = jnp.arange(tp_count * seq_count, dtype=jnp.int32)
    layer = jnp.arange(tp_count, dtype=jnp.int32)[:, None]
    valid = (blocks[None, :] > layer).astype(jnp.int32).reshape(-1)
    source = (new_start[None, :] + layer).reshape(-1)
    rank = jnp.sum(jnp.where(slots[None, :] < slots[:, None], valid[None, :], 0), axis=1)
    perm = jnp.sum(
        jnp.where(
            (jnp.arange(places)[:, None] == rank[None, :]) & (valid[None, :] > 0),
            source[None, :],
            0,
        ),
        axis=1,
    ).astype(jnp.int32)
    in_layer = (jnp.arange(tp_count) == tp_index)[:, None]
    place = jnp.sum(jnp.where(in_layer, rank.reshape(tp_count, seq_count), 0), axis=0)
    place = jnp.minimum(place, places - 1).astype(jnp.int32)
    mine = jnp.sum(jnp.where(jnp.arange(seq_count) == seq_index, blocks, 0))
    block = jnp.minimum((new_start + tp_index) // per_block, tokens // BLOCK - 1).astype(jnp.int32)
    piece = residual.shape[1:] if scattered else (8, HEAD)
    old_block = pltpu.VMEM((seq_count,) + piece, jnp.bfloat16)
    chunks = 4
    rows = tokens // chunks
    scratch_block = pltpu.VMEM((places, share, depth), jnp.bfloat16)
    swap_block = pltpu.VMEM((seq_count, share, depth), jnp.bfloat16)
    line_sem = pltpu.SemaphoreType.DMA((places,))
    gather_sem = pltpu.SemaphoreType.DMA((chunks, bits, heads))
    swap_sem = pltpu.SemaphoreType.DMA((seq_count,))
    result = pl.pallas_call(
        functools.partial(
            output_kernel, heads, copies, seq_count, tp_count, share, first, last, scattered
        ),
        out_shape=jax.ShapeDtypeStruct((share, width), jnp.bfloat16),
        in_specs=[pl.BlockSpec(memory_space=pltpu.SMEM)] * 3
        + [pl.BlockSpec(memory_space=pltpu.VMEM)] * 4,
        out_specs=pl.BlockSpec(memory_space=pltpu.VMEM),
        scratch_shapes=[
            pltpu.VMEM((chunks, rows, heads * HEAD), jnp.bfloat16),
            scratch_block,
            scratch_block,
            scratch_block,
            scratch_block,
            scratch_block,
            scratch_block,
            swap_block,
            swap_block,
            gather_sem,
            gather_sem,
            line_sem,
            line_sem,
            line_sem,
            line_sem,
            swap_sem,
            swap_sem,
            old_block,
            old_block,
            swap_sem,
            swap_sem,
        ],
        compiler_params=pltpu.CompilerParams(
            collective_id=0, has_side_effects=True, vmem_limit_bytes=56 * 2**20
        ),
        cost_estimate=pl.CostEstimate(
            flops=60_000_000_000, bytes_accessed=4 * tokens * depth, transcendentals=0
        ),
    )(perm, place, block, context.reshape(places, share, HEAD), w_out_t, residual, post_gain.reshape(1, -1))
    return jnp.where(tp_index < mine, result, jnp.zeros_like(result))


def per_device(
    x_old, old_blocks, new_blocks, order, pre_gain, post_gain, w_query, w_key, w_value, w_out_t
):
    seq_count = lax.axis_size("seq")
    tp_count = lax.axis_size("tp")
    capacity, quarter = x_old.shape
    width = quarter * tp_count
    tokens = seq_count * capacity // 2
    own = tokens // seq_count
    share = capacity // tp_count
    seq_index = lax.axis_index("seq")
    tp_index = lax.axis_index("tp")
    heads = w_query.shape[1] // HEAD
    kv_heads = w_key.shape[1] // HEAD
    scale = (width // (heads * tp_count)) ** (-0.5)
    if front_fits(seq_count, tp_count, heads, kv_heads, capacity):
        query, both, rows = front_phase(
            x_old, old_blocks, order, pre_gain, w_query, w_key, w_value, seq_count, tp_count, scale
        )
        context = attention(query, both[0], both[1])
        return output_phase(
            context, w_out_t, rows, post_gain, new_blocks, seq_count, tp_count, heads
        )
    old_start = offsets(old_blocks)
    new_start = offsets(new_blocks)
    device_ids = jnp.arange(seq_count, dtype=jnp.int32)

    gathered = lax.all_gather(x_old, "seq", axis=0, tiled=True)

    def stored(row, count):
        row = jnp.minimum(row, tokens - count)
        shard = jnp.sum((old_start <= row).astype(jnp.int32)) - 1
        holder = jnp.sum(jnp.where(order == shard, device_ids, 0))
        begin = jnp.sum(jnp.where(device_ids == shard, old_start, 0))
        return lax.dynamic_slice_in_dim(gathered, holder * capacity + row - begin, count, 0)

    def shift(k):
        return [(i, (i + k) % tp_count) for i in range(tp_count)]

    def by_source(received):
        stack = jnp.stack(received)
        pieces = [
            lax.dynamic_index_in_dim(stack, lax.rem(tp_index - u + tp_count, tp_count), 0, False)
            for u in range(tp_count)
        ]
        return jnp.concatenate(pieces, axis=1)

    mine = jnp.concatenate(
        [stored(seq_index * own + at, BLOCK) for at in range(0, own, BLOCK)], axis=0
    )
    full_rows = by_source(
        [mine] + [lax.ppermute(mine, "tp", shift(k)) for k in range(1, tp_count)]
    )
    my_start = jnp.sum(jnp.where(device_ids == seq_index, new_start, 0))

    def slot_rows(place):
        return stored(my_start + place * share, share)

    residual = by_source(
        [slot_rows(tp_index)]
        + [
            lax.ppermute(slot_rows(lax.rem(tp_index + k, tp_count)), "tp", shift(k))
            for k in range(1, tp_count)
        ]
    )

    weights = lax.all_gather(
        jnp.concatenate([w_query, w_key, w_value], axis=1), "seq", axis=0, tiled=True
    )

    normed = rms_scale(full_rows.astype(jnp.float32), pre_gain).astype(jnp.bfloat16)
    normed, residual = lax.optimization_barrier((normed, residual))
    group = heads // kv_heads
    copies = seq_count // heads
    raw = jnp.dot(normed, weights, preferred_element_type=jnp.float32)

    half = HEAD // 2
    inverse = jnp.exp(jnp.arange(half, dtype=jnp.float32) * (-2.0 * math.log(10000.0) / HEAD))
    places = seq_index * own + jnp.arange(own, dtype=jnp.int32)
    angles = places.astype(jnp.float32)[:, None] * inverse[None, :]
    cosine, sine = jnp.cos(angles), jnp.sin(angles)

    def rotate(at):
        first = raw[:, at * HEAD : at * HEAD + half]
        second = raw[:, at * HEAD + half : (at + 1) * HEAD]
        return jnp.concatenate(
            [first * cosine - second * sine, second * cosine + first * sine], axis=-1
        )

    queries = [(rotate(h) * scale).astype(jnp.bfloat16) for h in range(heads)]
    keys = [rotate(heads + g).astype(jnp.bfloat16) for g in range(kv_heads)]
    values = [
        raw[:, (heads + kv_heads + g) * HEAD : (heads + kv_heads + g + 1) * HEAD].astype(
            jnp.bfloat16
        )
        for g in range(kv_heads)
    ]
    sent = jnp.stack(
        [
            jnp.stack([queries[s // copies], keys[s // copies // group], values[s // copies // group]])
            for s in range(seq_count)
        ]
    )
    came = lax.all_to_all(sent, "seq", 0, 0, tiled=True)
    context = attention(
        came[:, 0].reshape(tokens, HEAD),
        came[:, 1].reshape(tokens, HEAD),
        came[:, 2].reshape(tokens, HEAD),
    )
    return output_phase(
        context, w_out_t, residual, post_gain, new_blocks, seq_count, tp_count, heads
    )


def solution(mesh):
    placed = (
        P("seq", "tp"),
        P(),
        P(),
        P(),
        P(),
        P(),
        P("seq", "tp"),
        P("seq", "tp"),
        P("seq", "tp"),
        P("seq", "tp"),
    )
    return jax.shard_map(
        per_device, mesh=mesh, in_specs=placed, out_specs=P(("seq", "tp"), None), check_vma=False
    )
```

```python
import functools
import math

import jax
import jax.numpy as jnp
import numpy as np
from jax import lax
from jax.experimental import pallas as pl
from jax.experimental.pallas import tpu as pltpu
from jax.sharding import PartitionSpec as P

HEAD = 128
BLOCK = 128
EPS = 1e-06
LAG = 4


def offsets(blocks):
    return (jnp.cumsum(blocks) - blocks) * BLOCK


def rms_scale(values, gain):
    return values * lax.rsqrt(jnp.mean(values * values, axis=-1, keepdims=True) + EPS) * gain


def attention_kernel(rows, span, q_ref, k_ref, v_ref, out_ref):
    first = pl.program_id(0) * rows
    query = q_ref[...]

    def step(at, carry, masked):
        numer, denom = carry
        start = pl.multiple_of(at * span, span)
        score = lax.dot_general(
            query,
            k_ref[pl.ds(start, span), :],
            (((1,), (1,)), ((), ())),
            preferred_element_type=jnp.float32,
        )
        weight = jnp.exp(50.0 * jnp.tanh(score * (1.0 / 50.0)))
        if masked:
            places = first + lax.broadcasted_iota(jnp.int32, weight.shape, 0)
            keys = start + lax.broadcasted_iota(jnp.int32, weight.shape, 1)
            weight = jnp.where(keys <= places, weight, 0.0)
        denom = denom + jnp.sum(weight, axis=1, keepdims=True)
        numer = numer + jnp.dot(
            weight.astype(jnp.bfloat16),
            v_ref[pl.ds(start, span), :],
            preferred_element_type=jnp.float32,
        )
        return numer, denom

    whole = first // span
    state = (jnp.zeros((rows, HEAD), jnp.float32), jnp.zeros((rows, 1), jnp.float32))
    state = lax.fori_loop(0, whole, lambda at, c: step(at, c, False), state)
    numer, denom = step(whole, state, True)
    out_ref[...] = (numer / denom).astype(out_ref.dtype)


def attention(query, key, value):
    tokens = query.shape[0]
    rows, span = 256, 512
    return pl.pallas_call(
        functools.partial(attention_kernel, rows, span),
        grid=(tokens // rows,),
        in_specs=[
            pl.BlockSpec((rows, HEAD), lambda i: (i, 0)),
            pl.BlockSpec((tokens, HEAD), lambda i: (0, 0)),
            pl.BlockSpec((tokens, HEAD), lambda i: (0, 0)),
        ],
        out_specs=pl.BlockSpec((rows, HEAD), lambda i: (i, 0)),
        out_shape=jax.ShapeDtypeStruct((tokens, HEAD), jnp.bfloat16),
        cost_estimate=pl.CostEstimate(
            flops=3 * tokens * tokens * HEAD,
            bytes_accessed=8 * tokens * HEAD,
            transcendentals=tokens * tokens,
        ),
    )(query, key, value)


MESH = pl.DeviceIdType.MESH


def arrangements(seq_count):
    found = []
    for second in range(1, seq_count + 1):
        for third in range(1, second + 1):
            fourth = seq_count - second - third
            if 1 <= fourth <= third:
                found.append((seq_count, second, third, fourth))
    return found


def layer_windows(seq_count, tp_count, per_block):
    first, last = [], []
    for layer in range(tp_count):
        starts, ends = [], []
        for counts in arrangements(seq_count):
            begin = sum(counts[u // per_block] for u in range(layer))
            starts.append(begin)
            ends.append(begin + counts[layer // per_block])
        first.append(min(starts))
        last.append(max(ends))
    return first, last


def pick(index, values):
    result = jnp.int32(values[0])
    for k in range(1, len(values)):
        result = jnp.where(index == k, jnp.int32(values[k]), result)
    return result


def flipped(index, mask):
    result = index
    bit = 1
    while bit <= mask:
        if mask & bit:
            result = result + bit - 2 * bit * lax.rem(index // bit, 2)
        bit *= 2
    return result


def output_kernel(
    heads,
    copies,
    seq_count,
    tp_count,
    share,
    first,
    last,
    scattered,
    perm_ref,
    place_ref,
    block_ref,
    context_ref,
    weight_ref,
    residual_ref,
    gain_ref,
    out_ref,
    full,
    partial,
    left_in,
    right_in,
    left_out,
    right_out,
    total,
    sent,
    came,
    gather_send,
    gather_recv,
    left_send,
    left_recv,
    right_send,
    right_recv,
    swap_send,
    swap_recv,
    old_sent,
    old_came,
    old_send,
    old_recv,
):
    seq_index = lax.axis_index("seq")
    tp_index = lax.axis_index("tp")
    places = partial.shape[0]
    depth = weight_ref.shape[0]
    head = seq_index // copies
    chunks = full.shape[0]
    per_chunk = places // chunks
    chunk_rows = full.shape[1]

    barrier = pltpu.get_barrier_semaphore()
    for k in range(1, seq_count):
        pl.semaphore_signal(
            barrier,
            inc=1,
            device_id=(lax.rem(seq_index + k, seq_count), tp_index),
            device_id_type=MESH,
        )

    @pl.when(tp_index > 0)
    def _():
        pl.semaphore_signal(
            barrier, inc=1, device_id=(seq_index, tp_index - 1), device_id_type=MESH
        )

    @pl.when(tp_index < tp_count - 1)
    def _():
        pl.semaphore_signal(
            barrier, inc=1, device_id=(seq_index, tp_index + 1), device_id_type=MESH
        )

    own_columns = pl.ds(pl.multiple_of(head * HEAD, HEAD), HEAD)
    for chunk in range(chunks):
        for at in range(per_chunk):
            full[chunk, at * share : (at + 1) * share, own_columns] = context_ref[
                perm_ref[chunk * per_chunk + at]
            ]

    neighbours = jnp.where(tp_index > 0, 1, 0) + jnp.where(tp_index < tp_count - 1, 1, 0)
    pl.semaphore_wait(barrier, seq_count - 1 + neighbours)

    bits = heads.bit_length() - 1
    order = list(range(chunks))[::-1]

    def dims(chunk):
        outer = list(range(1, bits))
        return (outer[::-1] if chunk % 2 else outer) + ([0] if bits > 0 else [])

    def gather_copy(chunk, bit, combo, to_me):
        slot = flipped(head, (combo ^ (1 << bit)) if to_me else combo)
        columns = pl.ds(pl.multiple_of(slot * HEAD, HEAD), HEAD)
        partner = flipped(seq_index, copies << bit)
        view = full.at[chunk, :, columns]
        return pltpu.make_async_remote_copy(
            src_ref=view,
            dst_ref=view,
            send_sem=gather_send.at[chunk, bit, combo],
            recv_sem=gather_recv.at[chunk, bit, combo],
            device_id=(partner, tp_index),
            device_id_type=MESH,
        )

    def steps(chunk):
        held = [0]
        for bit in dims(chunk):
            yield bit, list(held)
            held = held + [c ^ (1 << bit) for c in held]

    def offer(at):
        if at < chunks:
            for bit, _ in steps(order[at]):
                gather_copy(order[at], bit, 0, False).start()

    offer(0)
    total[...] = jnp.zeros_like(total)

    def relay(at):
        chunk = order[at]
        stages = list(steps(chunk))
        for level, (bit, held) in enumerate(stages):
            for combo in held:
                gather_copy(chunk, bit, combo, True).wait_recv()
                for later, _ in stages[level + 1 :]:
                    gather_copy(chunk, later, combo ^ (1 << bit), False).start()
            if level == 0:
                offer(at + 1)

    def multiply(chunk):
        product = lax.dot_general(
            full[chunk],
            weight_ref[...],
            (((1,), (1,)), ((), ())),
            preferred_element_type=jnp.float32,
        ).astype(jnp.bfloat16)
        for at in range(per_chunk):
            partial[chunk * per_chunk + at] = product[at * share : (at + 1) * share]

    left_has = jnp.where(tp_index < tp_count - 1, pick(tp_index, last), 0)
    left_gives = pick(tp_index, [0] + last[:-1])
    right_has = jnp.where(tp_index > 0, pick(tp_index, first), places)
    right_gives = pick(tp_index, first[1:] + [places])

    def line_copy(place, source, landing, send, recv, step):
        return pltpu.make_async_remote_copy(
            src_ref=source.at[place],
            dst_ref=landing.at[place],
            send_sem=send.at[place],
            recv_sem=recv.at[place],
            device_id=(seq_index, tp_index + step),
            device_id_type=MESH,
        )

    def flow(place, has, gives, source, landing, send, recv, step):
        @pl.when(has)
        def _():
            line_copy(place, source, landing, send, recv, step).wait_recv()

        @pl.when(jnp.logical_and(has, gives))
        def _():
            source[place] = (
                partial[place].astype(jnp.float32) + landing[place].astype(jnp.float32)
            ).astype(jnp.bfloat16)

        @pl.when(jnp.logical_and(jnp.logical_not(has), gives))
        def _():
            source[place] = partial[place]

        @pl.when(gives)
        def _():
            line_copy(place, source, landing, send, recv, step).start()

    def swap_copy(other, mine, at):
        return pltpu.make_async_remote_copy(
            src_ref=sent.at[other],
            dst_ref=came.at[mine],
            send_sem=swap_send.at[at],
            recv_sem=swap_recv.at[at],
            device_id=(other, tp_index),
            device_id_type=MESH,
        )

    def line_step(at, carry):
        passed = at - LAG * (tp_count - 1 - tp_index)
        place = places - 1 - passed
        valid = jnp.logical_and(passed >= 0, passed < places)
        has = jnp.logical_and(valid, place < left_has)
        gives = jnp.logical_and(valid, place < left_gives)
        flow(place, has, gives, left_out, left_in, left_send, left_recv, -1)
        ends = jnp.logical_and(
            jnp.logical_and(valid, tp_index == 0), place < seq_count
        )

        @pl.when(ends)
        def _():
            sent[place] = (
                partial[place].astype(jnp.float32) + left_in[place].astype(jnp.float32)
            ).astype(jnp.bfloat16)

            @pl.when(place == seq_index)
            def _():
                came[place] = sent[place]

            @pl.when(place != seq_index)
            def _():
                swap_copy(
                    place, seq_index, lax.rem(place + seq_count - seq_index, seq_count)
                ).start()

        passed = at - LAG * tp_index
        place = places - 1 - passed
        valid = jnp.logical_and(passed >= 0, passed < places)
        has = jnp.logical_and(valid, place >= right_has)
        gives = jnp.logical_and(valid, place >= right_gives)
        flow(place, has, gives, right_out, right_in, right_send, right_recv, 1)
        return carry

    for at, chunk in enumerate(order):
        relay(at)
        multiply(chunk)
        lax.fori_loop(at * per_chunk, (at + 1) * per_chunk, line_step, 0)

    def old_copy(other, mine, at):
        return pltpu.make_async_remote_copy(
            src_ref=old_sent.at[other],
            dst_ref=old_came.at[mine],
            send_sem=old_send.at[at],
            recv_sem=old_recv.at[at],
            device_id=(other, tp_index),
            device_id_type=MESH,
        )

    if scattered:
        for j in range(seq_count):
            old_sent[j] = residual_ref[block_ref[j]]
        for k in range(1, seq_count):
            old_copy(lax.rem(seq_index + k, seq_count), seq_index, k).start()
        old_came[seq_index] = old_sent[seq_index]
    lax.fori_loop(places, places + LAG * (tp_count - 1), line_step, 0)

    def sum_step(place, carry):
        value = partial[place].astype(jnp.float32) + right_in[place].astype(jnp.float32)

        @pl.when(place < left_has)
        def _():
            total[place] = (value + left_in[place].astype(jnp.float32)).astype(jnp.bfloat16)

        @pl.when(place >= left_has)
        def _():
            total[place] = value.astype(jnp.bfloat16)

        return carry

    @pl.when(tp_index > 0)
    def _():
        lax.fori_loop(pick(tp_index, first), pick(tp_index, last), sum_step, 0)
        for j in range(seq_count):
            sent[j] = total[place_ref[j]]
        for k in range(1, seq_count):
            swap_copy(lax.rem(seq_index + k, seq_count), seq_index, k).start()
        came[seq_index] = sent[seq_index]

    for k in range(1, seq_count):
        swap_copy(
            lax.rem(seq_index + k, seq_count),
            lax.rem(seq_index + seq_count - k, seq_count),
            k,
        ).wait_recv()

    if scattered:
        for k in range(1, seq_count):
            old_copy(
                lax.rem(seq_index + k, seq_count),
                lax.rem(seq_index + seq_count - k, seq_count),
                k,
            ).wait_recv()
    square = jnp.zeros((share, 1), jnp.float32)
    for s in range(seq_count):
        piece = came[s].astype(jnp.float32)
        square = square + jnp.sum(piece * piece, axis=1, keepdims=True)
    factor = lax.rsqrt(square * (1.0 / (depth * seq_count)) + EPS)
    for s in range(seq_count // 2):
        piece = jnp.concatenate([came[2 * s], came[2 * s + 1]], axis=1).astype(jnp.float32)
        columns = slice(2 * s * depth, (2 * s + 2) * depth)
        if scattered:
            old = jnp.concatenate([old_came[2 * s], old_came[2 * s + 1]], axis=0)
        else:
            old = residual_ref[:, columns]
        value = old.astype(jnp.float32) + (
            piece * factor * gain_ref[:, columns]
        )
        out_ref[:, columns] = value.astype(jnp.bfloat16)

    for k in range(1, seq_count):
        swap_copy(lax.rem(seq_index + k, seq_count), seq_index, k).wait_send()
    if scattered:
        for k in range(1, seq_count):
            old_copy(lax.rem(seq_index + k, seq_count), seq_index, k).wait_send()
    for chunk in range(chunks):
        for bit, held in steps(chunk):
            for combo in held:
                gather_copy(chunk, bit, combo, False).wait_send()

    def drain(place, carry):
        @pl.when(place < left_gives)
        def _():
            line_copy(place, left_out, left_in, left_send, left_recv, -1).wait_send()

        @pl.when(place >= right_gives)
        def _():
            line_copy(place, right_out, right_in, right_send, right_recv, 1).wait_send()

        return carry

    lax.fori_loop(0, places, drain, 0)


def front_kernel(
    seq_count,
    tp_count,
    group,
    scale,
    blocks_ref,
    order_ref,
    x_ref,
    gain_ref,
    query_ref,
    key_ref,
    value_ref,
    angle_ref,
    context_out,
    x_out,
    q_buf,
    kv_buf,
    near,
    send_a,
    send_b,
    far,
    line,
    twin,
    weight,
    normed,
    scale_row,
    scale_all,
    scale_column,
    first_out,
    first_in,
    second_out,
    second_in,
    kept,
    core_sem,
    weight_sem,
    stage_sem,
    line_send,
    line_recv,
    plane_send,
    plane_recv,
    twin_sem,
    stat_sem,
    factor_sem,
    first_sem,
    second_sem,
    kv_sem,
):
    seq_index = lax.axis_index("seq")
    tp_index = lax.axis_index("tp")
    chip = seq_index // 2
    core = lax.rem(seq_index, 2)
    partner = seq_index + 1 - 2 * core
    slots = x_ref.shape[0]
    chips = seq_count // 2
    each = line.shape[1]
    half = line.shape[2]
    quarter = line.shape[3]
    depth = query_ref.shape[0]
    pair = 2 * HEAD

    barrier = pltpu.get_barrier_semaphore()
    for k in range(1, seq_count):
        other = lax.rem(seq_index + k, seq_count)
        pl.semaphore_signal(barrier, inc=1, device_id=(other, tp_index), device_id_type=MESH)
    for k in range(1, tp_count):
        other = lax.rem(tp_index + k, tp_count)
        pl.semaphore_signal(barrier, inc=1, device_id=(seq_index, other), device_id_type=MESH)

    def remote(source, target, sems, at, seq, tp):
        return pltpu.make_async_remote_copy(
            src_ref=source,
            dst_ref=target,
            send_sem=sems[0].at[at],
            recv_sem=sems[1].at[at],
            device_id=(seq, tp),
            device_id_type=MESH,
        )

    core_sems = (core_sem.at[0], core_sem.at[1])

    def swap_slots(holder):
        return remote(
            x_ref.at[:, 1 - core],
            near.at[pl.ds(slots * holder, slots)],
            core_sems,
            0,
            partner,
            tp_index,
        )

    def lanes(head, count=1):
        return pl.ds(pl.multiple_of(head * HEAD, HEAD), count * HEAD)

    def weight_copy(source, column, target, at, holder):
        return remote(
            source.at[:, lanes(column)],
            weight.at[pl.ds(pl.multiple_of(holder * depth, depth), depth), lanes(target)],
            (weight_sem.at[0], weight_sem.at[1]),
            at,
            partner,
            tp_index,
        )

    pl.semaphore_wait(barrier, seq_count - 1 + tp_count - 1)
    swap_slots(core).start()
    for slot in range(slots):
        near[slots * core + slot] = x_ref[slot, core]

    starts, counts, holders = [], [], []
    begin = jnp.int32(0)
    for k in range(seq_count):
        starts.append(begin)
        counts.append(blocks_ref[k])
        begin = begin + blocks_ref[k]
        holder = jnp.int32(0)
        for place in range(1, seq_count):
            holder = holder + jnp.where(order_ref[place] == k, jnp.int32(place), jnp.int32(0))
        holders.append(holder)

    def found(block):
        at = jnp.int32(0)
        for k in range(seq_count):
            inside = jnp.logical_and(starts[k] <= block, block < starts[k] + counts[k])
            at = at + jnp.where(inside, holders[k] * slots + block - starts[k], jnp.int32(0))
        return at // (2 * slots), lax.rem(at, 2 * slots)

    first_chip = jnp.where(core == 0, flipped(chip, 1), flipped(chip, 2))
    second_chip = jnp.where(core == 0, flipped(chip, 2), flipped(chip, 1))
    cross_chip = flipped(chip, 3)
    swap_slots(1 - core).wait_recv()

    stage_sems = (stage_sem.at[0], stage_sem.at[1])
    table_a = []
    for at in range(2 * each):
        target = first_chip if at < each else cross_chip
        owner, index = found(chips * (at % each) + target)
        table_a.append(jnp.where(owner == chip, index, 0))
    across_first = list(range(each, 2 * each)) + list(range(each))
    for at in across_first:
        send_a[at] = near[table_a[at]]
        remote(
            send_a.at[at], far.at[at], stage_sems, at, 2 * first_chip + core, tp_index
        ).start()

    for c in range(chips):
        weight_copy(query_ref, 2 * c + 1 - core, 2 * c, 2 * c, core).start()

        @pl.when(core == 0)
        def _():
            weight_copy(value_ref, c, 2 * c + 1, 2 * c + 1, core).start()

        @pl.when(core == 1)
        def _():
            weight_copy(key_ref, c, 2 * c + 1, 2 * c + 1, core).start()

    own_rows = pl.ds(pl.multiple_of(core * depth, depth), depth)
    for c in range(chips):
        weight[own_rows, pl.ds(2 * c * HEAD, HEAD)] = query_ref[:, lanes(2 * c + core)]

        @pl.when(core == 0)
        def _():
            weight[own_rows, pl.ds((2 * c + 1) * HEAD, HEAD)] = key_ref[
                :, pl.ds(c * HEAD, HEAD)
            ]

        @pl.when(core == 1)
        def _():
            weight[own_rows, pl.ds((2 * c + 1) * HEAD, HEAD)] = value_ref[
                :, pl.ds(c * HEAD, HEAD)
            ]

    def arrive_a(at):
        remote(
            send_a.at[at], far.at[at], stage_sems, at, 2 * first_chip + core, tp_index
        ).wait_recv()

    both = 2 * slots
    for at in range(each, 2 * each):
        arrive_a(at)
        near[both + at] = far[at]
    for at in range(each):
        owner, index = found(chips * at + second_chip)
        send_b[at] = near[jnp.where(owner == chip, index, both + each + at)]
        remote(
            send_b.at[at],
            far.at[2 * each + at],
            stage_sems,
            2 * each + at,
            2 * second_chip + core,
            tp_index,
        ).start()
    for at in range(each):
        arrive_a(at)
        near[both + at] = far[at]
    for at in range(each):
        owner, index = found(chips * at + chip)
        near[both + 2 * each + at] = near[jnp.where(owner == chip, index, both + at)]
    for at in range(each):
        remote(
            send_b.at[at],
            far.at[2 * each + at],
            stage_sems,
            2 * each + at,
            2 * second_chip + core,
            tp_index,
        ).wait_recv()
        near[both + 3 * each + at] = far[2 * each + at]
    for at in range(each):
        owner, _ = found(chips * at + chip)
        local = jnp.logical_or(owner == chip, owner == first_chip)
        line[tp_index, at] = near[
            jnp.where(local, both + 2 * each + at, both + 3 * each + at)
        ]

    def line_copy(layer, at, step):
        view = line.at[layer, at]
        return pltpu.make_async_remote_copy(
            src_ref=view,
            dst_ref=view,
            send_sem=line_send.at[(step + 1) // 2, layer, at],
            recv_sem=line_recv.at[layer, at],
            device_id=(seq_index, tp_index + step),
            device_id_type=MESH,
        )

    def plane_copy(layer, at, holder):
        return pltpu.make_async_remote_copy(
            src_ref=line.at[layer, at],
            dst_ref=x_out.at[chips * at + holder],
            send_sem=plane_send.at[layer, at],
            recv_sem=plane_recv.at[chips * at + holder],
            device_id=(2 * layer + core, tp_index),
            device_id_type=MESH,
        )

    def twin_copy(block):
        return remote(
            x_out.at[block],
            twin.at[block],
            (twin_sem.at[0], twin_sem.at[1]),
            block,
            partner,
            tp_index,
        )

    def guarded(condition, action):
        @pl.when(condition)
        def _():
            action()

    def forward(layer, at):
        @pl.when(layer == chip)
        def _():
            x_out[chips * at + chip] = line[layer, at]

        @pl.when(layer != chip)
        def _():
            plane_copy(layer, at, chip).start()

    def own_step(at):
        guarded(tp_index > 0, lambda: line_copy(tp_index, at, -1).start())
        guarded(tp_index < tp_count - 1, lambda: line_copy(tp_index, at, 1).start())
        forward(tp_index, at)

    def hop_step(at, distance):
        @pl.when(tp_index >= distance)
        def _():
            layer = tp_index - distance
            line_copy(layer, at, 1).wait_recv()
            guarded(tp_index < tp_count - 1, lambda: line_copy(layer, at, 1).start())
            forward(layer, at)

        @pl.when(tp_index + distance < tp_count)
        def _():
            layer = tp_index + distance
            line_copy(layer, at, -1).wait_recv()
            guarded(tp_index > 0, lambda: line_copy(layer, at, -1).start())
            forward(layer, at)

    def plane_step(at):
        for c in range(chips):

            @pl.when(chip != c)
            def _():
                plane_copy(chip, at, c).wait_recv()

        for c in range(chips):
            twin_copy(chips * at + c).start()

    tiles = quarter // HEAD
    gain_at = pl.multiple_of(chip * quarter, HEAD)

    def normalize(source, block, holder, target):
        rows = pl.ds(pl.multiple_of((block // chips) * half, half), half)
        factor = scale_column[holder, rows, :]
        for tile in range(tiles):
            columns = slice(tile * HEAD, (tile + 1) * HEAD)
            values = source[block, :, columns].astype(jnp.float32)
            gains = gain_ref[:, pl.ds(pl.multiple_of(gain_at + tile * HEAD, HEAD), HEAD)]
            normed[target[0], target[1], target[2], :, columns] = (
                values * factor * gains
            ).astype(jnp.bfloat16)

    bits = (1, 2)

    def first_copy(at, side):
        bit = bits[side]
        return pltpu.make_async_remote_copy(
            src_ref=first_out.at[at, side],
            dst_ref=first_in.at[at, side],
            send_sem=first_sem.at[0, at, side],
            recv_sem=first_sem.at[1, at, side],
            device_id=(2 * flipped(chip, bit) + core, tp_index),
            device_id_type=MESH,
        )

    def second_copy(at, side):
        bit = bits[1 - side]
        return pltpu.make_async_remote_copy(
            src_ref=second_out.at[at, side],
            dst_ref=second_in.at[at, side],
            send_sem=second_sem.at[0, at, side],
            recv_sem=second_sem.at[1, at, side],
            device_id=(2 * flipped(chip, bit) + core, tp_index),
            device_id_type=MESH,
        )

    def multiply_step(at):
        for side in range(2):
            for u in range(2):
                c = 2 * side + u
                block = chips * at + c
                twin_copy(block).wait_recv()
                normalize(x_out, block, 2 * c + core, (side, u, core))
                normalize(twin, block, 2 * c + 1 - core, (side, u, 1 - core))
            rows = normed[side].reshape(4 * half, quarter)

            def part(mask):
                target = flipped(chip, mask)
                return jnp.dot(
                    rows,
                    weight[:, lanes(2 * target, 2)],
                    preferred_element_type=jnp.float32,
                )

            first, second = bits[side], bits[1 - side]
            first_out[at, side, 0] = part(first).astype(jnp.bfloat16)
            first_out[at, side, 1] = part(3).astype(jnp.bfloat16)
            first_copy(at, side).start()
            kept[at, side, 0] = part(0)
            kept[at, side, 1] = part(second)

    def add_step(at):
        for side in range(2):
            first_copy(at, side).wait_recv()
            second_out[at, side] = (
                kept[at, side, 1] + first_in[at, side, 1].astype(jnp.float32)
            ).astype(jnp.bfloat16)
            second_copy(at, side).start()

    def kv_copy(kind, block):
        rows = pl.ds(pl.multiple_of(block * BLOCK, BLOCK), BLOCK)
        view = kv_buf.at[kind, rows, :]
        return remote(
            view, view, (kv_sem.at[0], kv_sem.at[1]), block, partner, tp_index
        )

    lane = lax.broadcasted_iota(jnp.int32, (BLOCK, HEAD), 1)

    def turned(values, rows):
        angles = angle_ref[rows, :]
        swapped = pltpu.roll(angles, HEAD // 2, 1)
        low = lane < HEAD // 2
        cosine = jnp.where(low, angles, swapped)
        sine = jnp.where(low, -swapped, angles)
        return values * cosine + pltpu.roll(values, HEAD // 2, 1) * sine

    def finish_step(at):
        for side in range(2):
            second_copy(at, side).wait_recv()
            for u in range(2):
                block = chips * at + 2 * side + u
                part = slice(u * BLOCK, (u + 1) * BLOCK)
                value = (
                    kept[at, side, 0, part]
                    + first_in[at, side, 0, part].astype(jnp.float32)
                    + second_in[at, side, part].astype(jnp.float32)
                )
                rows = pl.ds(pl.multiple_of(block * BLOCK, BLOCK), BLOCK)
                q_buf[rows, :] = (turned(value[:, :HEAD], rows) * scale).astype(jnp.bfloat16)

                @pl.when(core == 0)
                def _():
                    kv_buf[0, rows, :] = turned(value[:, HEAD:], rows).astype(jnp.bfloat16)

                @pl.when(core == 1)
                def _():
                    kv_buf[1, rows, :] = value[:, HEAD:].astype(jnp.bfloat16)

                kv_copy(core, block).start()

    span = chips * BLOCK
    sub = span // 2
    mask = lax.broadcasted_iota(jnp.int32, (sub, sub), 1) <= lax.broadcasted_iota(
        jnp.int32, (sub, sub), 0
    )

    def attend_step(at):
        for c in range(chips):
            kv_copy(1 - core, chips * at + c).wait_recv()

        def attend(query, start, count, carry, masked):
            keys = pl.ds(pl.multiple_of(start, sub), count)
            score = lax.dot_general(
                query,
                kv_buf[0, keys, :],
                (((1,), (1,)), ((), ())),
                preferred_element_type=jnp.float32,
            )
            part = jnp.exp2((50.0 / math.log(2.0)) * jnp.tanh(score * (1.0 / 50.0)))
            if masked:
                part = jnp.where(mask, part, 0.0)
            numer, denom = carry
            denom = denom + jnp.sum(part, axis=1, keepdims=True)
            numer = numer + jnp.dot(
                part.astype(jnp.bfloat16), kv_buf[1, keys, :], preferred_element_type=jnp.float32
            )
            return numer, denom

        for piece in range(2):
            begin = at * span + piece * sub
            rows = pl.ds(pl.multiple_of(begin, sub), sub)
            query = q_buf[rows, :]
            state = (jnp.zeros((sub, HEAD), jnp.float32), jnp.zeros((sub, 1), jnp.float32))
            state = lax.fori_loop(
                0, at, lambda n, carry: attend(query, n * span, span, carry, False), state
            )
            if piece:
                state = attend(query, at * span, sub, state, False)
            numer, denom = attend(query, begin, sub, state, True)
            context_out[rows, :] = (numer / denom).astype(jnp.bfloat16)

    def stat_copy(layer_from, layer_to):
        return pltpu.make_async_remote_copy(
            src_ref=scale_row.at[layer_from],
            dst_ref=scale_row.at[layer_from],
            send_sem=stat_sem.at[0, layer_to],
            recv_sem=stat_sem.at[1, layer_from],
            device_id=(seq_index, layer_to),
            device_id_type=MESH,
        )

    def factor_copy(holder, other):
        return pltpu.make_async_remote_copy(
            src_ref=scale_all.at[holder],
            dst_ref=scale_all.at[holder],
            send_sem=factor_sem.at[0, other],
            recv_sem=factor_sem.at[1, holder],
            device_id=(other, tp_index),
            device_id_type=MESH,
        )

    own_step(0)
    squares = []
    for at in range(each):
        values = line[tp_index, at].astype(jnp.float32)
        squares.append(jnp.sum(values * values, axis=1, keepdims=True))
    column = jnp.broadcast_to(jnp.concatenate(squares, axis=0), (each * half, HEAD))
    scale_row[tp_index] = jnp.transpose(column)[:8, :]
    for k in range(1, tp_count):
        stat_copy(tp_index, lax.rem(tp_index + k, tp_count)).start()
    for c in range(2 * chips):
        weight_copy(query_ref, 0, 0, c, 1 - core).wait_recv()
    for k in range(1, tp_count):
        other = lax.rem(tp_index + k, tp_count)
        stat_copy(other, tp_index).wait_recv()
    square = scale_row[0]
    for k in range(1, tp_count):
        square = square + scale_row[k]
    scale_all[seq_index] = lax.rsqrt(square * (1.0 / (quarter * tp_count)) + EPS)
    for k in range(1, seq_count):
        factor_copy(seq_index, lax.rem(seq_index + k, seq_count)).start()

    def steps(i, carry):
        for lag, action in (
            (0, lambda at: guarded(at > 0, lambda: own_step(at))),
            (1, lambda at: hop_step(at, 1)),
            (2, lambda at: hop_step(at, 2)),
            (3, lambda at: hop_step(at, 3)),
            (4, plane_step),
            (5, multiply_step),
            (6, add_step),
            (7, finish_step),
            (8, attend_step),
        ):
            at = i - lag

            @pl.when(jnp.logical_and(at >= 0, at < each))
            def _():
                action(at)

        return carry

    lax.fori_loop(0, 5, steps, 0)
    for k in range(1, seq_count):
        other = lax.rem(seq_index + k, seq_count)
        factor_copy(other, seq_index).wait_recv()
    for s in range(seq_count):
        scale_column[s] = jnp.transpose(
            jnp.broadcast_to(scale_all[s, :1, :], (HEAD, each * half))
        )
    lax.fori_loop(5, each + 8, steps, 0)

    swap_slots(core).wait_send()
    for c in range(2 * chips):
        weight_copy(query_ref, 0, 0, c, core).wait_send()
    for at in range(2 * each):
        remote(
            send_a.at[at], far.at[at], stage_sems, at, 2 * first_chip + core, tp_index
        ).wait_send()
    for at in range(each):
        remote(
            send_b.at[at],
            far.at[2 * each + at],
            stage_sems,
            2 * each + at,
            2 * second_chip + core,
            tp_index,
        ).wait_send()
    for k in range(1, tp_count):
        stat_copy(tp_index, lax.rem(tp_index + k, tp_count)).wait_send()
    for k in range(1, seq_count):
        factor_copy(seq_index, lax.rem(seq_index + k, seq_count)).wait_send()

    def drain(at, carry):
        for layer in range(tp_count):
            right = jnp.logical_and(tp_index >= layer, tp_index < tp_count - 1)
            guarded(right, lambda: line_copy(layer, at, 1).wait_send())
            left = jnp.logical_and(tp_index <= layer, tp_index > 0)
            guarded(left, lambda: line_copy(layer, at, -1).wait_send())
            guarded(chip != layer, lambda: plane_copy(layer, at, chip).wait_send())
        for side in range(2):
            first_copy(at, side).wait_send()
            second_copy(at, side).wait_send()
        for c in range(chips):
            twin_copy(chips * at + c).wait_send()
            kv_copy(core, chips * at + c).wait_send()
        return carry

    lax.fori_loop(0, each, drain, 0)


def front_fits(seq_count, tp_count, heads, kv_heads, capacity):
    return (
        heads == seq_count == 8
        and 2 * kv_heads == heads
        and tp_count == 4
        and capacity == 4 * BLOCK
    )


def front_phase(
    x_old, old_blocks, order, pre_gain, w_query, w_key, w_value, seq_count, tp_count, scale
):
    capacity, quarter = x_old.shape
    depth = w_query.shape[0]
    slots = capacity // BLOCK
    half = BLOCK // 2
    tokens = seq_count * capacity // 2
    chips = seq_count // 2
    each = tokens // BLOCK // chips
    group = w_query.shape[1] // w_key.shape[1]
    angles = (
        np.arange(tokens, dtype=np.float32)[:, None]
        * np.exp(
            np.arange(HEAD // 2, dtype=np.float32) * np.float32(-2.0 * math.log(10000.0) / HEAD)
        )[None, :]
    )
    table = np.concatenate([np.cos(angles), np.sin(angles)], axis=1).astype(np.float32)
    bf16, f32 = jnp.bfloat16, jnp.float32
    piece = (half, quarter)
    dma = pltpu.SemaphoreType.DMA
    vmem = pl.BlockSpec(memory_space=pltpu.VMEM)
    smem = pl.BlockSpec(memory_space=pltpu.SMEM)
    square = (2 * BLOCK, 2 * HEAD)
    return pl.pallas_call(
        functools.partial(front_kernel, seq_count, tp_count, group, scale),
        out_shape=(
            jax.ShapeDtypeStruct((tokens, HEAD), bf16),
            jax.ShapeDtypeStruct((each * chips,) + piece, bf16),
        ),
        in_specs=[smem] * 2 + [vmem] * 6,
        out_specs=(vmem, vmem),
        scratch_shapes=[
            pltpu.VMEM((tokens, HEAD), bf16),
            pltpu.VMEM((2, tokens, HEAD), bf16),
            pltpu.VMEM((2 * slots + 4 * each,) + piece, bf16),
            pltpu.VMEM((2 * each,) + piece, bf16),
            pltpu.VMEM((each,) + piece, bf16),
            pltpu.VMEM((3 * each,) + piece, bf16),
            pltpu.VMEM((tp_count, each) + piece, bf16),
            pltpu.VMEM((each * chips,) + piece, bf16),
            pltpu.VMEM((2 * depth, 2 * chips * HEAD), bf16),
            pltpu.VMEM((2, 2, 2) + piece, bf16),
            pltpu.VMEM((tp_count, 8, each * half), f32),
            pltpu.VMEM((seq_count, 8, each * half), f32),
            pltpu.VMEM((seq_count, each * half, HEAD), f32),
            pltpu.VMEM((each, 2, 2) + square, bf16),
            pltpu.VMEM((each, 2, 2) + square, bf16),
            pltpu.VMEM((each, 2) + square, bf16),
            pltpu.VMEM((each, 2) + square, bf16),
            pltpu.VMEM((each, 2, 2) + square, f32),
            dma((2, 1)),
            dma((2, 2 * chips)),
            dma((2, 3 * each)),
            dma((2, tp_count, each)),
            dma((tp_count, each)),
            dma((tp_count, each)),
            dma((each * chips,)),
            dma((2, each * chips)),
            dma((2, tp_count)),
            dma((2, seq_count)),
            dma((2, each, 2)),
            dma((2, each, 2)),
            dma((2, each * chips)),
        ],
        compiler_params=pltpu.CompilerParams(
            collective_id=1, has_side_effects=True, vmem_limit_bytes=60 * 2**20
        ),
        cost_estimate=pl.CostEstimate(
            flops=60_000_000_000, bytes_accessed=8 * tokens * depth, transcendentals=0
        ),
    )(
        old_blocks,
        order,
        x_old.reshape(slots, 2, half, quarter),
        pre_gain.reshape(1, -1),
        w_query,
        w_key,
        w_value,
        jnp.asarray(table),
    )


def output_phase(context, w_out_t, residual, post_gain, new_blocks, seq_count, tp_count, heads):
    tokens = context.shape[0]
    depth = w_out_t.shape[0]
    width = depth * seq_count
    share = 2 * tokens // (seq_count * tp_count)
    scattered = residual.ndim == 3
    places = tokens // share
    per_block = BLOCK // share
    copies = seq_count // heads
    bits = heads.bit_length() - 1
    first, last = layer_windows(seq_count, tp_count, per_block)
    seq_index = lax.axis_index("seq")
    tp_index = lax.axis_index("tp")
    blocks = new_blocks * per_block
    new_start = jnp.sum(
        jnp.where(
            jnp.arange(seq_count)[None, :] < jnp.arange(seq_count)[:, None], blocks[None, :], 0
        ),
        axis=1,
    )
    slots = jnp.arange(tp_count * seq_count, dtype=jnp.int32)
    layer = jnp.arange(tp_count, dtype=jnp.int32)[:, None]
    valid = (blocks[None, :] > layer).astype(jnp.int32).reshape(-1)
    source = (new_start[None, :] + layer).reshape(-1)
    rank = jnp.sum(jnp.where(slots[None, :] < slots[:, None], valid[None, :], 0), axis=1)
    perm = jnp.sum(
        jnp.where(
            (jnp.arange(places)[:, None] == rank[None, :]) & (valid[None, :] > 0),
            source[None, :],
            0,
        ),
        axis=1,
    ).astype(jnp.int32)
    in_layer = (jnp.arange(tp_count) == tp_index)[:, None]
    place = jnp.sum(jnp.where(in_layer, rank.reshape(tp_count, seq_count), 0), axis=0)
    place = jnp.minimum(place, places - 1).astype(jnp.int32)
    mine = jnp.sum(jnp.where(jnp.arange(seq_count) == seq_index, blocks, 0))
    block = jnp.minimum((new_start + tp_index) // per_block, tokens // BLOCK - 1).astype(jnp.int32)
    piece = residual.shape[1:] if scattered else (8, HEAD)
    old_block = pltpu.VMEM((seq_count,) + piece, jnp.bfloat16)
    chunks = 4
    rows = tokens // chunks
    scratch_block = pltpu.VMEM((places, share, depth), jnp.bfloat16)
    swap_block = pltpu.VMEM((seq_count, share, depth), jnp.bfloat16)
    line_sem = pltpu.SemaphoreType.DMA((places,))
    gather_sem = pltpu.SemaphoreType.DMA((chunks, bits, heads))
    swap_sem = pltpu.SemaphoreType.DMA((seq_count,))
    result = pl.pallas_call(
        functools.partial(
            output_kernel, heads, copies, seq_count, tp_count, share, first, last, scattered
        ),
        out_shape=jax.ShapeDtypeStruct((share, width), jnp.bfloat16),
        in_specs=[pl.BlockSpec(memory_space=pltpu.SMEM)] * 3
        + [pl.BlockSpec(memory_space=pltpu.VMEM)] * 4,
        out_specs=pl.BlockSpec(memory_space=pltpu.VMEM),
        scratch_shapes=[
            pltpu.VMEM((chunks, rows, heads * HEAD), jnp.bfloat16),
            scratch_block,
            scratch_block,
            scratch_block,
            scratch_block,
            scratch_block,
            scratch_block,
            swap_block,
            swap_block,
            gather_sem,
            gather_sem,
            line_sem,
            line_sem,
            line_sem,
            line_sem,
            swap_sem,
            swap_sem,
            old_block,
            old_block,
            swap_sem,
            swap_sem,
        ],
        compiler_params=pltpu.CompilerParams(
            collective_id=0, has_side_effects=True, vmem_limit_bytes=56 * 2**20
        ),
        cost_estimate=pl.CostEstimate(
            flops=60_000_000_000, bytes_accessed=4 * tokens * depth, transcendentals=0
        ),
    )(perm, place, block, context.reshape(places, share, HEAD), w_out_t, residual, post_gain.reshape(1, -1))
    return jnp.where(tp_index < mine, result, jnp.zeros_like(result))


def per_device(
    x_old, old_blocks, new_blocks, order, pre_gain, post_gain, w_query, w_key, w_value, w_out_t
):
    seq_count = lax.axis_size("seq")
    tp_count = lax.axis_size("tp")
    capacity, quarter = x_old.shape
    width = quarter * tp_count
    tokens = seq_count * capacity // 2
    own = tokens // seq_count
    share = capacity // tp_count
    seq_index = lax.axis_index("seq")
    tp_index = lax.axis_index("tp")
    heads = w_query.shape[1] // HEAD
    kv_heads = w_key.shape[1] // HEAD
    scale = (width // (heads * tp_count)) ** (-0.5)
    if front_fits(seq_count, tp_count, heads, kv_heads, capacity):
        context, rows = front_phase(
            x_old, old_blocks, order, pre_gain, w_query, w_key, w_value, seq_count, tp_count, scale
        )
        return output_phase(
            context, w_out_t, rows, post_gain, new_blocks, seq_count, tp_count, heads
        )
    old_start = offsets(old_blocks)
    new_start = offsets(new_blocks)
    device_ids = jnp.arange(seq_count, dtype=jnp.int32)

    gathered = lax.all_gather(x_old, "seq", axis=0, tiled=True)

    def stored(row, count):
        row = jnp.minimum(row, tokens - count)
        shard = jnp.sum((old_start <= row).astype(jnp.int32)) - 1
        holder = jnp.sum(jnp.where(order == shard, device_ids, 0))
        begin = jnp.sum(jnp.where(device_ids == shard, old_start, 0))
        return lax.dynamic_slice_in_dim(gathered, holder * capacity + row - begin, count, 0)

    def shift(k):
        return [(i, (i + k) % tp_count) for i in range(tp_count)]

    def by_source(received):
        stack = jnp.stack(received)
        pieces = [
            lax.dynamic_index_in_dim(stack, lax.rem(tp_index - u + tp_count, tp_count), 0, False)
            for u in range(tp_count)
        ]
        return jnp.concatenate(pieces, axis=1)

    mine = jnp.concatenate(
        [stored(seq_index * own + at, BLOCK) for at in range(0, own, BLOCK)], axis=0
    )
    full_rows = by_source(
        [mine] + [lax.ppermute(mine, "tp", shift(k)) for k in range(1, tp_count)]
    )
    my_start = jnp.sum(jnp.where(device_ids == seq_index, new_start, 0))

    def slot_rows(place):
        return stored(my_start + place * share, share)

    residual = by_source(
        [slot_rows(tp_index)]
        + [
            lax.ppermute(slot_rows(lax.rem(tp_index + k, tp_count)), "tp", shift(k))
            for k in range(1, tp_count)
        ]
    )

    weights = lax.all_gather(
        jnp.concatenate([w_query, w_key, w_value], axis=1), "seq", axis=0, tiled=True
    )

    normed = rms_scale(full_rows.astype(jnp.float32), pre_gain).astype(jnp.bfloat16)
    normed, residual = lax.optimization_barrier((normed, residual))
    group = heads // kv_heads
    copies = seq_count // heads
    raw = jnp.dot(normed, weights, preferred_element_type=jnp.float32)

    half = HEAD // 2
    inverse = jnp.exp(jnp.arange(half, dtype=jnp.float32) * (-2.0 * math.log(10000.0) / HEAD))
    places = seq_index * own + jnp.arange(own, dtype=jnp.int32)
    angles = places.astype(jnp.float32)[:, None] * inverse[None, :]
    cosine, sine = jnp.cos(angles), jnp.sin(angles)

    def rotate(at):
        first = raw[:, at * HEAD : at * HEAD + half]
        second = raw[:, at * HEAD + half : (at + 1) * HEAD]
        return jnp.concatenate(
            [first * cosine - second * sine, second * cosine + first * sine], axis=-1
        )

    queries = [(rotate(h) * scale).astype(jnp.bfloat16) for h in range(heads)]
    keys = [rotate(heads + g).astype(jnp.bfloat16) for g in range(kv_heads)]
    values = [
        raw[:, (heads + kv_heads + g) * HEAD : (heads + kv_heads + g + 1) * HEAD].astype(
            jnp.bfloat16
        )
        for g in range(kv_heads)
    ]
    sent = jnp.stack(
        [
            jnp.stack([queries[s // copies], keys[s // copies // group], values[s // copies // group]])
            for s in range(seq_count)
        ]
    )
    came = lax.all_to_all(sent, "seq", 0, 0, tiled=True)
    context = attention(
        came[:, 0].reshape(tokens, HEAD),
        came[:, 1].reshape(tokens, HEAD),
        came[:, 2].reshape(tokens, HEAD),
    )
    return output_phase(
        context, w_out_t, residual, post_gain, new_blocks, seq_count, tp_count, heads
    )


def solution(mesh):
    placed = (
        P("seq", "tp"),
        P(),
        P(),
        P(),
        P(),
        P(),
        P("seq", "tp"),
        P("seq", "tp"),
        P("seq", "tp"),
        P("seq", "tp"),
    )
    return jax.shard_map(
        per_device, mesh=mesh, in_specs=placed, out_specs=P(("seq", "tp"), None), check_vma=False
    )
```

```python
import functools
import math

import jax
import jax.numpy as jnp
import numpy as np
from jax import lax
from jax.experimental import pallas as pl
from jax.experimental.pallas import tpu as pltpu
from jax.sharding import PartitionSpec as P

HEAD = 128
BLOCK = 128
EPS = 1e-06
LAG = 4


def offsets(blocks):
    return (jnp.cumsum(blocks) - blocks) * BLOCK


def rms_scale(values, gain):
    return values * lax.rsqrt(jnp.mean(values * values, axis=-1, keepdims=True) + EPS) * gain


def attention_kernel(rows, span, q_ref, k_ref, v_ref, out_ref):
    first = pl.program_id(0) * rows
    query = q_ref[...]

    def step(at, carry, masked):
        numer, denom = carry
        start = pl.multiple_of(at * span, span)
        score = lax.dot_general(
            query,
            k_ref[pl.ds(start, span), :],
            (((1,), (1,)), ((), ())),
            preferred_element_type=jnp.float32,
        )
        weight = jnp.exp(50.0 * jnp.tanh(score * (1.0 / 50.0)))
        if masked:
            places = first + lax.broadcasted_iota(jnp.int32, weight.shape, 0)
            keys = start + lax.broadcasted_iota(jnp.int32, weight.shape, 1)
            weight = jnp.where(keys <= places, weight, 0.0)
        denom = denom + jnp.sum(weight, axis=1, keepdims=True)
        numer = numer + jnp.dot(
            weight.astype(jnp.bfloat16),
            v_ref[pl.ds(start, span), :],
            preferred_element_type=jnp.float32,
        )
        return numer, denom

    whole = first // span
    state = (jnp.zeros((rows, HEAD), jnp.float32), jnp.zeros((rows, 1), jnp.float32))
    state = lax.fori_loop(0, whole, lambda at, c: step(at, c, False), state)
    numer, denom = step(whole, state, True)
    out_ref[...] = (numer / denom).astype(out_ref.dtype)


def attention(query, key, value):
    tokens = query.shape[0]
    rows, span = 256, 512
    return pl.pallas_call(
        functools.partial(attention_kernel, rows, span),
        grid=(tokens // rows,),
        in_specs=[
            pl.BlockSpec((rows, HEAD), lambda i: (i, 0)),
            pl.BlockSpec((tokens, HEAD), lambda i: (0, 0)),
            pl.BlockSpec((tokens, HEAD), lambda i: (0, 0)),
        ],
        out_specs=pl.BlockSpec((rows, HEAD), lambda i: (i, 0)),
        out_shape=jax.ShapeDtypeStruct((tokens, HEAD), jnp.bfloat16),
        cost_estimate=pl.CostEstimate(
            flops=3 * tokens * tokens * HEAD,
            bytes_accessed=8 * tokens * HEAD,
            transcendentals=tokens * tokens,
        ),
    )(query, key, value)


MESH = pl.DeviceIdType.MESH


def arrangements(seq_count):
    found = []
    for second in range(1, seq_count + 1):
        for third in range(1, second + 1):
            fourth = seq_count - second - third
            if 1 <= fourth <= third:
                found.append((seq_count, second, third, fourth))
    return found


def layer_windows(seq_count, tp_count, per_block):
    first, last = [], []
    for layer in range(tp_count):
        starts, ends = [], []
        for counts in arrangements(seq_count):
            begin = sum(counts[u // per_block] for u in range(layer))
            starts.append(begin)
            ends.append(begin + counts[layer // per_block])
        first.append(min(starts))
        last.append(max(ends))
    return first, last


def pick(index, values):
    result = jnp.int32(values[0])
    for k in range(1, len(values)):
        result = jnp.where(index == k, jnp.int32(values[k]), result)
    return result


def flipped(index, mask):
    result = index
    bit = 1
    while bit <= mask:
        if mask & bit:
            result = result + bit - 2 * bit * lax.rem(index // bit, 2)
        bit *= 2
    return result


def output_kernel(
    heads,
    copies,
    seq_count,
    tp_count,
    share,
    first,
    last,
    scattered,
    perm_ref,
    place_ref,
    block_ref,
    context_ref,
    weight_ref,
    residual_ref,
    gain_ref,
    out_ref,
    full,
    partial,
    left_in,
    right_in,
    left_out,
    right_out,
    total,
    sent,
    came,
    gather_send,
    gather_recv,
    left_send,
    left_recv,
    right_send,
    right_recv,
    swap_send,
    swap_recv,
    old_sent,
    old_came,
    old_send,
    old_recv,
    weight,
    staged,
    weight_sem,
    staged_sem,
):
    seq_index = lax.axis_index("seq")
    tp_index = lax.axis_index("tp")
    places = partial.shape[0]
    depth = weight_ref.shape[0]
    half = partial.shape[1]
    core = lax.rem(seq_index, 2)
    partner = seq_index + 1 - 2 * core
    shared = copies == 1
    unit = 2 if shared else copies
    span = 2 * HEAD if shared else HEAD
    slot_index = seq_index // unit
    chunks = full.shape[0]
    per_chunk = places // chunks

    barrier = pltpu.get_barrier_semaphore()
    for k in range(1, seq_count):
        pl.semaphore_signal(
            barrier,
            inc=1,
            device_id=(lax.rem(seq_index + k, seq_count), tp_index),
            device_id_type=MESH,
        )

    @pl.when(tp_index > 0)
    def _():
        pl.semaphore_signal(
            barrier, inc=1, device_id=(seq_index, tp_index - 1), device_id_type=MESH
        )

    @pl.when(tp_index < tp_count - 1)
    def _():
        pl.semaphore_signal(
            barrier, inc=1, device_id=(seq_index, tp_index + 1), device_id_type=MESH
        )

    neighbours = jnp.where(tp_index > 0, 1, 0) + jnp.where(tp_index < tp_count - 1, 1, 0)
    pl.semaphore_wait(barrier, seq_count - 1 + neighbours)

    bits = (seq_count // unit).bit_length() - 1
    order = list(range(chunks))[::-1]
    head = seq_index // copies
    own_columns = pl.ds(pl.multiple_of(head * HEAD, HEAD), HEAD)

    def staged_copy(chunk):
        return pltpu.make_async_remote_copy(
            src_ref=staged.at[chunk],
            dst_ref=full.at[chunk, :, own_columns],
            send_sem=staged_sem.at[0, chunk],
            recv_sem=staged_sem.at[1, chunk],
            device_id=(partner, tp_index),
            device_id_type=MESH,
        )

    own_rows = pl.ds(pl.multiple_of(core * depth, depth), depth)
    weight_copy = pltpu.make_async_remote_copy(
        src_ref=weight_ref,
        dst_ref=weight.at[own_rows],
        send_sem=weight_sem.at[0],
        recv_sem=weight_sem.at[1],
        device_id=(partner, tp_index),
        device_id_type=MESH,
    )

    for chunk in order:
        for at in range(per_chunk):
            source = perm_ref[chunk * per_chunk + at]
            rows = slice(at * half, (at + 1) * half)
            full[chunk, rows, own_columns] = context_ref[source, core]
            if shared:
                staged[chunk, rows] = context_ref[source, 1 - core]
        if shared:
            staged_copy(chunk).start()
    weight_copy.start()

    def dims(chunk):
        outer = list(range(bits))
        return outer[::-1] if chunk % 2 else outer

    def gather_copy(chunk, bit, combo, to_me):
        slot = flipped(slot_index, (combo ^ (1 << bit)) if to_me else combo)
        view = full.at[chunk, :, pl.ds(pl.multiple_of(slot * span, span), span)]
        return pltpu.make_async_remote_copy(
            src_ref=view,
            dst_ref=view,
            send_sem=gather_send.at[chunk, bit, combo],
            recv_sem=gather_recv.at[chunk, bit, combo],
            device_id=(flipped(seq_index, unit << bit), tp_index),
            device_id_type=MESH,
        )

    def steps(chunk):
        held = [0]
        for bit in dims(chunk):
            yield bit, list(held)
            held = held + [c ^ (1 << bit) for c in held]

    def offer(at):
        if at < chunks:
            if shared:
                staged_copy(order[at]).wait_recv()
            for bit, _ in steps(order[at]):
                gather_copy(order[at], bit, 0, False).start()

    offer(0)
    weight[own_rows] = weight_ref[...]
    total[...] = jnp.zeros_like(total)

    def relay(at):
        chunk = order[at]
        stages = list(steps(chunk))
        for level, (bit, held) in enumerate(stages):
            for combo in held:
                gather_copy(chunk, bit, combo, True).wait_recv()
                for later, _ in stages[level + 1 :]:
                    gather_copy(chunk, later, combo ^ (1 << bit), False).start()
            if level == 0:
                offer(at + 1)

    def multiply(chunk):
        product = lax.dot_general(
            full[chunk],
            weight[...],
            (((1,), (1,)), ((), ())),
            preferred_element_type=jnp.float32,
        ).astype(jnp.bfloat16)
        for at in range(per_chunk):
            partial[chunk * per_chunk + at] = product[at * half : (at + 1) * half]

    left_has = jnp.where(tp_index < tp_count - 1, pick(tp_index, last), 0)
    left_gives = pick(tp_index, [0] + last[:-1])
    right_has = jnp.where(tp_index > 0, pick(tp_index, first), places)
    right_gives = pick(tp_index, first[1:] + [places])

    def line_copy(place, source, landing, send, recv, step):
        return pltpu.make_async_remote_copy(
            src_ref=source.at[place],
            dst_ref=landing.at[place],
            send_sem=send.at[place],
            recv_sem=recv.at[place],
            device_id=(seq_index, tp_index + step),
            device_id_type=MESH,
        )

    def flow(place, has, gives, source, landing, send, recv, step):
        @pl.when(has)
        def _():
            line_copy(place, source, landing, send, recv, step).wait_recv()

        @pl.when(jnp.logical_and(has, gives))
        def _():
            source[place] = (
                partial[place].astype(jnp.float32) + landing[place].astype(jnp.float32)
            ).astype(jnp.bfloat16)

        @pl.when(jnp.logical_and(jnp.logical_not(has), gives))
        def _():
            source[place] = partial[place]

        @pl.when(gives)
        def _():
            line_copy(place, source, landing, send, recv, step).start()

    def swap_copy(other, mine, at):
        return pltpu.make_async_remote_copy(
            src_ref=sent.at[other],
            dst_ref=came.at[mine],
            send_sem=swap_send.at[at],
            recv_sem=swap_recv.at[at],
            device_id=(other, tp_index),
            device_id_type=MESH,
        )

    def line_step(at, carry):
        passed = at - LAG * (tp_count - 1 - tp_index)
        place = places - 1 - passed
        valid = jnp.logical_and(passed >= 0, passed < places)
        has = jnp.logical_and(valid, place < left_has)
        gives = jnp.logical_and(valid, place < left_gives)
        flow(place, has, gives, left_out, left_in, left_send, left_recv, -1)
        ends = jnp.logical_and(
            jnp.logical_and(valid, tp_index == 0), place < seq_count
        )

        @pl.when(ends)
        def _():
            sent[place] = (
                partial[place].astype(jnp.float32) + left_in[place].astype(jnp.float32)
            ).astype(jnp.bfloat16)

            @pl.when(place == seq_index)
            def _():
                came[place] = sent[place]

            @pl.when(place != seq_index)
            def _():
                swap_copy(
                    place, seq_index, lax.rem(place + seq_count - seq_index, seq_count)
                ).start()

        passed = at - LAG * tp_index
        place = places - 1 - passed
        valid = jnp.logical_and(passed >= 0, passed < places)
        has = jnp.logical_and(valid, place >= right_has)
        gives = jnp.logical_and(valid, place >= right_gives)
        flow(place, has, gives, right_out, right_in, right_send, right_recv, 1)
        return carry

    def old_copy(other, mine, at):
        return pltpu.make_async_remote_copy(
            src_ref=old_sent.at[other],
            dst_ref=old_came.at[mine],
            send_sem=old_send.at[at],
            recv_sem=old_recv.at[at],
            device_id=(other, tp_index),
            device_id_type=MESH,
        )

    for at, chunk in enumerate(order):
        relay(at)
        if at == 0:
            weight_from = pltpu.make_async_remote_copy(
                src_ref=weight_ref,
                dst_ref=weight.at[pl.ds(pl.multiple_of((1 - core) * depth, depth), depth)],
                send_sem=weight_sem.at[0],
                recv_sem=weight_sem.at[1],
                device_id=(partner, tp_index),
                device_id_type=MESH,
            )
            weight_from.wait_recv()
        multiply(chunk)
        if scattered and at == chunks - 1:
            for j in range(seq_count):
                old_sent[j] = residual_ref[block_ref[j]]
            for k in range(1, seq_count):
                old_copy(lax.rem(seq_index + k, seq_count), seq_index, k).start()
            old_came[seq_index] = old_sent[seq_index]
        lax.fori_loop(at * per_chunk, (at + 1) * per_chunk, line_step, 0)
    lax.fori_loop(places, places + LAG * (tp_count - 1), line_step, 0)

    def sum_step(place, carry):
        value = partial[place].astype(jnp.float32) + right_in[place].astype(jnp.float32)

        @pl.when(place < left_has)
        def _():
            total[place] = (value + left_in[place].astype(jnp.float32)).astype(jnp.bfloat16)

        @pl.when(place >= left_has)
        def _():
            total[place] = value.astype(jnp.bfloat16)

        return carry

    @pl.when(tp_index > 0)
    def _():
        lax.fori_loop(pick(tp_index, first), pick(tp_index, last), sum_step, 0)
        for j in range(seq_count):
            sent[j] = total[place_ref[j]]
        for k in range(1, seq_count):
            swap_copy(lax.rem(seq_index + k, seq_count), seq_index, k).start()
        came[seq_index] = sent[seq_index]

    for k in range(1, seq_count):
        swap_copy(
            lax.rem(seq_index + k, seq_count),
            lax.rem(seq_index + seq_count - k, seq_count),
            k,
        ).wait_recv()

    if scattered:
        for k in range(1, seq_count):
            old_copy(
                lax.rem(seq_index + k, seq_count),
                lax.rem(seq_index + seq_count - k, seq_count),
                k,
            ).wait_recv()
    wide = 2 * depth
    for side in range(2):
        square = jnp.zeros((half, 1), jnp.float32)
        for c in range(seq_count // 2):
            piece = came[2 * c + side].astype(jnp.float32)
            square = square + jnp.sum(piece * piece, axis=1, keepdims=True)
        factor = lax.rsqrt(square * (1.0 / (depth * seq_count)) + EPS)
        rows = slice(side * half, (side + 1) * half)
        for c in range(seq_count // 2):
            columns = slice(c * wide, (c + 1) * wide)
            old = old_came[2 * c + side] if scattered else residual_ref[rows, columns]
            value = old.astype(jnp.float32) + (
                came[2 * c + side].astype(jnp.float32) * factor * gain_ref[:, columns]
            )
            out_ref[rows, columns] = value.astype(jnp.bfloat16)

    for k in range(1, seq_count):
        swap_copy(lax.rem(seq_index + k, seq_count), seq_index, k).wait_send()
    if scattered:
        for k in range(1, seq_count):
            old_copy(lax.rem(seq_index + k, seq_count), seq_index, k).wait_send()
    weight_copy.wait_send()
    for chunk in range(chunks):
        if shared:
            staged_copy(chunk).wait_send()
        for bit, held in steps(chunk):
            for combo in held:
                gather_copy(chunk, bit, combo, False).wait_send()

    def drain(place, carry):
        @pl.when(place < left_gives)
        def _():
            line_copy(place, left_out, left_in, left_send, left_recv, -1).wait_send()

        @pl.when(place >= right_gives)
        def _():
            line_copy(place, right_out, right_in, right_send, right_recv, 1).wait_send()

        return carry

    lax.fori_loop(0, places, drain, 0)


def front_kernel(
    seq_count,
    tp_count,
    group,
    scale,
    blocks_ref,
    order_ref,
    x_ref,
    gain_ref,
    query_ref,
    key_ref,
    value_ref,
    angle_ref,
    context_out,
    x_out,
    q_buf,
    kv_buf,
    near,
    send_a,
    send_b,
    far,
    line,
    twin,
    weight,
    normed,
    scale_row,
    scale_all,
    scale_column,
    first_out,
    first_in,
    second_out,
    second_in,
    kept,
    core_sem,
    weight_sem,
    stage_sem,
    line_send,
    line_recv,
    plane_send,
    plane_recv,
    twin_sem,
    stat_sem,
    factor_sem,
    first_sem,
    second_sem,
    kv_sem,
):
    seq_index = lax.axis_index("seq")
    tp_index = lax.axis_index("tp")
    chip = seq_index // 2
    core = lax.rem(seq_index, 2)
    partner = seq_index + 1 - 2 * core
    slots = x_ref.shape[0]
    chips = seq_count // 2
    each = line.shape[1]
    half = line.shape[2]
    quarter = line.shape[3]
    depth = query_ref.shape[0]
    pair = 2 * HEAD

    barrier = pltpu.get_barrier_semaphore()
    for k in range(1, seq_count):
        other = lax.rem(seq_index + k, seq_count)
        pl.semaphore_signal(barrier, inc=1, device_id=(other, tp_index), device_id_type=MESH)
    for k in range(1, tp_count):
        other = lax.rem(tp_index + k, tp_count)
        pl.semaphore_signal(barrier, inc=1, device_id=(seq_index, other), device_id_type=MESH)

    def remote(source, target, sems, at, seq, tp):
        return pltpu.make_async_remote_copy(
            src_ref=source,
            dst_ref=target,
            send_sem=sems[0].at[at],
            recv_sem=sems[1].at[at],
            device_id=(seq, tp),
            device_id_type=MESH,
        )

    core_sems = (core_sem.at[0], core_sem.at[1])

    def swap_slots(holder):
        return remote(
            x_ref.at[:, 1 - core],
            near.at[pl.ds(slots * holder, slots)],
            core_sems,
            0,
            partner,
            tp_index,
        )

    def lanes(head, count=1):
        return pl.ds(pl.multiple_of(head * HEAD, HEAD), count * HEAD)

    def weight_copy(source, column, target, at, holder):
        return remote(
            source.at[:, lanes(column)],
            weight.at[pl.ds(pl.multiple_of(holder * depth, depth), depth), lanes(target)],
            (weight_sem.at[0], weight_sem.at[1]),
            at,
            partner,
            tp_index,
        )

    pl.semaphore_wait(barrier, seq_count - 1 + tp_count - 1)
    swap_slots(core).start()
    for slot in range(slots):
        near[slots * core + slot] = x_ref[slot, core]

    starts, counts, holders = [], [], []
    begin = jnp.int32(0)
    for k in range(seq_count):
        starts.append(begin)
        counts.append(blocks_ref[k])
        begin = begin + blocks_ref[k]
        holder = jnp.int32(0)
        for place in range(1, seq_count):
            holder = holder + jnp.where(order_ref[place] == k, jnp.int32(place), jnp.int32(0))
        holders.append(holder)

    def found(block):
        at = jnp.int32(0)
        for k in range(seq_count):
            inside = jnp.logical_and(starts[k] <= block, block < starts[k] + counts[k])
            at = at + jnp.where(inside, holders[k] * slots + block - starts[k], jnp.int32(0))
        return at // (2 * slots), lax.rem(at, 2 * slots)

    first_chip = jnp.where(core == 0, flipped(chip, 1), flipped(chip, 2))
    second_chip = jnp.where(core == 0, flipped(chip, 2), flipped(chip, 1))
    cross_chip = flipped(chip, 3)
    swap_slots(1 - core).wait_recv()

    stage_sems = (stage_sem.at[0], stage_sem.at[1])
    table_a = []
    for at in range(2 * each):
        target = first_chip if at < each else cross_chip
        owner, index = found(chips * (at % each) + target)
        table_a.append(jnp.where(owner == chip, index, 0))
    across_first = list(range(each, 2 * each)) + list(range(each))
    for at in across_first:
        send_a[at] = near[table_a[at]]
        remote(
            send_a.at[at], far.at[at], stage_sems, at, 2 * first_chip + core, tp_index
        ).start()

    for c in range(chips):
        weight_copy(query_ref, 2 * c + 1 - core, 2 * c, 2 * c, core).start()

        @pl.when(core == 0)
        def _():
            weight_copy(value_ref, c, 2 * c + 1, 2 * c + 1, core).start()

        @pl.when(core == 1)
        def _():
            weight_copy(key_ref, c, 2 * c + 1, 2 * c + 1, core).start()

    own_rows = pl.ds(pl.multiple_of(core * depth, depth), depth)
    for c in range(chips):
        weight[own_rows, pl.ds(2 * c * HEAD, HEAD)] = query_ref[:, lanes(2 * c + core)]

        @pl.when(core == 0)
        def _():
            weight[own_rows, pl.ds((2 * c + 1) * HEAD, HEAD)] = key_ref[
                :, pl.ds(c * HEAD, HEAD)
            ]

        @pl.when(core == 1)
        def _():
            weight[own_rows, pl.ds((2 * c + 1) * HEAD, HEAD)] = value_ref[
                :, pl.ds(c * HEAD, HEAD)
            ]

    def arrive_a(at):
        remote(
            send_a.at[at], far.at[at], stage_sems, at, 2 * first_chip + core, tp_index
        ).wait_recv()

    both = 2 * slots
    for at in range(each, 2 * each):
        arrive_a(at)
        near[both + at] = far[at]
    for at in range(each):
        owner, index = found(chips * at + second_chip)
        send_b[at] = near[jnp.where(owner == chip, index, both + each + at)]
        remote(
            send_b.at[at],
            far.at[2 * each + at],
            stage_sems,
            2 * each + at,
            2 * second_chip + core,
            tp_index,
        ).start()
    for at in range(each):
        arrive_a(at)
        near[both + at] = far[at]
    for at in range(each):
        owner, index = found(chips * at + chip)
        near[both + 2 * each + at] = near[jnp.where(owner == chip, index, both + at)]
    for at in range(each):
        remote(
            send_b.at[at],
            far.at[2 * each + at],
            stage_sems,
            2 * each + at,
            2 * second_chip + core,
            tp_index,
        ).wait_recv()
        near[both + 3 * each + at] = far[2 * each + at]
    for at in range(each):
        owner, _ = found(chips * at + chip)
        local = jnp.logical_or(owner == chip, owner == first_chip)
        line[tp_index, at] = near[
            jnp.where(local, both + 2 * each + at, both + 3 * each + at)
        ]

    def line_copy(layer, at, step):
        view = line.at[layer, at]
        return pltpu.make_async_remote_copy(
            src_ref=view,
            dst_ref=view,
            send_sem=line_send.at[(step + 1) // 2, layer, at],
            recv_sem=line_recv.at[layer, at],
            device_id=(seq_index, tp_index + step),
            device_id_type=MESH,
        )

    def plane_copy(layer, at, holder):
        return pltpu.make_async_remote_copy(
            src_ref=line.at[layer, at],
            dst_ref=x_out.at[chips * at + holder],
            send_sem=plane_send.at[layer, at],
            recv_sem=plane_recv.at[chips * at + holder],
            device_id=(2 * layer + core, tp_index),
            device_id_type=MESH,
        )

    def twin_copy(block):
        return remote(
            x_out.at[block],
            twin.at[block],
            (twin_sem.at[0], twin_sem.at[1]),
            block,
            partner,
            tp_index,
        )

    def guarded(condition, action):
        @pl.when(condition)
        def _():
            action()

    def forward(layer, at):
        @pl.when(layer == chip)
        def _():
            x_out[chips * at + chip] = line[layer, at]

        @pl.when(layer != chip)
        def _():
            plane_copy(layer, at, chip).start()

    def own_step(at):
        guarded(tp_index > 0, lambda: line_copy(tp_index, at, -1).start())
        guarded(tp_index < tp_count - 1, lambda: line_copy(tp_index, at, 1).start())
        forward(tp_index, at)

    def hop_step(at, distance):
        @pl.when(tp_index >= distance)
        def _():
            layer = tp_index - distance
            line_copy(layer, at, 1).wait_recv()
            guarded(tp_index < tp_count - 1, lambda: line_copy(layer, at, 1).start())
            forward(layer, at)

        @pl.when(tp_index + distance < tp_count)
        def _():
            layer = tp_index + distance
            line_copy(layer, at, -1).wait_recv()
            guarded(tp_index > 0, lambda: line_copy(layer, at, -1).start())
            forward(layer, at)

    def plane_step(at):
        for c in range(chips):

            @pl.when(chip != c)
            def _():
                plane_copy(chip, at, c).wait_recv()

        for c in range(chips):
            twin_copy(chips * at + c).start()

    tiles = quarter // HEAD
    gain_at = pl.multiple_of(chip * quarter, HEAD)

    def normalize(source, block, holder, target):
        rows = pl.ds(pl.multiple_of((block // chips) * half, half), half)
        factor = scale_column[holder, rows, :]
        for tile in range(tiles):
            columns = slice(tile * HEAD, (tile + 1) * HEAD)
            values = source[block, :, columns].astype(jnp.float32)
            gains = gain_ref[:, pl.ds(pl.multiple_of(gain_at + tile * HEAD, HEAD), HEAD)]
            normed[target[0], target[1], target[2], :, columns] = (
                values * factor * gains
            ).astype(jnp.bfloat16)

    bits = (1, 2)

    def first_copy(at, side):
        bit = bits[side]
        return pltpu.make_async_remote_copy(
            src_ref=first_out.at[at, side],
            dst_ref=first_in.at[at, side],
            send_sem=first_sem.at[0, at, side],
            recv_sem=first_sem.at[1, at, side],
            device_id=(2 * flipped(chip, bit) + core, tp_index),
            device_id_type=MESH,
        )

    def second_copy(at, side):
        bit = bits[1 - side]
        return pltpu.make_async_remote_copy(
            src_ref=second_out.at[at, side],
            dst_ref=second_in.at[at, side],
            send_sem=second_sem.at[0, at, side],
            recv_sem=second_sem.at[1, at, side],
            device_id=(2 * flipped(chip, bit) + core, tp_index),
            device_id_type=MESH,
        )

    def multiply_step(at):
        for side in range(2):
            for u in range(2):
                c = 2 * side + u
                block = chips * at + c
                twin_copy(block).wait_recv()
                normalize(x_out, block, 2 * c + core, (side, u, core))
                normalize(twin, block, 2 * c + 1 - core, (side, u, 1 - core))
            rows = normed[side].reshape(4 * half, quarter)

            def part(mask):
                target = flipped(chip, mask)
                return jnp.dot(
                    rows,
                    weight[:, lanes(2 * target, 2)],
                    preferred_element_type=jnp.float32,
                )

            first, second = bits[side], bits[1 - side]
            first_out[at, side, 0] = part(first).astype(jnp.bfloat16)
            first_out[at, side, 1] = part(3).astype(jnp.bfloat16)
            first_copy(at, side).start()
            kept[at, side, 0] = part(0)
            kept[at, side, 1] = part(second)

    def add_step(at):
        for side in range(2):
            first_copy(at, side).wait_recv()
            second_out[at, side] = (
                kept[at, side, 1] + first_in[at, side, 1].astype(jnp.float32)
            ).astype(jnp.bfloat16)
            second_copy(at, side).start()

    def kv_copy(kind, block):
        rows = pl.ds(pl.multiple_of(block * BLOCK, BLOCK), BLOCK)
        view = kv_buf.at[kind, rows, :]
        return remote(
            view, view, (kv_sem.at[0], kv_sem.at[1]), block, partner, tp_index
        )

    lane = lax.broadcasted_iota(jnp.int32, (BLOCK, HEAD), 1)

    def turned(values, rows):
        angles = angle_ref[rows, :]
        swapped = pltpu.roll(angles, HEAD // 2, 1)
        low = lane < HEAD // 2
        cosine = jnp.where(low, angles, swapped)
        sine = jnp.where(low, -swapped, angles)
        return values * cosine + pltpu.roll(values, HEAD // 2, 1) * sine

    def finish_step(at):
        for side in range(2):
            second_copy(at, side).wait_recv()
            for u in range(2):
                block = chips * at + 2 * side + u
                part = slice(u * BLOCK, (u + 1) * BLOCK)
                value = (
                    kept[at, side, 0, part]
                    + first_in[at, side, 0, part].astype(jnp.float32)
                    + second_in[at, side, part].astype(jnp.float32)
                )
                rows = pl.ds(pl.multiple_of(block * BLOCK, BLOCK), BLOCK)
                q_buf[rows, :] = (turned(value[:, :HEAD], rows) * scale).astype(jnp.bfloat16)

                @pl.when(core == 0)
                def _():
                    kv_buf[0, rows, :] = turned(value[:, HEAD:], rows).astype(jnp.bfloat16)

                @pl.when(core == 1)
                def _():
                    kv_buf[1, rows, :] = value[:, HEAD:].astype(jnp.bfloat16)

                kv_copy(core, block).start()

    span = chips * BLOCK
    sub = span // 2
    mask = lax.broadcasted_iota(jnp.int32, (sub, sub), 1) <= lax.broadcasted_iota(
        jnp.int32, (sub, sub), 0
    )

    def attend_step(at):
        for c in range(chips):
            kv_copy(1 - core, chips * at + c).wait_recv()

        def attend(query, start, count, carry, masked):
            keys = pl.ds(pl.multiple_of(start, sub), count)
            score = lax.dot_general(
                query,
                kv_buf[0, keys, :],
                (((1,), (1,)), ((), ())),
                preferred_element_type=jnp.float32,
            )
            part = jnp.exp2((50.0 / math.log(2.0)) * jnp.tanh(score * (1.0 / 50.0)))
            if masked:
                part = jnp.where(mask, part, 0.0)
            numer, denom = carry
            denom = denom + jnp.sum(part, axis=1, keepdims=True)
            numer = numer + jnp.dot(
                part.astype(jnp.bfloat16), kv_buf[1, keys, :], preferred_element_type=jnp.float32
            )
            return numer, denom

        for piece in range(2):
            begin = at * span + piece * sub
            rows = pl.ds(pl.multiple_of(begin, sub), sub)
            query = q_buf[rows, :]
            state = (jnp.zeros((sub, HEAD), jnp.float32), jnp.zeros((sub, 1), jnp.float32))
            state = lax.fori_loop(
                0, at, lambda n, carry: attend(query, n * span, span, carry, False), state
            )
            if piece:
                state = attend(query, at * span, sub, state, False)
            numer, denom = attend(query, begin, sub, state, True)
            context_out[rows, :] = (numer / denom).astype(jnp.bfloat16)

    def stat_copy(layer_from, layer_to):
        return pltpu.make_async_remote_copy(
            src_ref=scale_row.at[layer_from],
            dst_ref=scale_row.at[layer_from],
            send_sem=stat_sem.at[0, layer_to],
            recv_sem=stat_sem.at[1, layer_from],
            device_id=(seq_index, layer_to),
            device_id_type=MESH,
        )

    def factor_copy(holder, other):
        return pltpu.make_async_remote_copy(
            src_ref=scale_all.at[holder],
            dst_ref=scale_all.at[holder],
            send_sem=factor_sem.at[0, other],
            recv_sem=factor_sem.at[1, holder],
            device_id=(other, tp_index),
            device_id_type=MESH,
        )

    own_step(0)
    squares = []
    for at in range(each):
        values = line[tp_index, at].astype(jnp.float32)
        squares.append(jnp.sum(values * values, axis=1, keepdims=True))
    column = jnp.broadcast_to(jnp.concatenate(squares, axis=0), (each * half, HEAD))
    scale_row[tp_index] = jnp.transpose(column)[:8, :]
    for k in range(1, tp_count):
        stat_copy(tp_index, lax.rem(tp_index + k, tp_count)).start()
    for c in range(2 * chips):
        weight_copy(query_ref, 0, 0, c, 1 - core).wait_recv()
    for k in range(1, tp_count):
        other = lax.rem(tp_index + k, tp_count)
        stat_copy(other, tp_index).wait_recv()
    square = scale_row[0]
    for k in range(1, tp_count):
        square = square + scale_row[k]
    scale_all[seq_index] = lax.rsqrt(square * (1.0 / (quarter * tp_count)) + EPS)
    for k in range(1, seq_count):
        factor_copy(seq_index, lax.rem(seq_index + k, seq_count)).start()

    def steps(i, carry):
        for lag, action in (
            (0, lambda at: guarded(at > 0, lambda: own_step(at))),
            (1, lambda at: hop_step(at, 1)),
            (2, lambda at: hop_step(at, 2)),
            (3, lambda at: hop_step(at, 3)),
            (4, plane_step),
            (5, multiply_step),
            (6, add_step),
            (7, finish_step),
            (8, attend_step),
        ):
            at = i - lag

            @pl.when(jnp.logical_and(at >= 0, at < each))
            def _():
                action(at)

        return carry

    lax.fori_loop(0, 5, steps, 0)
    for k in range(1, seq_count):
        other = lax.rem(seq_index + k, seq_count)
        factor_copy(other, seq_index).wait_recv()
    for s in range(seq_count):
        scale_column[s] = jnp.transpose(
            jnp.broadcast_to(scale_all[s, :1, :], (HEAD, each * half))
        )
    lax.fori_loop(5, each + 8, steps, 0)

    swap_slots(core).wait_send()
    for c in range(2 * chips):
        weight_copy(query_ref, 0, 0, c, core).wait_send()
    for at in range(2 * each):
        remote(
            send_a.at[at], far.at[at], stage_sems, at, 2 * first_chip + core, tp_index
        ).wait_send()
    for at in range(each):
        remote(
            send_b.at[at],
            far.at[2 * each + at],
            stage_sems,
            2 * each + at,
            2 * second_chip + core,
            tp_index,
        ).wait_send()
    for k in range(1, tp_count):
        stat_copy(tp_index, lax.rem(tp_index + k, tp_count)).wait_send()
    for k in range(1, seq_count):
        factor_copy(seq_index, lax.rem(seq_index + k, seq_count)).wait_send()

    def drain(at, carry):
        for layer in range(tp_count):
            right = jnp.logical_and(tp_index >= layer, tp_index < tp_count - 1)
            guarded(right, lambda: line_copy(layer, at, 1).wait_send())
            left = jnp.logical_and(tp_index <= layer, tp_index > 0)
            guarded(left, lambda: line_copy(layer, at, -1).wait_send())
            guarded(chip != layer, lambda: plane_copy(layer, at, chip).wait_send())
        for side in range(2):
            first_copy(at, side).wait_send()
            second_copy(at, side).wait_send()
        for c in range(chips):
            twin_copy(chips * at + c).wait_send()
            kv_copy(core, chips * at + c).wait_send()
        return carry

    lax.fori_loop(0, each, drain, 0)


def front_fits(seq_count, tp_count, heads, kv_heads, capacity):
    return (
        heads == seq_count == 8
        and 2 * kv_heads == heads
        and tp_count == 4
        and capacity == 4 * BLOCK
    )


def front_phase(
    x_old, old_blocks, order, pre_gain, w_query, w_key, w_value, seq_count, tp_count, scale
):
    capacity, quarter = x_old.shape
    depth = w_query.shape[0]
    slots = capacity // BLOCK
    half = BLOCK // 2
    tokens = seq_count * capacity // 2
    chips = seq_count // 2
    each = tokens // BLOCK // chips
    group = w_query.shape[1] // w_key.shape[1]
    angles = (
        np.arange(tokens, dtype=np.float32)[:, None]
        * np.exp(
            np.arange(HEAD // 2, dtype=np.float32) * np.float32(-2.0 * math.log(10000.0) / HEAD)
        )[None, :]
    )
    table = np.concatenate([np.cos(angles), np.sin(angles)], axis=1).astype(np.float32)
    bf16, f32 = jnp.bfloat16, jnp.float32
    piece = (half, quarter)
    dma = pltpu.SemaphoreType.DMA
    vmem = pl.BlockSpec(memory_space=pltpu.VMEM)
    smem = pl.BlockSpec(memory_space=pltpu.SMEM)
    square = (2 * BLOCK, 2 * HEAD)
    return pl.pallas_call(
        functools.partial(front_kernel, seq_count, tp_count, group, scale),
        out_shape=(
            jax.ShapeDtypeStruct((tokens, HEAD), bf16),
            jax.ShapeDtypeStruct((each * chips,) + piece, bf16),
        ),
        in_specs=[smem] * 2 + [vmem] * 6,
        out_specs=(vmem, vmem),
        scratch_shapes=[
            pltpu.VMEM((tokens, HEAD), bf16),
            pltpu.VMEM((2, tokens, HEAD), bf16),
            pltpu.VMEM((2 * slots + 4 * each,) + piece, bf16),
            pltpu.VMEM((2 * each,) + piece, bf16),
            pltpu.VMEM((each,) + piece, bf16),
            pltpu.VMEM((3 * each,) + piece, bf16),
            pltpu.VMEM((tp_count, each) + piece, bf16),
            pltpu.VMEM((each * chips,) + piece, bf16),
            pltpu.VMEM((2 * depth, 2 * chips * HEAD), bf16),
            pltpu.VMEM((2, 2, 2) + piece, bf16),
            pltpu.VMEM((tp_count, 8, each * half), f32),
            pltpu.VMEM((seq_count, 8, each * half), f32),
            pltpu.VMEM((seq_count, each * half, HEAD), f32),
            pltpu.VMEM((each, 2, 2) + square, bf16),
            pltpu.VMEM((each, 2, 2) + square, bf16),
            pltpu.VMEM((each, 2) + square, bf16),
            pltpu.VMEM((each, 2) + square, bf16),
            pltpu.VMEM((each, 2, 2) + square, f32),
            dma((2, 1)),
            dma((2, 2 * chips)),
            dma((2, 3 * each)),
            dma((2, tp_count, each)),
            dma((tp_count, each)),
            dma((tp_count, each)),
            dma((each * chips,)),
            dma((2, each * chips)),
            dma((2, tp_count)),
            dma((2, seq_count)),
            dma((2, each, 2)),
            dma((2, each, 2)),
            dma((2, each * chips)),
        ],
        compiler_params=pltpu.CompilerParams(
            collective_id=1, has_side_effects=True, vmem_limit_bytes=60 * 2**20
        ),
        cost_estimate=pl.CostEstimate(
            flops=60_000_000_000, bytes_accessed=8 * tokens * depth, transcendentals=0
        ),
    )(
        old_blocks,
        order,
        x_old.reshape(slots, 2, half, quarter),
        pre_gain.reshape(1, -1),
        w_query,
        w_key,
        w_value,
        jnp.asarray(table),
    )


def output_phase(context, w_out_t, residual, post_gain, new_blocks, seq_count, tp_count, heads):
    tokens = context.shape[0]
    depth = w_out_t.shape[0]
    width = depth * seq_count
    share = 2 * tokens // (seq_count * tp_count)
    scattered = residual.ndim == 3
    places = tokens // share
    per_block = BLOCK // share
    copies = seq_count // heads
    bits = heads.bit_length() - 1
    first, last = layer_windows(seq_count, tp_count, per_block)
    seq_index = lax.axis_index("seq")
    tp_index = lax.axis_index("tp")
    blocks = new_blocks * per_block
    new_start = jnp.sum(
        jnp.where(
            jnp.arange(seq_count)[None, :] < jnp.arange(seq_count)[:, None], blocks[None, :], 0
        ),
        axis=1,
    )
    slots = jnp.arange(tp_count * seq_count, dtype=jnp.int32)
    layer = jnp.arange(tp_count, dtype=jnp.int32)[:, None]
    valid = (blocks[None, :] > layer).astype(jnp.int32).reshape(-1)
    source = (new_start[None, :] + layer).reshape(-1)
    rank = jnp.sum(jnp.where(slots[None, :] < slots[:, None], valid[None, :], 0), axis=1)
    perm = jnp.sum(
        jnp.where(
            (jnp.arange(places)[:, None] == rank[None, :]) & (valid[None, :] > 0),
            source[None, :],
            0,
        ),
        axis=1,
    ).astype(jnp.int32)
    in_layer = (jnp.arange(tp_count) == tp_index)[:, None]
    place = jnp.sum(jnp.where(in_layer, rank.reshape(tp_count, seq_count), 0), axis=0)
    place = jnp.minimum(place, places - 1).astype(jnp.int32)
    mine = jnp.sum(jnp.where(jnp.arange(seq_count) == seq_index, blocks, 0))
    block = jnp.minimum((new_start + tp_index) // per_block, tokens // BLOCK - 1).astype(jnp.int32)
    piece = residual.shape[1:] if scattered else (8, HEAD)
    old_block = pltpu.VMEM((seq_count,) + piece, jnp.bfloat16)
    chunks = 4
    rows = tokens // chunks // 2
    half = share // 2
    scratch_block = pltpu.VMEM((places, half, 2 * depth), jnp.bfloat16)
    swap_block = pltpu.VMEM((seq_count, half, 2 * depth), jnp.bfloat16)
    line_sem = pltpu.SemaphoreType.DMA((places,))
    gather_sem = pltpu.SemaphoreType.DMA((chunks, bits, heads))
    swap_sem = pltpu.SemaphoreType.DMA((seq_count,))
    result = pl.pallas_call(
        functools.partial(
            output_kernel, heads, copies, seq_count, tp_count, share, first, last, scattered
        ),
        out_shape=jax.ShapeDtypeStruct((share, width), jnp.bfloat16),
        in_specs=[pl.BlockSpec(memory_space=pltpu.SMEM)] * 3
        + [pl.BlockSpec(memory_space=pltpu.VMEM)] * 4,
        out_specs=pl.BlockSpec(memory_space=pltpu.VMEM),
        scratch_shapes=[
            pltpu.VMEM((chunks, rows, heads * HEAD), jnp.bfloat16),
            scratch_block,
            scratch_block,
            scratch_block,
            scratch_block,
            scratch_block,
            scratch_block,
            swap_block,
            swap_block,
            gather_sem,
            gather_sem,
            line_sem,
            line_sem,
            line_sem,
            line_sem,
            swap_sem,
            swap_sem,
            old_block,
            old_block,
            swap_sem,
            swap_sem,
            pltpu.VMEM((2 * depth, heads * HEAD), jnp.bfloat16),
            pltpu.VMEM((chunks, rows, HEAD), jnp.bfloat16),
            pltpu.SemaphoreType.DMA((2,)),
            pltpu.SemaphoreType.DMA((2, chunks)),
        ],
        compiler_params=pltpu.CompilerParams(
            collective_id=0, has_side_effects=True, vmem_limit_bytes=56 * 2**20
        ),
        cost_estimate=pl.CostEstimate(
            flops=60_000_000_000, bytes_accessed=4 * tokens * depth, transcendentals=0
        ),
    )(perm, place, block, context.reshape(places, 2, half, HEAD), w_out_t, residual, post_gain.reshape(1, -1))
    return jnp.where(tp_index < mine, result, jnp.zeros_like(result))


def per_device(
    x_old, old_blocks, new_blocks, order, pre_gain, post_gain, w_query, w_key, w_value, w_out_t
):
    seq_count = lax.axis_size("seq")
    tp_count = lax.axis_size("tp")
    capacity, quarter = x_old.shape
    width = quarter * tp_count
    tokens = seq_count * capacity // 2
    own = tokens // seq_count
    share = capacity // tp_count
    seq_index = lax.axis_index("seq")
    tp_index = lax.axis_index("tp")
    heads = w_query.shape[1] // HEAD
    kv_heads = w_key.shape[1] // HEAD
    scale = (width // (heads * tp_count)) ** (-0.5)
    if front_fits(seq_count, tp_count, heads, kv_heads, capacity):
        context, rows = front_phase(
            x_old, old_blocks, order, pre_gain, w_query, w_key, w_value, seq_count, tp_count, scale
        )
        return output_phase(
            context, w_out_t, rows, post_gain, new_blocks, seq_count, tp_count, heads
        )
    old_start = offsets(old_blocks)
    new_start = offsets(new_blocks)
    device_ids = jnp.arange(seq_count, dtype=jnp.int32)

    gathered = lax.all_gather(x_old, "seq", axis=0, tiled=True)

    def stored(row, count):
        row = jnp.minimum(row, tokens - count)
        shard = jnp.sum((old_start <= row).astype(jnp.int32)) - 1
        holder = jnp.sum(jnp.where(order == shard, device_ids, 0))
        begin = jnp.sum(jnp.where(device_ids == shard, old_start, 0))
        return lax.dynamic_slice_in_dim(gathered, holder * capacity + row - begin, count, 0)

    def shift(k):
        return [(i, (i + k) % tp_count) for i in range(tp_count)]

    def by_source(received):
        stack = jnp.stack(received)
        pieces = [
            lax.dynamic_index_in_dim(stack, lax.rem(tp_index - u + tp_count, tp_count), 0, False)
            for u in range(tp_count)
        ]
        return jnp.concatenate(pieces, axis=1)

    mine = jnp.concatenate(
        [stored(seq_index * own + at, BLOCK) for at in range(0, own, BLOCK)], axis=0
    )
    full_rows = by_source(
        [mine] + [lax.ppermute(mine, "tp", shift(k)) for k in range(1, tp_count)]
    )
    my_start = jnp.sum(jnp.where(device_ids == seq_index, new_start, 0))

    def slot_rows(place):
        return stored(my_start + place * share, share)

    residual = by_source(
        [slot_rows(tp_index)]
        + [
            lax.ppermute(slot_rows(lax.rem(tp_index + k, tp_count)), "tp", shift(k))
            for k in range(1, tp_count)
        ]
    )

    weights = lax.all_gather(
        jnp.concatenate([w_query, w_key, w_value], axis=1), "seq", axis=0, tiled=True
    )

    normed = rms_scale(full_rows.astype(jnp.float32), pre_gain).astype(jnp.bfloat16)
    normed, residual = lax.optimization_barrier((normed, residual))
    group = heads // kv_heads
    copies = seq_count // heads
    raw = jnp.dot(normed, weights, preferred_element_type=jnp.float32)

    half = HEAD // 2
    inverse = jnp.exp(jnp.arange(half, dtype=jnp.float32) * (-2.0 * math.log(10000.0) / HEAD))
    places = seq_index * own + jnp.arange(own, dtype=jnp.int32)
    angles = places.astype(jnp.float32)[:, None] * inverse[None, :]
    cosine, sine = jnp.cos(angles), jnp.sin(angles)

    def rotate(at):
        first = raw[:, at * HEAD : at * HEAD + half]
        second = raw[:, at * HEAD + half : (at + 1) * HEAD]
        return jnp.concatenate(
            [first * cosine - second * sine, second * cosine + first * sine], axis=-1
        )

    queries = [(rotate(h) * scale).astype(jnp.bfloat16) for h in range(heads)]
    keys = [rotate(heads + g).astype(jnp.bfloat16) for g in range(kv_heads)]
    values = [
        raw[:, (heads + kv_heads + g) * HEAD : (heads + kv_heads + g + 1) * HEAD].astype(
            jnp.bfloat16
        )
        for g in range(kv_heads)
    ]
    sent = jnp.stack(
        [
            jnp.stack([queries[s // copies], keys[s // copies // group], values[s // copies // group]])
            for s in range(seq_count)
        ]
    )
    came = lax.all_to_all(sent, "seq", 0, 0, tiled=True)
    context = attention(
        came[:, 0].reshape(tokens, HEAD),
        came[:, 1].reshape(tokens, HEAD),
        came[:, 2].reshape(tokens, HEAD),
    )
    return output_phase(
        context, w_out_t, residual, post_gain, new_blocks, seq_count, tp_count, heads
    )


def solution(mesh):
    placed = (
        P("seq", "tp"),
        P(),
        P(),
        P(),
        P(),
        P(),
        P("seq", "tp"),
        P("seq", "tp"),
        P("seq", "tp"),
        P("seq", "tp"),
    )
    return jax.shard_map(
        per_device, mesh=mesh, in_specs=placed, out_specs=P(("seq", "tp"), None), check_vma=False
    )
```

```python
import functools
import math

import jax
import jax.numpy as jnp
import numpy as np
from jax import lax
from jax.experimental import pallas as pl
from jax.experimental.pallas import tpu as pltpu
from jax.sharding import PartitionSpec as P

HEAD = 128
BLOCK = 128
EPS = 1e-06
LAG = 4


def offsets(blocks):
    return (jnp.cumsum(blocks) - blocks) * BLOCK


def rms_scale(values, gain):
    return values * lax.rsqrt(jnp.mean(values * values, axis=-1, keepdims=True) + EPS) * gain


def attention_kernel(rows, span, q_ref, k_ref, v_ref, out_ref):
    first = pl.program_id(0) * rows
    query = q_ref[...]

    def step(at, carry, masked):
        numer, denom = carry
        start = pl.multiple_of(at * span, span)
        score = lax.dot_general(
            query,
            k_ref[pl.ds(start, span), :],
            (((1,), (1,)), ((), ())),
            preferred_element_type=jnp.float32,
        )
        weight = jnp.exp(50.0 * jnp.tanh(score * (1.0 / 50.0)))
        if masked:
            places = first + lax.broadcasted_iota(jnp.int32, weight.shape, 0)
            keys = start + lax.broadcasted_iota(jnp.int32, weight.shape, 1)
            weight = jnp.where(keys <= places, weight, 0.0)
        denom = denom + jnp.sum(weight, axis=1, keepdims=True)
        numer = numer + jnp.dot(
            weight.astype(jnp.bfloat16),
            v_ref[pl.ds(start, span), :],
            preferred_element_type=jnp.float32,
        )
        return numer, denom

    whole = first // span
    state = (jnp.zeros((rows, HEAD), jnp.float32), jnp.zeros((rows, 1), jnp.float32))
    state = lax.fori_loop(0, whole, lambda at, c: step(at, c, False), state)
    numer, denom = step(whole, state, True)
    out_ref[...] = (numer / denom).astype(out_ref.dtype)


def attention(query, key, value):
    tokens = query.shape[0]
    rows, span = 256, 512
    return pl.pallas_call(
        functools.partial(attention_kernel, rows, span),
        grid=(tokens // rows,),
        in_specs=[
            pl.BlockSpec((rows, HEAD), lambda i: (i, 0)),
            pl.BlockSpec((tokens, HEAD), lambda i: (0, 0)),
            pl.BlockSpec((tokens, HEAD), lambda i: (0, 0)),
        ],
        out_specs=pl.BlockSpec((rows, HEAD), lambda i: (i, 0)),
        out_shape=jax.ShapeDtypeStruct((tokens, HEAD), jnp.bfloat16),
        cost_estimate=pl.CostEstimate(
            flops=3 * tokens * tokens * HEAD,
            bytes_accessed=8 * tokens * HEAD,
            transcendentals=tokens * tokens,
        ),
    )(query, key, value)


MESH = pl.DeviceIdType.MESH


def arrangements(seq_count):
    found = []
    for second in range(1, seq_count + 1):
        for third in range(1, second + 1):
            fourth = seq_count - second - third
            if 1 <= fourth <= third:
                found.append((seq_count, second, third, fourth))
    return found


def layer_windows(seq_count, tp_count, per_block):
    first, last = [], []
    for layer in range(tp_count):
        starts, ends = [], []
        for counts in arrangements(seq_count):
            begin = sum(counts[u // per_block] for u in range(layer))
            starts.append(begin)
            ends.append(begin + counts[layer // per_block])
        first.append(min(starts))
        last.append(max(ends))
    return first, last


def pick(index, values):
    result = jnp.int32(values[0])
    for k in range(1, len(values)):
        result = jnp.where(index == k, jnp.int32(values[k]), result)
    return result


def flipped(index, mask):
    result = index
    bit = 1
    while bit <= mask:
        if mask & bit:
            result = result + bit - 2 * bit * lax.rem(index // bit, 2)
        bit *= 2
    return result


def output_kernel(
    heads,
    copies,
    seq_count,
    tp_count,
    share,
    first,
    last,
    scattered,
    perm_ref,
    place_ref,
    block_ref,
    context_ref,
    weight_ref,
    residual_ref,
    gain_ref,
    out_ref,
    full,
    partial,
    left_in,
    right_in,
    left_out,
    right_out,
    total,
    sent,
    came,
    gather_send,
    gather_recv,
    left_send,
    left_recv,
    right_send,
    right_recv,
    swap_send,
    swap_recv,
    old_sent,
    old_came,
    old_send,
    old_recv,
    weight,
    staged,
    weight_sem,
    staged_sem,
):
    seq_index = lax.axis_index("seq")
    tp_index = lax.axis_index("tp")
    places = partial.shape[0]
    depth = weight_ref.shape[0]
    half = partial.shape[1]
    core = lax.rem(seq_index, 2)
    partner = seq_index + 1 - 2 * core
    shared = copies == 1
    unit = 2 if shared else copies
    span = 2 * HEAD if shared else HEAD
    slot_index = seq_index // unit
    chunks = full.shape[0]
    per_chunk = places // chunks

    barrier = pltpu.get_barrier_semaphore()
    for k in range(1, seq_count):
        pl.semaphore_signal(
            barrier,
            inc=1,
            device_id=(lax.rem(seq_index + k, seq_count), tp_index),
            device_id_type=MESH,
        )

    @pl.when(tp_index > 0)
    def _():
        pl.semaphore_signal(
            barrier, inc=1, device_id=(seq_index, tp_index - 1), device_id_type=MESH
        )

    @pl.when(tp_index < tp_count - 1)
    def _():
        pl.semaphore_signal(
            barrier, inc=1, device_id=(seq_index, tp_index + 1), device_id_type=MESH
        )

    neighbours = jnp.where(tp_index > 0, 1, 0) + jnp.where(tp_index < tp_count - 1, 1, 0)
    pl.semaphore_wait(barrier, seq_count - 1 + neighbours)

    bits = (seq_count // unit).bit_length() - 1
    order = list(range(chunks))[::-1]
    head = seq_index // copies
    own_columns = pl.ds(pl.multiple_of(head * HEAD, HEAD), HEAD)

    def staged_copy(chunk):
        return pltpu.make_async_remote_copy(
            src_ref=staged.at[chunk],
            dst_ref=full.at[chunk, :, own_columns],
            send_sem=staged_sem.at[0, chunk],
            recv_sem=staged_sem.at[1, chunk],
            device_id=(partner, tp_index),
            device_id_type=MESH,
        )

    own_rows = pl.ds(pl.multiple_of(core * depth, depth), depth)
    weight_copy = pltpu.make_async_remote_copy(
        src_ref=weight_ref,
        dst_ref=weight.at[own_rows],
        send_sem=weight_sem.at[0],
        recv_sem=weight_sem.at[1],
        device_id=(partner, tp_index),
        device_id_type=MESH,
    )

    for chunk in order:
        for at in range(per_chunk):
            source = perm_ref[chunk * per_chunk + at]
            rows = slice(at * half, (at + 1) * half)
            full[chunk, rows, own_columns] = context_ref[source, core]
            if shared:
                staged[chunk, rows] = context_ref[source, 1 - core]
        if shared:
            staged_copy(chunk).start()
    weight_copy.start()

    def dims(chunk):
        outer = list(range(bits))
        return outer[::-1] if chunk % 2 else outer

    def gather_copy(chunk, bit, combo, to_me):
        slot = flipped(slot_index, (combo ^ (1 << bit)) if to_me else combo)
        view = full.at[chunk, :, pl.ds(pl.multiple_of(slot * span, span), span)]
        return pltpu.make_async_remote_copy(
            src_ref=view,
            dst_ref=view,
            send_sem=gather_send.at[chunk, bit, combo],
            recv_sem=gather_recv.at[chunk, bit, combo],
            device_id=(flipped(seq_index, unit << bit), tp_index),
            device_id_type=MESH,
        )

    def steps(chunk):
        held = [0]
        for bit in dims(chunk):
            yield bit, list(held)
            held = held + [c ^ (1 << bit) for c in held]

    def offer(at):
        if at < chunks:
            if shared:
                staged_copy(order[at]).wait_recv()
            for bit, _ in steps(order[at]):
                gather_copy(order[at], bit, 0, False).start()

    offer(0)
    weight[own_rows] = weight_ref[...]
    total[...] = jnp.zeros_like(total)

    def relay(at):
        chunk = order[at]
        stages = list(steps(chunk))
        for level, (bit, held) in enumerate(stages):
            for combo in held:
                gather_copy(chunk, bit, combo, True).wait_recv()
                for later, _ in stages[level + 1 :]:
                    gather_copy(chunk, later, combo ^ (1 << bit), False).start()
            if level == 0:
                offer(at + 1)

    def multiply(chunk):
        product = lax.dot_general(
            full[chunk],
            weight[...],
            (((1,), (1,)), ((), ())),
            preferred_element_type=jnp.float32,
        ).astype(jnp.bfloat16)
        for at in range(per_chunk):
            partial[chunk * per_chunk + at] = product[at * half : (at + 1) * half]

    left_has = jnp.where(tp_index < tp_count - 1, pick(tp_index, last), 0)
    left_gives = pick(tp_index, [0] + last[:-1])
    right_has = jnp.where(tp_index > 0, pick(tp_index, first), places)
    right_gives = pick(tp_index, first[1:] + [places])

    def line_copy(place, source, landing, send, recv, step):
        return pltpu.make_async_remote_copy(
            src_ref=source.at[place],
            dst_ref=landing.at[place],
            send_sem=send.at[place],
            recv_sem=recv.at[place],
            device_id=(seq_index, tp_index + step),
            device_id_type=MESH,
        )

    def flow(place, has, gives, source, landing, send, recv, step):
        @pl.when(has)
        def _():
            line_copy(place, source, landing, send, recv, step).wait_recv()

        @pl.when(jnp.logical_and(has, gives))
        def _():
            source[place] = (
                partial[place].astype(jnp.float32) + landing[place].astype(jnp.float32)
            ).astype(jnp.bfloat16)

        @pl.when(jnp.logical_and(jnp.logical_not(has), gives))
        def _():
            source[place] = partial[place]

        @pl.when(gives)
        def _():
            line_copy(place, source, landing, send, recv, step).start()

    def swap_copy(other, mine, at):
        return pltpu.make_async_remote_copy(
            src_ref=sent.at[other],
            dst_ref=came.at[mine],
            send_sem=swap_send.at[at],
            recv_sem=swap_recv.at[at],
            device_id=(other, tp_index),
            device_id_type=MESH,
        )

    def line_step(at, carry):
        passed = at - LAG * (tp_count - 1 - tp_index)
        place = places - 1 - passed
        valid = jnp.logical_and(passed >= 0, passed < places)
        has = jnp.logical_and(valid, place < left_has)
        gives = jnp.logical_and(valid, place < left_gives)
        flow(place, has, gives, left_out, left_in, left_send, left_recv, -1)
        ends = jnp.logical_and(
            jnp.logical_and(valid, tp_index == 0), place < seq_count
        )

        @pl.when(ends)
        def _():
            sent[place] = (
                partial[place].astype(jnp.float32) + left_in[place].astype(jnp.float32)
            ).astype(jnp.bfloat16)

            @pl.when(place == seq_index)
            def _():
                came[place] = sent[place]

            @pl.when(place != seq_index)
            def _():
                swap_copy(
                    place, seq_index, lax.rem(place + seq_count - seq_index, seq_count)
                ).start()

        passed = at - LAG * tp_index
        place = places - 1 - passed
        valid = jnp.logical_and(passed >= 0, passed < places)
        has = jnp.logical_and(valid, place >= right_has)
        gives = jnp.logical_and(valid, place >= right_gives)
        flow(place, has, gives, right_out, right_in, right_send, right_recv, 1)
        return carry

    def old_copy(other, mine, at):
        return pltpu.make_async_remote_copy(
            src_ref=old_sent.at[other],
            dst_ref=old_came.at[mine],
            send_sem=old_send.at[at],
            recv_sem=old_recv.at[at],
            device_id=(other, tp_index),
            device_id_type=MESH,
        )

    for at, chunk in enumerate(order):
        relay(at)
        if at == 0:
            weight_from = pltpu.make_async_remote_copy(
                src_ref=weight_ref,
                dst_ref=weight.at[pl.ds(pl.multiple_of((1 - core) * depth, depth), depth)],
                send_sem=weight_sem.at[0],
                recv_sem=weight_sem.at[1],
                device_id=(partner, tp_index),
                device_id_type=MESH,
            )
            weight_from.wait_recv()
        multiply(chunk)
        if scattered and at == chunks - 1:
            for j in range(seq_count):
                old_sent[j] = residual_ref[block_ref[j]]
            for k in range(1, seq_count):
                old_copy(lax.rem(seq_index + k, seq_count), seq_index, k).start()
            old_came[seq_index] = old_sent[seq_index]
        lax.fori_loop(at * per_chunk, (at + 1) * per_chunk, line_step, 0)
    lax.fori_loop(places, places + LAG * (tp_count - 1), line_step, 0)

    def sum_step(place, carry):
        value = partial[place].astype(jnp.float32) + right_in[place].astype(jnp.float32)

        @pl.when(place < left_has)
        def _():
            total[place] = (value + left_in[place].astype(jnp.float32)).astype(jnp.bfloat16)

        @pl.when(place >= left_has)
        def _():
            total[place] = value.astype(jnp.bfloat16)

        return carry

    @pl.when(tp_index > 0)
    def _():
        lax.fori_loop(pick(tp_index, first), pick(tp_index, last), sum_step, 0)
        for j in range(seq_count):
            sent[j] = total[place_ref[j]]
        for k in range(1, seq_count):
            swap_copy(lax.rem(seq_index + k, seq_count), seq_index, k).start()
        came[seq_index] = sent[seq_index]

    for k in range(1, seq_count):
        swap_copy(
            lax.rem(seq_index + k, seq_count),
            lax.rem(seq_index + seq_count - k, seq_count),
            k,
        ).wait_recv()

    if scattered:
        for k in range(1, seq_count):
            old_copy(
                lax.rem(seq_index + k, seq_count),
                lax.rem(seq_index + seq_count - k, seq_count),
                k,
            ).wait_recv()
    wide = 2 * depth
    for side in range(2):
        square = jnp.zeros((half, 1), jnp.float32)
        for c in range(seq_count // 2):
            piece = came[2 * c + side].astype(jnp.float32)
            square = square + jnp.sum(piece * piece, axis=1, keepdims=True)
        factor = lax.rsqrt(square * (1.0 / (depth * seq_count)) + EPS)
        rows = slice(side * half, (side + 1) * half)
        for c in range(seq_count // 2):
            columns = slice(c * wide, (c + 1) * wide)
            old = old_came[2 * c + side] if scattered else residual_ref[rows, columns]
            value = old.astype(jnp.float32) + (
                came[2 * c + side].astype(jnp.float32) * factor * gain_ref[:, columns]
            )
            out_ref[rows, columns] = value.astype(jnp.bfloat16)

    for k in range(1, seq_count):
        swap_copy(lax.rem(seq_index + k, seq_count), seq_index, k).wait_send()
    if scattered:
        for k in range(1, seq_count):
            old_copy(lax.rem(seq_index + k, seq_count), seq_index, k).wait_send()
    weight_copy.wait_send()
    for chunk in range(chunks):
        if shared:
            staged_copy(chunk).wait_send()
        for bit, held in steps(chunk):
            for combo in held:
                gather_copy(chunk, bit, combo, False).wait_send()

    def drain(place, carry):
        @pl.when(place < left_gives)
        def _():
            line_copy(place, left_out, left_in, left_send, left_recv, -1).wait_send()

        @pl.when(place >= right_gives)
        def _():
            line_copy(place, right_out, right_in, right_send, right_recv, 1).wait_send()

        return carry

    lax.fori_loop(0, places, drain, 0)


def front_kernel(
    seq_count,
    tp_count,
    group,
    scale,
    blocks_ref,
    order_ref,
    new_ref,
    x_ref,
    gain_ref,
    query_ref,
    key_ref,
    value_ref,
    angle_ref,
    output_ref,
    out_ref,
    context,
    x_out,
    q_buf,
    kv_buf,
    near,
    send_a,
    send_b,
    far,
    line,
    twin,
    weight,
    normed,
    scale_row,
    scale_all,
    scale_column,
    first_out,
    first_in,
    second_out,
    second_in,
    kept,
    core_sem,
    weight_sem,
    stage_sem,
    line_send,
    line_recv,
    plane_send,
    plane_recv,
    twin_sem,
    stat_sem,
    factor_sem,
    first_sem,
    second_sem,
    kv_sem,
    full,
    staged,
    out_weight,
    partial,
    left_in,
    right_in,
    left_out,
    right_out,
    total,
    sent,
    came,
    old_sent,
    old_came,
    staged_sem,
    out_weight_sem,
    gather_sem,
    left_sem,
    right_sem,
    swap_sem,
    old_sem,
):
    seq_index = lax.axis_index("seq")
    tp_index = lax.axis_index("tp")
    chip = seq_index // 2
    core = lax.rem(seq_index, 2)
    partner = seq_index + 1 - 2 * core
    slots = x_ref.shape[0]
    chips = seq_count // 2
    each = line.shape[1]
    half = line.shape[2]
    quarter = line.shape[3]
    depth = query_ref.shape[0]
    pair = 2 * HEAD

    barrier = pltpu.get_barrier_semaphore()
    for k in range(1, seq_count):
        other = lax.rem(seq_index + k, seq_count)
        pl.semaphore_signal(barrier, inc=1, device_id=(other, tp_index), device_id_type=MESH)
    for k in range(1, tp_count):
        other = lax.rem(tp_index + k, tp_count)
        pl.semaphore_signal(barrier, inc=1, device_id=(seq_index, other), device_id_type=MESH)

    def remote(source, target, sems, at, seq, tp):
        return pltpu.make_async_remote_copy(
            src_ref=source,
            dst_ref=target,
            send_sem=sems[0].at[at],
            recv_sem=sems[1].at[at],
            device_id=(seq, tp),
            device_id_type=MESH,
        )

    core_sems = (core_sem.at[0], core_sem.at[1])

    def swap_slots(holder):
        return remote(
            x_ref.at[:, 1 - core],
            near.at[pl.ds(slots * holder, slots)],
            core_sems,
            0,
            partner,
            tp_index,
        )

    def lanes(head, count=1):
        return pl.ds(pl.multiple_of(head * HEAD, HEAD), count * HEAD)

    def weight_copy(source, column, target, at, holder):
        return remote(
            source.at[:, lanes(column)],
            weight.at[pl.ds(pl.multiple_of(holder * depth, depth), depth), lanes(target)],
            (weight_sem.at[0], weight_sem.at[1]),
            at,
            partner,
            tp_index,
        )

    pl.semaphore_wait(barrier, seq_count - 1 + tp_count - 1)
    swap_slots(core).start()
    for slot in range(slots):
        near[slots * core + slot] = x_ref[slot, core]

    starts, counts, holders = [], [], []
    begin = jnp.int32(0)
    for k in range(seq_count):
        starts.append(begin)
        counts.append(blocks_ref[k])
        begin = begin + blocks_ref[k]
        holder = jnp.int32(0)
        for place in range(1, seq_count):
            holder = holder + jnp.where(order_ref[place] == k, jnp.int32(place), jnp.int32(0))
        holders.append(holder)

    def found(block):
        at = jnp.int32(0)
        for k in range(seq_count):
            inside = jnp.logical_and(starts[k] <= block, block < starts[k] + counts[k])
            at = at + jnp.where(inside, holders[k] * slots + block - starts[k], jnp.int32(0))
        return at // (2 * slots), lax.rem(at, 2 * slots)

    first_chip = jnp.where(core == 0, flipped(chip, 1), flipped(chip, 2))
    second_chip = jnp.where(core == 0, flipped(chip, 2), flipped(chip, 1))
    cross_chip = flipped(chip, 3)
    swap_slots(1 - core).wait_recv()

    stage_sems = (stage_sem.at[0], stage_sem.at[1])
    table_a = []
    for at in range(2 * each):
        target = first_chip if at < each else cross_chip
        owner, index = found(chips * (at % each) + target)
        table_a.append(jnp.where(owner == chip, index, 0))
    across_first = list(range(each, 2 * each)) + list(range(each))
    for at in across_first:
        send_a[at] = near[table_a[at]]
        remote(
            send_a.at[at], far.at[at], stage_sems, at, 2 * first_chip + core, tp_index
        ).start()

    for c in range(chips):
        weight_copy(query_ref, 2 * c + 1 - core, 2 * c, 2 * c, core).start()

        @pl.when(core == 0)
        def _():
            weight_copy(value_ref, c, 2 * c + 1, 2 * c + 1, core).start()

        @pl.when(core == 1)
        def _():
            weight_copy(key_ref, c, 2 * c + 1, 2 * c + 1, core).start()

    def output_copy(holder):
        return remote(
            output_ref,
            out_weight.at[pl.ds(pl.multiple_of(holder * depth, depth), depth)],
            (out_weight_sem.at[0], out_weight_sem.at[1]),
            0,
            partner,
            tp_index,
        )

    output_copy(core).start()
    own_rows = pl.ds(pl.multiple_of(core * depth, depth), depth)
    out_weight[own_rows] = output_ref[...]
    for c in range(chips):
        weight[own_rows, pl.ds(2 * c * HEAD, HEAD)] = query_ref[:, lanes(2 * c + core)]

        @pl.when(core == 0)
        def _():
            weight[own_rows, pl.ds((2 * c + 1) * HEAD, HEAD)] = key_ref[
                :, pl.ds(c * HEAD, HEAD)
            ]

        @pl.when(core == 1)
        def _():
            weight[own_rows, pl.ds((2 * c + 1) * HEAD, HEAD)] = value_ref[
                :, pl.ds(c * HEAD, HEAD)
            ]

    def arrive_a(at):
        remote(
            send_a.at[at], far.at[at], stage_sems, at, 2 * first_chip + core, tp_index
        ).wait_recv()

    both = 2 * slots
    for at in range(each, 2 * each):
        arrive_a(at)
        near[both + at] = far[at]
    for at in range(each):
        owner, index = found(chips * at + second_chip)
        send_b[at] = near[jnp.where(owner == chip, index, both + each + at)]
        remote(
            send_b.at[at],
            far.at[2 * each + at],
            stage_sems,
            2 * each + at,
            2 * second_chip + core,
            tp_index,
        ).start()
    for at in range(each):
        arrive_a(at)
        near[both + at] = far[at]
    for at in range(each):
        owner, index = found(chips * at + chip)
        near[both + 2 * each + at] = near[jnp.where(owner == chip, index, both + at)]
    for at in range(each):
        remote(
            send_b.at[at],
            far.at[2 * each + at],
            stage_sems,
            2 * each + at,
            2 * second_chip + core,
            tp_index,
        ).wait_recv()
        near[both + 3 * each + at] = far[2 * each + at]
    for at in range(each):
        owner, _ = found(chips * at + chip)
        local = jnp.logical_or(owner == chip, owner == first_chip)
        line[tp_index, at] = near[
            jnp.where(local, both + 2 * each + at, both + 3 * each + at)
        ]

    def line_copy(layer, at, step):
        view = line.at[layer, at]
        return pltpu.make_async_remote_copy(
            src_ref=view,
            dst_ref=view,
            send_sem=line_send.at[(step + 1) // 2, layer, at],
            recv_sem=line_recv.at[layer, at],
            device_id=(seq_index, tp_index + step),
            device_id_type=MESH,
        )

    def plane_copy(layer, at, holder):
        return pltpu.make_async_remote_copy(
            src_ref=line.at[layer, at],
            dst_ref=x_out.at[chips * at + holder],
            send_sem=plane_send.at[layer, at],
            recv_sem=plane_recv.at[chips * at + holder],
            device_id=(2 * layer + core, tp_index),
            device_id_type=MESH,
        )

    def twin_copy(block):
        return remote(
            x_out.at[block],
            twin.at[block],
            (twin_sem.at[0], twin_sem.at[1]),
            block,
            partner,
            tp_index,
        )

    def guarded(condition, action):
        @pl.when(condition)
        def _():
            action()

    def forward(layer, at):
        @pl.when(layer == chip)
        def _():
            x_out[chips * at + chip] = line[layer, at]

        @pl.when(layer != chip)
        def _():
            plane_copy(layer, at, chip).start()

    def own_step(at):
        guarded(tp_index > 0, lambda: line_copy(tp_index, at, -1).start())
        guarded(tp_index < tp_count - 1, lambda: line_copy(tp_index, at, 1).start())
        forward(tp_index, at)

    def hop_step(at, distance):
        @pl.when(tp_index >= distance)
        def _():
            layer = tp_index - distance
            line_copy(layer, at, 1).wait_recv()
            guarded(tp_index < tp_count - 1, lambda: line_copy(layer, at, 1).start())
            forward(layer, at)

        @pl.when(tp_index + distance < tp_count)
        def _():
            layer = tp_index + distance
            line_copy(layer, at, -1).wait_recv()
            guarded(tp_index > 0, lambda: line_copy(layer, at, -1).start())
            forward(layer, at)

    def plane_step(at):
        for c in range(chips):

            @pl.when(chip != c)
            def _():
                plane_copy(chip, at, c).wait_recv()

        for c in range(chips):
            twin_copy(chips * at + c).start()

    tiles = quarter // HEAD
    gain_at = pl.multiple_of(chip * quarter, HEAD)

    def normalize(source, block, holder, target):
        rows = pl.ds(pl.multiple_of((block // chips) * half, half), half)
        factor = scale_column[holder, rows, :]
        for tile in range(tiles):
            columns = slice(tile * HEAD, (tile + 1) * HEAD)
            values = source[block, :, columns].astype(jnp.float32)
            gains = gain_ref[:1, pl.ds(pl.multiple_of(gain_at + tile * HEAD, HEAD), HEAD)]
            normed[target[0], target[1], target[2], :, columns] = (
                values * factor * gains
            ).astype(jnp.bfloat16)

    bits = (1, 2)

    def first_copy(at, side):
        bit = bits[side]
        return pltpu.make_async_remote_copy(
            src_ref=first_out.at[at, side],
            dst_ref=first_in.at[at, side],
            send_sem=first_sem.at[0, at, side],
            recv_sem=first_sem.at[1, at, side],
            device_id=(2 * flipped(chip, bit) + core, tp_index),
            device_id_type=MESH,
        )

    def second_copy(at, side):
        bit = bits[1 - side]
        return pltpu.make_async_remote_copy(
            src_ref=second_out.at[at, side],
            dst_ref=second_in.at[at, side],
            send_sem=second_sem.at[0, at, side],
            recv_sem=second_sem.at[1, at, side],
            device_id=(2 * flipped(chip, bit) + core, tp_index),
            device_id_type=MESH,
        )

    def multiply_step(at):
        for side in range(2):
            for u in range(2):
                c = 2 * side + u
                block = chips * at + c
                twin_copy(block).wait_recv()
                normalize(x_out, block, 2 * c + core, (side, u, core))
                normalize(twin, block, 2 * c + 1 - core, (side, u, 1 - core))
            rows = normed[side].reshape(4 * half, quarter)

            def part(mask):
                target = flipped(chip, mask)
                return jnp.dot(
                    rows,
                    weight[:, lanes(2 * target, 2)],
                    preferred_element_type=jnp.float32,
                )

            first, second = bits[side], bits[1 - side]
            first_out[at, side, 0] = part(first).astype(jnp.bfloat16)
            first_out[at, side, 1] = part(3).astype(jnp.bfloat16)
            first_copy(at, side).start()
            kept[at, side, 0] = part(0)
            kept[at, side, 1] = part(second)

    def add_step(at):
        for side in range(2):
            first_copy(at, side).wait_recv()
            second_out[at, side] = (
                kept[at, side, 1] + first_in[at, side, 1].astype(jnp.float32)
            ).astype(jnp.bfloat16)
            second_copy(at, side).start()

    def kv_copy(kind, block):
        rows = pl.ds(pl.multiple_of(block * BLOCK, BLOCK), BLOCK)
        view = kv_buf.at[kind, rows, :]
        return remote(
            view, view, (kv_sem.at[0], kv_sem.at[1]), block, partner, tp_index
        )

    lane = lax.broadcasted_iota(jnp.int32, (BLOCK, HEAD), 1)

    def turned(values, rows):
        angles = angle_ref[rows, :]
        swapped = pltpu.roll(angles, HEAD // 2, 1)
        low = lane < HEAD // 2
        cosine = jnp.where(low, angles, swapped)
        sine = jnp.where(low, -swapped, angles)
        return values * cosine + pltpu.roll(values, HEAD // 2, 1) * sine

    def finish_step(at):
        for side in range(2):
            second_copy(at, side).wait_recv()
            for u in range(2):
                block = chips * at + 2 * side + u
                part = slice(u * BLOCK, (u + 1) * BLOCK)
                value = (
                    kept[at, side, 0, part]
                    + first_in[at, side, 0, part].astype(jnp.float32)
                    + second_in[at, side, part].astype(jnp.float32)
                )
                rows = pl.ds(pl.multiple_of(block * BLOCK, BLOCK), BLOCK)
                q_buf[rows, :] = (turned(value[:, :HEAD], rows) * scale).astype(jnp.bfloat16)

                @pl.when(core == 0)
                def _():
                    kv_buf[0, rows, :] = turned(value[:, HEAD:], rows).astype(jnp.bfloat16)

                @pl.when(core == 1)
                def _():
                    kv_buf[1, rows, :] = value[:, HEAD:].astype(jnp.bfloat16)

                kv_copy(core, block).start()

    span = chips * BLOCK
    sub = span // 2
    mask = lax.broadcasted_iota(jnp.int32, (sub, sub), 1) <= lax.broadcasted_iota(
        jnp.int32, (sub, sub), 0
    )

    def attend_step(at):
        for c in range(chips):
            kv_copy(1 - core, chips * at + c).wait_recv()

        def attend(query, start, count, carry, masked):
            keys = pl.ds(pl.multiple_of(start, sub), count)
            score = lax.dot_general(
                query,
                kv_buf[0, keys, :],
                (((1,), (1,)), ((), ())),
                preferred_element_type=jnp.float32,
            )
            part = jnp.exp2((50.0 / math.log(2.0)) * jnp.tanh(score * (1.0 / 50.0)))
            if masked:
                part = jnp.where(mask, part, 0.0)
            numer, denom = carry
            denom = denom + jnp.sum(part, axis=1, keepdims=True)
            numer = numer + jnp.dot(
                part.astype(jnp.bfloat16), kv_buf[1, keys, :], preferred_element_type=jnp.float32
            )
            return numer, denom

        for piece in range(2):
            begin = at * span + piece * sub
            rows = pl.ds(pl.multiple_of(begin, sub), sub)
            query = q_buf[rows, :]
            state = (jnp.zeros((sub, HEAD), jnp.float32), jnp.zeros((sub, 1), jnp.float32))
            state = lax.fori_loop(
                0, at, lambda n, carry: attend(query, n * span, span, carry, False), state
            )
            if piece:
                state = attend(query, at * span, sub, state, False)
            numer, denom = attend(query, begin, sub, state, True)
            value = (numer / denom).astype(jnp.bfloat16)
            place = chips * at + piece * (chips // 2)
            for u in range(chips // 2):
                for k in range(2):
                    low = u * BLOCK + k * half
                    context[place + u, k] = value[low : low + half]
        for c in range(chips):
            rows = slice(c * half, (c + 1) * half)
            full[at, rows, own_columns] = context[chips * at + c, core]
            staged[at, rows] = context[chips * at + c, 1 - core]
        staged_copy(at).start()
        staged_copy(at).wait_recv()
        for bit in (0, 1):
            gather_copy(at, bit, 0, False).start()

    own_columns = lanes(seq_index)

    def staged_copy(at):
        return remote(
            staged.at[at],
            full.at[at, :, own_columns],
            (staged_sem.at[0], staged_sem.at[1]),
            at,
            partner,
            tp_index,
        )

    def gather_copy(at, bit, combo, to_me):
        slot = flipped(chip, (combo ^ (1 << bit)) if to_me else combo)
        view = full.at[at, :, lanes(2 * slot, 2)]
        return pltpu.make_async_remote_copy(
            src_ref=view,
            dst_ref=view,
            send_sem=gather_sem.at[0, at, bit, combo // 2 + combo % 2],
            recv_sem=gather_sem.at[1, at, bit, combo // 2 + combo % 2],
            device_id=(2 * flipped(chip, 1 << bit) + core, tp_index),
            device_id_type=MESH,
        )

    def product_step(at):
        def relay(first_bit):
            second_bit = 1 - first_bit
            gather_copy(at, first_bit, 0, True).wait_recv()
            gather_copy(at, second_bit, 1 << first_bit, False).start()
            gather_copy(at, second_bit, 0, True).wait_recv()
            gather_copy(at, second_bit, 1 << first_bit, True).wait_recv()

        guarded(lax.rem(at, 2) == 0, lambda: relay(0))
        guarded(lax.rem(at, 2) == 1, lambda: relay(1))
        product = lax.dot_general(
            full[at], out_weight[...], (((1,), (1,)), ((), ())), preferred_element_type=jnp.float32
        ).astype(jnp.bfloat16)
        for c in range(chips):
            partial[chips * at + c] = product[c * half : (c + 1) * half]

    def down_copy(place, source, landing, sems, step):
        return remote(
            source.at[place],
            landing.at[place],
            (sems.at[0], sems.at[1]),
            place,
            seq_index,
            tp_index + step,
        )

    down = (left_out, left_in, left_sem, -1)
    up = (right_out, right_in, right_sem, 1)

    def flow(at, has, gives, way):
        def one(c, carry):
            place = chips * at + c

            @pl.when(has)
            def _():
                down_copy(place, *way).wait_recv()

                @pl.when(gives)
                def _():
                    way[0][place] = (
                        partial[place].astype(jnp.float32) + way[1][place].astype(jnp.float32)
                    ).astype(jnp.bfloat16)

            @pl.when(jnp.logical_and(jnp.logical_not(has), gives))
            def _():
                way[0][place] = partial[place]

            guarded(gives, lambda: down_copy(place, *way).start())
            return carry

        lax.fori_loop(0, chips, one, 0)

    def left_step(at, hop):
        @pl.when(tp_index == tp_count - 1 - hop)
        def _():
            flow(at, tp_index < tp_count - 1, tp_index > 0, down)

    def right_step(at, hop):
        @pl.when(tp_index == hop)
        def _():
            flow(at, tp_index > 0, tp_index < tp_count - 1, up)

    def line_step(at, hop):
        left_step(at, hop)
        right_step(at, hop)

    def total_step(at):
        def one(c, carry):
            place = chips * at + c
            value = partial[place].astype(jnp.float32)

            @pl.when(tp_index == 0)
            def _():
                total[place] = (value + left_in[place].astype(jnp.float32)).astype(jnp.bfloat16)

            @pl.when(tp_index == tp_count - 1)
            def _():
                total[place] = (value + right_in[place].astype(jnp.float32)).astype(jnp.bfloat16)

            @pl.when(jnp.logical_and(tp_index > 0, tp_index < tp_count - 1))
            def _():
                total[place] = (
                    value
                    + left_in[place].astype(jnp.float32)
                    + right_in[place].astype(jnp.float32)
                ).astype(jnp.bfloat16)

            return carry

        lax.fori_loop(0, chips, one, 0)

    def stat_copy(layer_from, layer_to):
        return pltpu.make_async_remote_copy(
            src_ref=scale_row.at[layer_from],
            dst_ref=scale_row.at[layer_from],
            send_sem=stat_sem.at[0, layer_to],
            recv_sem=stat_sem.at[1, layer_from],
            device_id=(seq_index, layer_to),
            device_id_type=MESH,
        )

    def factor_copy(holder, other):
        return pltpu.make_async_remote_copy(
            src_ref=scale_all.at[holder],
            dst_ref=scale_all.at[holder],
            send_sem=factor_sem.at[0, other],
            recv_sem=factor_sem.at[1, holder],
            device_id=(other, tp_index),
            device_id_type=MESH,
        )

    own_step(0)
    squares = []
    for at in range(each):
        values = line[tp_index, at].astype(jnp.float32)
        squares.append(jnp.sum(values * values, axis=1, keepdims=True))
    column = jnp.broadcast_to(jnp.concatenate(squares, axis=0), (each * half, HEAD))
    scale_row[tp_index] = jnp.transpose(column)[:8, :]
    for k in range(1, tp_count):
        stat_copy(tp_index, lax.rem(tp_index + k, tp_count)).start()
    for c in range(2 * chips):
        weight_copy(query_ref, 0, 0, c, 1 - core).wait_recv()
    for k in range(1, tp_count):
        other = lax.rem(tp_index + k, tp_count)
        stat_copy(other, tp_index).wait_recv()
    square = scale_row[0]
    for k in range(1, tp_count):
        square = square + scale_row[k]
    scale_all[seq_index] = lax.rsqrt(square * (1.0 / (quarter * tp_count)) + EPS)
    for k in range(1, seq_count):
        factor_copy(seq_index, lax.rem(seq_index + k, seq_count)).start()

    def steps(i, carry):
        for lag, action in (
            (0, lambda at: guarded(at > 0, lambda: own_step(at))),
            (1, lambda at: hop_step(at, 1)),
            (2, lambda at: hop_step(at, 2)),
            (3, lambda at: hop_step(at, 3)),
            (4, plane_step),
            (5, multiply_step),
            (6, add_step),
            (7, finish_step),
            (8, attend_step),
            (9, product_step),
            (9, lambda at: line_step(at, 0)),
            (10, lambda at: line_step(at, 1)),
            (11, lambda at: line_step(at, 2)),
            (12, lambda at: line_step(at, 3)),
            (12, total_step),
        ):
            at = i - lag

            @pl.when(jnp.logical_and(at >= 0, at < each))
            def _():
                action(at)

        return carry

    lax.fori_loop(0, 5, steps, 0)
    for k in range(1, seq_count):
        other = lax.rem(seq_index + k, seq_count)
        factor_copy(other, seq_index).wait_recv()
    for s in range(seq_count):
        scale_column[s] = jnp.transpose(
            jnp.broadcast_to(scale_all[s, :1, :], (HEAD, each * half))
        )
    lax.fori_loop(5, 9, steps, 0)
    output_copy(1 - core).wait_recv()
    lax.fori_loop(9, each + 9, steps, 0)

    starts_new = []
    begin = jnp.int32(0)
    for j in range(seq_count):
        starts_new.append(jnp.minimum(begin + tp_index, each * chips - 1))
        begin = begin + new_ref[j]

    def swap(sources, landings, sems, other, mine, k):
        return remote(
            sources.at[other], landings.at[mine], (sems.at[0], sems.at[1]), k, other, tp_index
        )

    def rows_of(k):
        return lax.rem(seq_index + k, seq_count)

    old = (old_sent, old_came, old_sem)
    new = (sent, came, swap_sem)

    def send_all(ways, values):
        for j in range(seq_count):
            ways[0][j] = values[starts_new[j]]
        for k in range(1, seq_count):
            swap(*ways, rows_of(k), seq_index, k).start()
        ways[1][seq_index] = ways[0][seq_index]

    send_all(old, x_out)
    lax.fori_loop(each + 9, each + 12, steps, 0)
    send_all(new, total)
    for ways in (old, new):
        for k in range(1, seq_count):
            swap(*ways, rows_of(k), rows_of(seq_count - k), k).wait_recv()
    for side in range(2):
        square = jnp.zeros((half, 1), jnp.float32)
        for c in range(chips):
            piece = came[2 * c + side].astype(jnp.float32)
            square = square + jnp.sum(piece * piece, axis=1, keepdims=True)
        factor = lax.rsqrt(square * (1.0 / (quarter * tp_count)) + EPS)
        rows = slice(side * half, (side + 1) * half)
        for c in range(chips):
            columns = slice(c * quarter, (c + 1) * quarter)
            value = old_came[2 * c + side].astype(jnp.float32) + (
                came[2 * c + side].astype(jnp.float32) * factor * gain_ref[1:2, columns]
            )
            out_ref[rows, columns] = value.astype(jnp.bfloat16)

    swap_slots(core).wait_send()
    output_copy(core).wait_send()
    for ways in (old, new):
        for k in range(1, seq_count):
            swap(*ways, rows_of(k), seq_index, k).wait_send()
    for c in range(2 * chips):
        weight_copy(query_ref, 0, 0, c, core).wait_send()
    for at in range(2 * each):
        remote(
            send_a.at[at], far.at[at], stage_sems, at, 2 * first_chip + core, tp_index
        ).wait_send()
    for at in range(each):
        remote(
            send_b.at[at],
            far.at[2 * each + at],
            stage_sems,
            2 * each + at,
            2 * second_chip + core,
            tp_index,
        ).wait_send()
    for k in range(1, tp_count):
        stat_copy(tp_index, lax.rem(tp_index + k, tp_count)).wait_send()
    for k in range(1, seq_count):
        factor_copy(seq_index, lax.rem(seq_index + k, seq_count)).wait_send()

    def drain(at, carry):
        for layer in range(tp_count):
            right = jnp.logical_and(tp_index >= layer, tp_index < tp_count - 1)
            guarded(right, lambda: line_copy(layer, at, 1).wait_send())
            left = jnp.logical_and(tp_index <= layer, tp_index > 0)
            guarded(left, lambda: line_copy(layer, at, -1).wait_send())
            guarded(chip != layer, lambda: plane_copy(layer, at, chip).wait_send())
        for side in range(2):
            first_copy(at, side).wait_send()
            second_copy(at, side).wait_send()
        for c in range(chips):
            twin_copy(chips * at + c).wait_send()
            kv_copy(core, chips * at + c).wait_send()
            guarded(tp_index > 0, lambda: down_copy(chips * at + c, *down).wait_send())
            guarded(
                tp_index < tp_count - 1, lambda: down_copy(chips * at + c, *up).wait_send()
            )
        staged_copy(at).wait_send()
        gather_copy(at, 0, 0, False).wait_send()
        gather_copy(at, 1, 0, False).wait_send()
        guarded(lax.rem(at, 2) == 0, lambda: gather_copy(at, 1, 1, False).wait_send())
        guarded(lax.rem(at, 2) == 1, lambda: gather_copy(at, 0, 2, False).wait_send())
        return carry

    lax.fori_loop(0, each, drain, 0)


def front_fits(seq_count, tp_count, heads, kv_heads, capacity):
    return (
        heads == seq_count == 8
        and 2 * kv_heads == heads
        and tp_count == 4
        and capacity == 4 * BLOCK
    )


def front_phase(
    x_old,
    old_blocks,
    new_blocks,
    order,
    pre_gain,
    post_gain,
    w_query,
    w_key,
    w_value,
    w_out_t,
    seq_count,
    tp_count,
    scale,
):
    capacity, quarter = x_old.shape
    depth = w_query.shape[0]
    slots = capacity // BLOCK
    half = BLOCK // 2
    tokens = seq_count * capacity // 2
    chips = seq_count // 2
    each = tokens // BLOCK // chips
    group = w_query.shape[1] // w_key.shape[1]
    angles = (
        np.arange(tokens, dtype=np.float32)[:, None]
        * np.exp(
            np.arange(HEAD // 2, dtype=np.float32) * np.float32(-2.0 * math.log(10000.0) / HEAD)
        )[None, :]
    )
    table = np.concatenate([np.cos(angles), np.sin(angles)], axis=1).astype(np.float32)
    bf16, f32 = jnp.bfloat16, jnp.float32
    piece = (half, quarter)
    dma = pltpu.SemaphoreType.DMA
    vmem = pl.BlockSpec(memory_space=pltpu.VMEM)
    smem = pl.BlockSpec(memory_space=pltpu.SMEM)
    square = (2 * BLOCK, 2 * HEAD)
    heads = seq_count
    blocks = pltpu.VMEM((each * chips,) + piece, bf16)
    owners = pltpu.VMEM((seq_count,) + piece, bf16)
    result = pl.pallas_call(
        functools.partial(front_kernel, seq_count, tp_count, group, scale),
        out_shape=jax.ShapeDtypeStruct((BLOCK, quarter * tp_count), bf16),
        in_specs=[smem] * 3 + [vmem] * 7,
        out_specs=vmem,
        scratch_shapes=[
            pltpu.VMEM((each * chips, 2, half, HEAD), bf16),
            blocks,
            pltpu.VMEM((tokens, HEAD), bf16),
            pltpu.VMEM((2, tokens, HEAD), bf16),
            pltpu.VMEM((2 * slots + 4 * each,) + piece, bf16),
            pltpu.VMEM((2 * each,) + piece, bf16),
            pltpu.VMEM((each,) + piece, bf16),
            pltpu.VMEM((3 * each,) + piece, bf16),
            pltpu.VMEM((tp_count, each) + piece, bf16),
            pltpu.VMEM((each * chips,) + piece, bf16),
            pltpu.VMEM((2 * depth, 2 * chips * HEAD), bf16),
            pltpu.VMEM((2, 2, 2) + piece, bf16),
            pltpu.VMEM((tp_count, 8, each * half), f32),
            pltpu.VMEM((seq_count, 8, each * half), f32),
            pltpu.VMEM((seq_count, each * half, HEAD), f32),
            pltpu.VMEM((each, 2, 2) + square, bf16),
            pltpu.VMEM((each, 2, 2) + square, bf16),
            pltpu.VMEM((each, 2) + square, bf16),
            pltpu.VMEM((each, 2) + square, bf16),
            pltpu.VMEM((each, 2, 2) + square, f32),
            dma((2, 1)),
            dma((2, 2 * chips)),
            dma((2, 3 * each)),
            dma((2, tp_count, each)),
            dma((tp_count, each)),
            dma((tp_count, each)),
            dma((each * chips,)),
            dma((2, each * chips)),
            dma((2, tp_count)),
            dma((2, seq_count)),
            dma((2, each, 2)),
            dma((2, each, 2)),
            dma((2, each * chips)),
            pltpu.VMEM((each, chips * half, heads * HEAD), bf16),
            pltpu.VMEM((each, chips * half, HEAD), bf16),
            pltpu.VMEM((2 * depth, heads * HEAD), bf16),
            blocks,
            blocks,
            blocks,
            blocks,
            blocks,
            blocks,
            owners,
            owners,
            owners,
            owners,
            dma((2, each)),
            dma((2, 1)),
            dma((2, each, 2, 2)),
            dma((2, each * chips)),
            dma((2, each * chips)),
            dma((2, seq_count)),
            dma((2, seq_count)),
        ],
        compiler_params=pltpu.CompilerParams(
            collective_id=1, has_side_effects=True, vmem_limit_bytes=67_043_328
        ),
        cost_estimate=pl.CostEstimate(
            flops=60_000_000_000, bytes_accessed=8 * tokens * depth, transcendentals=0
        ),
    )(
        old_blocks,
        order,
        new_blocks,
        x_old.reshape(slots, 2, half, quarter),
        jnp.stack([pre_gain, post_gain]),
        w_query,
        w_key,
        w_value,
        jnp.asarray(table),
        w_out_t,
    )
    mine = jnp.sum(jnp.where(jnp.arange(seq_count) == lax.axis_index("seq"), new_blocks, 0))
    return jnp.where(lax.axis_index("tp") < mine, result, jnp.zeros_like(result))


def output_phase(context, w_out_t, residual, post_gain, new_blocks, seq_count, tp_count, heads):
    tokens = context.shape[0]
    depth = w_out_t.shape[0]
    width = depth * seq_count
    share = 2 * tokens // (seq_count * tp_count)
    scattered = residual.ndim == 3
    places = tokens // share
    per_block = BLOCK // share
    copies = seq_count // heads
    bits = heads.bit_length() - 1
    first, last = layer_windows(seq_count, tp_count, per_block)
    seq_index = lax.axis_index("seq")
    tp_index = lax.axis_index("tp")
    blocks = new_blocks * per_block
    new_start = jnp.sum(
        jnp.where(
            jnp.arange(seq_count)[None, :] < jnp.arange(seq_count)[:, None], blocks[None, :], 0
        ),
        axis=1,
    )
    slots = jnp.arange(tp_count * seq_count, dtype=jnp.int32)
    layer = jnp.arange(tp_count, dtype=jnp.int32)[:, None]
    valid = (blocks[None, :] > layer).astype(jnp.int32).reshape(-1)
    source = (new_start[None, :] + layer).reshape(-1)
    rank = jnp.sum(jnp.where(slots[None, :] < slots[:, None], valid[None, :], 0), axis=1)
    perm = jnp.sum(
        jnp.where(
            (jnp.arange(places)[:, None] == rank[None, :]) & (valid[None, :] > 0),
            source[None, :],
            0,
        ),
        axis=1,
    ).astype(jnp.int32)
    in_layer = (jnp.arange(tp_count) == tp_index)[:, None]
    place = jnp.sum(jnp.where(in_layer, rank.reshape(tp_count, seq_count), 0), axis=0)
    place = jnp.minimum(place, places - 1).astype(jnp.int32)
    mine = jnp.sum(jnp.where(jnp.arange(seq_count) == seq_index, blocks, 0))
    block = jnp.minimum((new_start + tp_index) // per_block, tokens // BLOCK - 1).astype(jnp.int32)
    piece = residual.shape[1:] if scattered else (8, HEAD)
    old_block = pltpu.VMEM((seq_count,) + piece, jnp.bfloat16)
    chunks = 4
    rows = tokens // chunks // 2
    half = share // 2
    scratch_block = pltpu.VMEM((places, half, 2 * depth), jnp.bfloat16)
    swap_block = pltpu.VMEM((seq_count, half, 2 * depth), jnp.bfloat16)
    line_sem = pltpu.SemaphoreType.DMA((places,))
    gather_sem = pltpu.SemaphoreType.DMA((chunks, bits, heads))
    swap_sem = pltpu.SemaphoreType.DMA((seq_count,))
    result = pl.pallas_call(
        functools.partial(
            output_kernel, heads, copies, seq_count, tp_count, share, first, last, scattered
        ),
        out_shape=jax.ShapeDtypeStruct((share, width), jnp.bfloat16),
        in_specs=[pl.BlockSpec(memory_space=pltpu.SMEM)] * 3
        + [pl.BlockSpec(memory_space=pltpu.VMEM)] * 4,
        out_specs=pl.BlockSpec(memory_space=pltpu.VMEM),
        scratch_shapes=[
            pltpu.VMEM((chunks, rows, heads * HEAD), jnp.bfloat16),
            scratch_block,
            scratch_block,
            scratch_block,
            scratch_block,
            scratch_block,
            scratch_block,
            swap_block,
            swap_block,
            gather_sem,
            gather_sem,
            line_sem,
            line_sem,
            line_sem,
            line_sem,
            swap_sem,
            swap_sem,
            old_block,
            old_block,
            swap_sem,
            swap_sem,
            pltpu.VMEM((2 * depth, heads * HEAD), jnp.bfloat16),
            pltpu.VMEM((chunks, rows, HEAD), jnp.bfloat16),
            pltpu.SemaphoreType.DMA((2,)),
            pltpu.SemaphoreType.DMA((2, chunks)),
        ],
        compiler_params=pltpu.CompilerParams(
            collective_id=0, has_side_effects=True, vmem_limit_bytes=56 * 2**20
        ),
        cost_estimate=pl.CostEstimate(
            flops=60_000_000_000, bytes_accessed=4 * tokens * depth, transcendentals=0
        ),
    )(perm, place, block, context.reshape(places, 2, half, HEAD), w_out_t, residual, post_gain.reshape(1, -1))
    return jnp.where(tp_index < mine, result, jnp.zeros_like(result))


def per_device(
    x_old, old_blocks, new_blocks, order, pre_gain, post_gain, w_query, w_key, w_value, w_out_t
):
    seq_count = lax.axis_size("seq")
    tp_count = lax.axis_size("tp")
    capacity, quarter = x_old.shape
    width = quarter * tp_count
    tokens = seq_count * capacity // 2
    own = tokens // seq_count
    share = capacity // tp_count
    seq_index = lax.axis_index("seq")
    tp_index = lax.axis_index("tp")
    heads = w_query.shape[1] // HEAD
    kv_heads = w_key.shape[1] // HEAD
    scale = (width // (heads * tp_count)) ** (-0.5)
    if front_fits(seq_count, tp_count, heads, kv_heads, capacity):
        return front_phase(
            x_old,
            old_blocks,
            new_blocks,
            order,
            pre_gain,
            post_gain,
            w_query,
            w_key,
            w_value,
            w_out_t,
            seq_count,
            tp_count,
            scale,
        )
    old_start = offsets(old_blocks)
    new_start = offsets(new_blocks)
    device_ids = jnp.arange(seq_count, dtype=jnp.int32)

    gathered = lax.all_gather(x_old, "seq", axis=0, tiled=True)

    def stored(row, count):
        row = jnp.minimum(row, tokens - count)
        shard = jnp.sum((old_start <= row).astype(jnp.int32)) - 1
        holder = jnp.sum(jnp.where(order == shard, device_ids, 0))
        begin = jnp.sum(jnp.where(device_ids == shard, old_start, 0))
        return lax.dynamic_slice_in_dim(gathered, holder * capacity + row - begin, count, 0)

    def shift(k):
        return [(i, (i + k) % tp_count) for i in range(tp_count)]

    def by_source(received):
        stack = jnp.stack(received)
        pieces = [
            lax.dynamic_index_in_dim(stack, lax.rem(tp_index - u + tp_count, tp_count), 0, False)
            for u in range(tp_count)
        ]
        return jnp.concatenate(pieces, axis=1)

    mine = jnp.concatenate(
        [stored(seq_index * own + at, BLOCK) for at in range(0, own, BLOCK)], axis=0
    )
    full_rows = by_source(
        [mine] + [lax.ppermute(mine, "tp", shift(k)) for k in range(1, tp_count)]
    )
    my_start = jnp.sum(jnp.where(device_ids == seq_index, new_start, 0))

    def slot_rows(place):
        return stored(my_start + place * share, share)

    residual = by_source(
        [slot_rows(tp_index)]
        + [
            lax.ppermute(slot_rows(lax.rem(tp_index + k, tp_count)), "tp", shift(k))
            for k in range(1, tp_count)
        ]
    )

    weights = lax.all_gather(
        jnp.concatenate([w_query, w_key, w_value], axis=1), "seq", axis=0, tiled=True
    )

    normed = rms_scale(full_rows.astype(jnp.float32), pre_gain).astype(jnp.bfloat16)
    normed, residual = lax.optimization_barrier((normed, residual))
    group = heads // kv_heads
    copies = seq_count // heads
    raw = jnp.dot(normed, weights, preferred_element_type=jnp.float32)

    half = HEAD // 2
    inverse = jnp.exp(jnp.arange(half, dtype=jnp.float32) * (-2.0 * math.log(10000.0) / HEAD))
    places = seq_index * own + jnp.arange(own, dtype=jnp.int32)
    angles = places.astype(jnp.float32)[:, None] * inverse[None, :]
    cosine, sine = jnp.cos(angles), jnp.sin(angles)

    def rotate(at):
        first = raw[:, at * HEAD : at * HEAD + half]
        second = raw[:, at * HEAD + half : (at + 1) * HEAD]
        return jnp.concatenate(
            [first * cosine - second * sine, second * cosine + first * sine], axis=-1
        )

    queries = [(rotate(h) * scale).astype(jnp.bfloat16) for h in range(heads)]
    keys = [rotate(heads + g).astype(jnp.bfloat16) for g in range(kv_heads)]
    values = [
        raw[:, (heads + kv_heads + g) * HEAD : (heads + kv_heads + g + 1) * HEAD].astype(
            jnp.bfloat16
        )
        for g in range(kv_heads)
    ]
    sent = jnp.stack(
        [
            jnp.stack([queries[s // copies], keys[s // copies // group], values[s // copies // group]])
            for s in range(seq_count)
        ]
    )
    came = lax.all_to_all(sent, "seq", 0, 0, tiled=True)
    context = attention(
        came[:, 0].reshape(tokens, HEAD),
        came[:, 1].reshape(tokens, HEAD),
        came[:, 2].reshape(tokens, HEAD),
    )
    return output_phase(
        context, w_out_t, residual, post_gain, new_blocks, seq_count, tp_count, heads
    )


def solution(mesh):
    placed = (
        P("seq", "tp"),
        P(),
        P(),
        P(),
        P(),
        P(),
        P("seq", "tp"),
        P("seq", "tp"),
        P("seq", "tp"),
        P("seq", "tp"),
    )
    return jax.shard_map(
        per_device, mesh=mesh, in_specs=placed, out_specs=P(("seq", "tp"), None), check_vma=False
    )
```

```python
import functools
import math

import jax
import jax.numpy as jnp
import numpy as np
from jax import lax
from jax.experimental import pallas as pl
from jax.experimental.pallas import tpu as pltpu
from jax.sharding import PartitionSpec as P

HEAD = 128
BLOCK = 128
EPS = 1e-06
LAG = 4


def offsets(blocks):
    return (jnp.cumsum(blocks) - blocks) * BLOCK


def rms_scale(values, gain):
    return values * lax.rsqrt(jnp.mean(values * values, axis=-1, keepdims=True) + EPS) * gain


def attention_kernel(rows, span, q_ref, k_ref, v_ref, out_ref):
    first = pl.program_id(0) * rows
    query = q_ref[...]

    def step(at, carry, masked):
        numer, denom = carry
        start = pl.multiple_of(at * span, span)
        score = lax.dot_general(
            query,
            k_ref[pl.ds(start, span), :],
            (((1,), (1,)), ((), ())),
            preferred_element_type=jnp.float32,
        )
        weight = jnp.exp(50.0 * jnp.tanh(score * (1.0 / 50.0)))
        if masked:
            places = first + lax.broadcasted_iota(jnp.int32, weight.shape, 0)
            keys = start + lax.broadcasted_iota(jnp.int32, weight.shape, 1)
            weight = jnp.where(keys <= places, weight, 0.0)
        denom = denom + jnp.sum(weight, axis=1, keepdims=True)
        numer = numer + jnp.dot(
            weight.astype(jnp.bfloat16),
            v_ref[pl.ds(start, span), :],
            preferred_element_type=jnp.float32,
        )
        return numer, denom

    whole = first // span
    state = (jnp.zeros((rows, HEAD), jnp.float32), jnp.zeros((rows, 1), jnp.float32))
    state = lax.fori_loop(0, whole, lambda at, c: step(at, c, False), state)
    numer, denom = step(whole, state, True)
    out_ref[...] = (numer / denom).astype(out_ref.dtype)


def attention(query, key, value):
    tokens = query.shape[0]
    rows, span = 256, 512
    return pl.pallas_call(
        functools.partial(attention_kernel, rows, span),
        grid=(tokens // rows,),
        in_specs=[
            pl.BlockSpec((rows, HEAD), lambda i: (i, 0)),
            pl.BlockSpec((tokens, HEAD), lambda i: (0, 0)),
            pl.BlockSpec((tokens, HEAD), lambda i: (0, 0)),
        ],
        out_specs=pl.BlockSpec((rows, HEAD), lambda i: (i, 0)),
        out_shape=jax.ShapeDtypeStruct((tokens, HEAD), jnp.bfloat16),
        cost_estimate=pl.CostEstimate(
            flops=3 * tokens * tokens * HEAD,
            bytes_accessed=8 * tokens * HEAD,
            transcendentals=tokens * tokens,
        ),
    )(query, key, value)


MESH = pl.DeviceIdType.MESH


def arrangements(seq_count):
    found = []
    for second in range(1, seq_count + 1):
        for third in range(1, second + 1):
            fourth = seq_count - second - third
            if 1 <= fourth <= third:
                found.append((seq_count, second, third, fourth))
    return found


def layer_windows(seq_count, tp_count, per_block):
    first, last = [], []
    for layer in range(tp_count):
        starts, ends = [], []
        for counts in arrangements(seq_count):
            begin = sum(counts[u // per_block] for u in range(layer))
            starts.append(begin)
            ends.append(begin + counts[layer // per_block])
        first.append(min(starts))
        last.append(max(ends))
    return first, last


def pick(index, values):
    result = jnp.int32(values[0])
    for k in range(1, len(values)):
        result = jnp.where(index == k, jnp.int32(values[k]), result)
    return result


def flipped(index, mask):
    result = index
    bit = 1
    while bit <= mask:
        if mask & bit:
            result = result + bit - 2 * bit * lax.rem(index // bit, 2)
        bit *= 2
    return result


def output_kernel(
    heads,
    copies,
    seq_count,
    tp_count,
    share,
    first,
    last,
    scattered,
    perm_ref,
    place_ref,
    block_ref,
    context_ref,
    weight_ref,
    residual_ref,
    gain_ref,
    out_ref,
    full,
    partial,
    left_in,
    right_in,
    left_out,
    right_out,
    total,
    sent,
    came,
    gather_send,
    gather_recv,
    left_send,
    left_recv,
    right_send,
    right_recv,
    swap_send,
    swap_recv,
    old_sent,
    old_came,
    old_send,
    old_recv,
    weight,
    staged,
    weight_sem,
    staged_sem,
):
    seq_index = lax.axis_index("seq")
    tp_index = lax.axis_index("tp")
    places = partial.shape[0]
    depth = weight_ref.shape[0]
    half = partial.shape[1]
    core = lax.rem(seq_index, 2)
    partner = seq_index + 1 - 2 * core
    shared = copies == 1
    unit = 2 if shared else copies
    span = 2 * HEAD if shared else HEAD
    slot_index = seq_index // unit
    chunks = full.shape[0]
    per_chunk = places // chunks

    barrier = pltpu.get_barrier_semaphore()
    for k in range(1, seq_count):
        pl.semaphore_signal(
            barrier,
            inc=1,
            device_id=(lax.rem(seq_index + k, seq_count), tp_index),
            device_id_type=MESH,
        )

    @pl.when(tp_index > 0)
    def _():
        pl.semaphore_signal(
            barrier, inc=1, device_id=(seq_index, tp_index - 1), device_id_type=MESH
        )

    @pl.when(tp_index < tp_count - 1)
    def _():
        pl.semaphore_signal(
            barrier, inc=1, device_id=(seq_index, tp_index + 1), device_id_type=MESH
        )

    if scattered:
        per_block = BLOCK // share
        counts = [perm_ref[j] * per_block for j in range(seq_count)]
        begins, begin = [], jnp.int32(0)
        for j in range(seq_count):
            begins.append(begin)
            begin = begin + counts[j]
        perm = [jnp.int32(0)] * places
        place_of = [jnp.int32(0)] * seq_count
        rank = jnp.int32(0)
        for layer in range(tp_count):
            for j in range(seq_count):
                valid = jnp.minimum(jnp.maximum(counts[j] - layer, 0), 1)
                for q in range(first[layer], last[layer]):
                    here = jnp.where(rank == q, valid, 0)
                    perm[q] = perm[q] + here * (begins[j] + layer)
                place_of[j] = place_of[j] + jnp.where(tp_index == layer, rank, 0)
                rank = rank + valid
        place_of = [jnp.minimum(place, places - 1) for place in place_of]
        block_of = [
            jnp.minimum((begins[j] + tp_index) // per_block, places // per_block - 1)
            for j in range(seq_count)
        ]
        mine = jnp.int32(0)
        for j in range(seq_count):
            mine = mine + jnp.where(seq_index == j, counts[j], 0)
        live = jnp.minimum(jnp.maximum(mine - tp_index, 0), 1)
    else:
        perm = [perm_ref[q] for q in range(places)]
        place_of = [place_ref[j] for j in range(seq_count)]
        live = block_ref[0]
    live = live.astype(jnp.float32)

    neighbours = jnp.where(tp_index > 0, 1, 0) + jnp.where(tp_index < tp_count - 1, 1, 0)
    pl.semaphore_wait(barrier, seq_count - 1 + neighbours)

    bits = (seq_count // unit).bit_length() - 1
    order = list(range(chunks))[::-1]
    head = seq_index // copies
    own_columns = pl.ds(pl.multiple_of(head * HEAD, HEAD), HEAD)

    def staged_copy(chunk):
        return pltpu.make_async_remote_copy(
            src_ref=staged.at[chunk],
            dst_ref=full.at[chunk, :, own_columns],
            send_sem=staged_sem.at[0, chunk],
            recv_sem=staged_sem.at[1, chunk],
            device_id=(partner, tp_index),
            device_id_type=MESH,
        )

    own_rows = pl.ds(pl.multiple_of(core * depth, depth), depth)
    weight_copy = pltpu.make_async_remote_copy(
        src_ref=weight_ref,
        dst_ref=weight.at[own_rows],
        send_sem=weight_sem.at[0],
        recv_sem=weight_sem.at[1],
        device_id=(partner, tp_index),
        device_id_type=MESH,
    )

    for chunk in order:
        for at in range(per_chunk):
            source = perm[chunk * per_chunk + at]
            rows = slice(at * half, (at + 1) * half)
            full[chunk, rows, own_columns] = context_ref[source, core]
            if shared:
                staged[chunk, rows] = context_ref[source, 1 - core]
        if shared:
            staged_copy(chunk).start()
    weight_copy.start()

    def dims(chunk):
        outer = list(range(bits))
        return outer[::-1] if chunk % 2 else outer

    def gather_copy(chunk, bit, combo, to_me):
        slot = flipped(slot_index, (combo ^ (1 << bit)) if to_me else combo)
        view = full.at[chunk, :, pl.ds(pl.multiple_of(slot * span, span), span)]
        return pltpu.make_async_remote_copy(
            src_ref=view,
            dst_ref=view,
            send_sem=gather_send.at[chunk, bit, combo],
            recv_sem=gather_recv.at[chunk, bit, combo],
            device_id=(flipped(seq_index, unit << bit), tp_index),
            device_id_type=MESH,
        )

    def steps(chunk):
        held = [0]
        for bit in dims(chunk):
            yield bit, list(held)
            held = held + [c ^ (1 << bit) for c in held]

    def offer(at):
        if at < chunks:
            if shared:
                staged_copy(order[at]).wait_recv()
            for bit, _ in steps(order[at]):
                gather_copy(order[at], bit, 0, False).start()

    offer(0)
    weight[own_rows] = weight_ref[...]
    total[...] = jnp.zeros_like(total)

    def relay(at):
        chunk = order[at]
        stages = list(steps(chunk))
        for level, (bit, held) in enumerate(stages):
            for combo in held:
                gather_copy(chunk, bit, combo, True).wait_recv()
                for later, _ in stages[level + 1 :]:
                    gather_copy(chunk, later, combo ^ (1 << bit), False).start()
            if level == 0:
                offer(at + 1)

    def multiply(chunk):
        product = lax.dot_general(
            full[chunk],
            weight[...],
            (((1,), (1,)), ((), ())),
            preferred_element_type=jnp.float32,
        ).astype(jnp.bfloat16)
        for at in range(per_chunk):
            partial[chunk * per_chunk + at] = product[at * half : (at + 1) * half]

    left_has = jnp.where(tp_index < tp_count - 1, pick(tp_index, last), 0)
    left_gives = pick(tp_index, [0] + last[:-1])
    right_has = jnp.where(tp_index > 0, pick(tp_index, first), places)
    right_gives = pick(tp_index, first[1:] + [places])

    def line_copy(place, source, landing, send, recv, step):
        return pltpu.make_async_remote_copy(
            src_ref=source.at[place],
            dst_ref=landing.at[place],
            send_sem=send.at[place],
            recv_sem=recv.at[place],
            device_id=(seq_index, tp_index + step),
            device_id_type=MESH,
        )

    def flow(place, has, gives, source, landing, send, recv, step):
        @pl.when(has)
        def _():
            line_copy(place, source, landing, send, recv, step).wait_recv()

        @pl.when(jnp.logical_and(has, gives))
        def _():
            source[place] = (
                partial[place].astype(jnp.float32) + landing[place].astype(jnp.float32)
            ).astype(jnp.bfloat16)

        @pl.when(jnp.logical_and(jnp.logical_not(has), gives))
        def _():
            source[place] = partial[place]

        @pl.when(gives)
        def _():
            line_copy(place, source, landing, send, recv, step).start()

    def swap_copy(other, mine, at):
        return pltpu.make_async_remote_copy(
            src_ref=sent.at[other],
            dst_ref=came.at[mine],
            send_sem=swap_send.at[at],
            recv_sem=swap_recv.at[at],
            device_id=(other, tp_index),
            device_id_type=MESH,
        )

    def line_step(at, carry):
        passed = at - LAG * (tp_count - 1 - tp_index)
        place = places - 1 - passed
        valid = jnp.logical_and(passed >= 0, passed < places)
        has = jnp.logical_and(valid, place < left_has)
        gives = jnp.logical_and(valid, place < left_gives)
        flow(place, has, gives, left_out, left_in, left_send, left_recv, -1)
        ends = jnp.logical_and(
            jnp.logical_and(valid, tp_index == 0), place < seq_count
        )

        @pl.when(ends)
        def _():
            sent[place] = (
                partial[place].astype(jnp.float32) + left_in[place].astype(jnp.float32)
            ).astype(jnp.bfloat16)

            @pl.when(place == seq_index)
            def _():
                came[place] = sent[place]

            @pl.when(place != seq_index)
            def _():
                swap_copy(
                    place, seq_index, lax.rem(place + seq_count - seq_index, seq_count)
                ).start()

        passed = at - LAG * tp_index
        place = places - 1 - passed
        valid = jnp.logical_and(passed >= 0, passed < places)
        has = jnp.logical_and(valid, place >= right_has)
        gives = jnp.logical_and(valid, place >= right_gives)
        flow(place, has, gives, right_out, right_in, right_send, right_recv, 1)
        return carry

    def old_copy(other, mine, at):
        return pltpu.make_async_remote_copy(
            src_ref=old_sent.at[other],
            dst_ref=old_came.at[mine],
            send_sem=old_send.at[at],
            recv_sem=old_recv.at[at],
            device_id=(other, tp_index),
            device_id_type=MESH,
        )

    for at, chunk in enumerate(order):
        relay(at)
        if at == 0:
            weight_from = pltpu.make_async_remote_copy(
                src_ref=weight_ref,
                dst_ref=weight.at[pl.ds(pl.multiple_of((1 - core) * depth, depth), depth)],
                send_sem=weight_sem.at[0],
                recv_sem=weight_sem.at[1],
                device_id=(partner, tp_index),
                device_id_type=MESH,
            )
            weight_from.wait_recv()
        multiply(chunk)
        if scattered and at == chunks - 1:
            for j in range(seq_count):
                old_sent[j] = residual_ref[block_of[j]]
            for k in range(1, seq_count):
                old_copy(lax.rem(seq_index + k, seq_count), seq_index, k).start()
            old_came[seq_index] = old_sent[seq_index]
        lax.fori_loop(at * per_chunk, (at + 1) * per_chunk, line_step, 0)
    lax.fori_loop(places, places + LAG * (tp_count - 1), line_step, 0)

    def sum_step(place, carry):
        value = partial[place].astype(jnp.float32) + right_in[place].astype(jnp.float32)

        @pl.when(place < left_has)
        def _():
            total[place] = (value + left_in[place].astype(jnp.float32)).astype(jnp.bfloat16)

        @pl.when(place >= left_has)
        def _():
            total[place] = value.astype(jnp.bfloat16)

        return carry

    @pl.when(tp_index > 0)
    def _():
        lax.fori_loop(pick(tp_index, first), pick(tp_index, last), sum_step, 0)
        for j in range(seq_count):
            sent[j] = total[place_of[j]]
        for k in range(1, seq_count):
            swap_copy(lax.rem(seq_index + k, seq_count), seq_index, k).start()
        came[seq_index] = sent[seq_index]

    for k in range(1, seq_count):
        swap_copy(
            lax.rem(seq_index + k, seq_count),
            lax.rem(seq_index + seq_count - k, seq_count),
            k,
        ).wait_recv()

    if scattered:
        for k in range(1, seq_count):
            old_copy(
                lax.rem(seq_index + k, seq_count),
                lax.rem(seq_index + seq_count - k, seq_count),
                k,
            ).wait_recv()
    wide = 2 * depth
    for side in range(2):
        square = jnp.zeros((half, 1), jnp.float32)
        for c in range(seq_count // 2):
            piece = came[2 * c + side].astype(jnp.float32)
            square = square + jnp.sum(piece * piece, axis=1, keepdims=True)
        factor = lax.rsqrt(square * (1.0 / (depth * seq_count)) + EPS)
        rows = slice(side * half, (side + 1) * half)
        for c in range(seq_count // 2):
            columns = slice(c * wide, (c + 1) * wide)
            old = old_came[2 * c + side] if scattered else residual_ref[rows, columns]
            value = old.astype(jnp.float32) + (
                came[2 * c + side].astype(jnp.float32) * factor * gain_ref[1:2, columns]
            )
            out_ref[rows, columns] = (value * live).astype(jnp.bfloat16)

    for k in range(1, seq_count):
        swap_copy(lax.rem(seq_index + k, seq_count), seq_index, k).wait_send()
    if scattered:
        for k in range(1, seq_count):
            old_copy(lax.rem(seq_index + k, seq_count), seq_index, k).wait_send()
    weight_copy.wait_send()
    for chunk in range(chunks):
        if shared:
            staged_copy(chunk).wait_send()
        for bit, held in steps(chunk):
            for combo in held:
                gather_copy(chunk, bit, combo, False).wait_send()

    def drain(place, carry):
        @pl.when(place < left_gives)
        def _():
            line_copy(place, left_out, left_in, left_send, left_recv, -1).wait_send()

        @pl.when(place >= right_gives)
        def _():
            line_copy(place, right_out, right_in, right_send, right_recv, 1).wait_send()

        return carry

    lax.fori_loop(0, places, drain, 0)


def front_kernel(
    seq_count,
    tp_count,
    group,
    scale,
    blocks_ref,
    order_ref,
    x_ref,
    gain_ref,
    query_ref,
    key_ref,
    value_ref,
    angle_ref,
    context_out,
    x_out,
    q_buf,
    kv_buf,
    near,
    send_a,
    send_b,
    far,
    line,
    twin,
    weight,
    normed,
    scale_row,
    scale_all,
    scale_column,
    first_out,
    first_in,
    second_out,
    second_in,
    kept,
    core_sem,
    weight_sem,
    stage_sem,
    line_send,
    line_recv,
    plane_send,
    plane_recv,
    twin_sem,
    stat_sem,
    factor_sem,
    first_sem,
    second_sem,
    kv_sem,
):
    seq_index = lax.axis_index("seq")
    tp_index = lax.axis_index("tp")
    chip = seq_index // 2
    core = lax.rem(seq_index, 2)
    partner = seq_index + 1 - 2 * core
    slots = x_ref.shape[0]
    chips = seq_count // 2
    each = line.shape[1]
    half = line.shape[2]
    quarter = line.shape[3]
    depth = query_ref.shape[0]
    pair = 2 * HEAD

    barrier = pltpu.get_barrier_semaphore()
    for k in range(1, seq_count):
        other = lax.rem(seq_index + k, seq_count)
        pl.semaphore_signal(barrier, inc=1, device_id=(other, tp_index), device_id_type=MESH)
    for k in range(1, tp_count):
        other = lax.rem(tp_index + k, tp_count)
        pl.semaphore_signal(barrier, inc=1, device_id=(seq_index, other), device_id_type=MESH)

    def remote(source, target, sems, at, seq, tp):
        return pltpu.make_async_remote_copy(
            src_ref=source,
            dst_ref=target,
            send_sem=sems[0].at[at],
            recv_sem=sems[1].at[at],
            device_id=(seq, tp),
            device_id_type=MESH,
        )

    core_sems = (core_sem.at[0], core_sem.at[1])

    def swap_slots(holder):
        return remote(
            x_ref.at[:, 1 - core],
            near.at[pl.ds(slots * holder, slots)],
            core_sems,
            0,
            partner,
            tp_index,
        )

    def lanes(head, count=1):
        return pl.ds(pl.multiple_of(head * HEAD, HEAD), count * HEAD)

    def weight_copy(source, column, target, at, holder):
        return remote(
            source.at[:, lanes(column)],
            weight.at[pl.ds(pl.multiple_of(holder * depth, depth), depth), lanes(target)],
            (weight_sem.at[0], weight_sem.at[1]),
            at,
            partner,
            tp_index,
        )

    pl.semaphore_wait(barrier, seq_count - 1 + tp_count - 1)
    swap_slots(core).start()
    for slot in range(slots):
        near[slots * core + slot] = x_ref[slot, core]

    starts, counts, holders = [], [], []
    begin = jnp.int32(0)
    for k in range(seq_count):
        starts.append(begin)
        counts.append(blocks_ref[k])
        begin = begin + blocks_ref[k]
        holder = jnp.int32(0)
        for place in range(1, seq_count):
            holder = holder + jnp.where(order_ref[place] == k, jnp.int32(place), jnp.int32(0))
        holders.append(holder)

    def found(block):
        at = jnp.int32(0)
        for k in range(seq_count):
            inside = jnp.logical_and(starts[k] <= block, block < starts[k] + counts[k])
            at = at + jnp.where(inside, holders[k] * slots + block - starts[k], jnp.int32(0))
        return at // (2 * slots), lax.rem(at, 2 * slots)

    first_chip = jnp.where(core == 0, flipped(chip, 1), flipped(chip, 2))
    second_chip = jnp.where(core == 0, flipped(chip, 2), flipped(chip, 1))
    cross_chip = flipped(chip, 3)
    swap_slots(1 - core).wait_recv()

    stage_sems = (stage_sem.at[0], stage_sem.at[1])
    table_a = []
    for at in range(2 * each):
        target = first_chip if at < each else cross_chip
        owner, index = found(chips * (at % each) + target)
        table_a.append(jnp.where(owner == chip, index, 0))
    across_first = list(range(each, 2 * each)) + list(range(each))
    for at in across_first:
        send_a[at] = near[table_a[at]]
        remote(
            send_a.at[at], far.at[at], stage_sems, at, 2 * first_chip + core, tp_index
        ).start()

    for c in range(chips):
        weight_copy(query_ref, 2 * c + 1 - core, 2 * c, 2 * c, core).start()

        @pl.when(core == 0)
        def _():
            weight_copy(value_ref, c, 2 * c + 1, 2 * c + 1, core).start()

        @pl.when(core == 1)
        def _():
            weight_copy(key_ref, c, 2 * c + 1, 2 * c + 1, core).start()

    own_rows = pl.ds(pl.multiple_of(core * depth, depth), depth)
    for c in range(chips):
        weight[own_rows, pl.ds(2 * c * HEAD, HEAD)] = query_ref[:, lanes(2 * c + core)]

        @pl.when(core == 0)
        def _():
            weight[own_rows, pl.ds((2 * c + 1) * HEAD, HEAD)] = key_ref[
                :, pl.ds(c * HEAD, HEAD)
            ]

        @pl.when(core == 1)
        def _():
            weight[own_rows, pl.ds((2 * c + 1) * HEAD, HEAD)] = value_ref[
                :, pl.ds(c * HEAD, HEAD)
            ]

    def arrive_a(at):
        remote(
            send_a.at[at], far.at[at], stage_sems, at, 2 * first_chip + core, tp_index
        ).wait_recv()

    both = 2 * slots
    for at in range(each, 2 * each):
        arrive_a(at)
        near[both + at] = far[at]
    for at in range(each):
        owner, index = found(chips * at + second_chip)
        send_b[at] = near[jnp.where(owner == chip, index, both + each + at)]
        remote(
            send_b.at[at],
            far.at[2 * each + at],
            stage_sems,
            2 * each + at,
            2 * second_chip + core,
            tp_index,
        ).start()
    for at in range(each):
        arrive_a(at)
        near[both + at] = far[at]
    for at in range(each):
        owner, index = found(chips * at + chip)
        near[both + 2 * each + at] = near[jnp.where(owner == chip, index, both + at)]
    for at in range(each):
        remote(
            send_b.at[at],
            far.at[2 * each + at],
            stage_sems,
            2 * each + at,
            2 * second_chip + core,
            tp_index,
        ).wait_recv()
        near[both + 3 * each + at] = far[2 * each + at]
    for at in range(each):
        owner, _ = found(chips * at + chip)
        local = jnp.logical_or(owner == chip, owner == first_chip)
        line[tp_index, at] = near[
            jnp.where(local, both + 2 * each + at, both + 3 * each + at)
        ]

    def line_copy(layer, at, step):
        view = line.at[layer, at]
        return pltpu.make_async_remote_copy(
            src_ref=view,
            dst_ref=view,
            send_sem=line_send.at[(step + 1) // 2, layer, at],
            recv_sem=line_recv.at[layer, at],
            device_id=(seq_index, tp_index + step),
            device_id_type=MESH,
        )

    def plane_copy(layer, at, holder):
        return pltpu.make_async_remote_copy(
            src_ref=line.at[layer, at],
            dst_ref=x_out.at[chips * at + holder],
            send_sem=plane_send.at[layer, at],
            recv_sem=plane_recv.at[chips * at + holder],
            device_id=(2 * layer + core, tp_index),
            device_id_type=MESH,
        )

    def twin_copy(block):
        return remote(
            x_out.at[block],
            twin.at[block],
            (twin_sem.at[0], twin_sem.at[1]),
            block,
            partner,
            tp_index,
        )

    def guarded(condition, action):
        @pl.when(condition)
        def _():
            action()

    def forward(layer, at):
        @pl.when(layer == chip)
        def _():
            x_out[chips * at + chip] = line[layer, at]

        @pl.when(layer != chip)
        def _():
            plane_copy(layer, at, chip).start()

    def own_step(at):
        guarded(tp_index > 0, lambda: line_copy(tp_index, at, -1).start())
        guarded(tp_index < tp_count - 1, lambda: line_copy(tp_index, at, 1).start())
        forward(tp_index, at)

    def hop_step(at, distance):
        @pl.when(tp_index >= distance)
        def _():
            layer = tp_index - distance
            line_copy(layer, at, 1).wait_recv()
            guarded(tp_index < tp_count - 1, lambda: line_copy(layer, at, 1).start())
            forward(layer, at)

        @pl.when(tp_index + distance < tp_count)
        def _():
            layer = tp_index + distance
            line_copy(layer, at, -1).wait_recv()
            guarded(tp_index > 0, lambda: line_copy(layer, at, -1).start())
            forward(layer, at)

    def plane_step(at):
        for c in range(chips):

            @pl.when(chip != c)
            def _():
                plane_copy(chip, at, c).wait_recv()

        for c in range(chips):
            twin_copy(chips * at + c).start()

    tiles = quarter // HEAD
    gain_at = pl.multiple_of(chip * quarter, HEAD)

    def normalize(source, block, holder, target):
        rows = pl.ds(pl.multiple_of((block // chips) * half, half), half)
        factor = scale_column[holder, rows, :]
        for tile in range(tiles):
            columns = slice(tile * HEAD, (tile + 1) * HEAD)
            values = source[block, :, columns].astype(jnp.float32)
            gains = gain_ref[:1, pl.ds(pl.multiple_of(gain_at + tile * HEAD, HEAD), HEAD)]
            normed[target[0], target[1], target[2], :, columns] = (
                values * factor * gains
            ).astype(jnp.bfloat16)

    bits = (1, 2)

    def first_copy(at, side):
        bit = bits[side]
        return pltpu.make_async_remote_copy(
            src_ref=first_out.at[at, side],
            dst_ref=first_in.at[at, side],
            send_sem=first_sem.at[0, at, side],
            recv_sem=first_sem.at[1, at, side],
            device_id=(2 * flipped(chip, bit) + core, tp_index),
            device_id_type=MESH,
        )

    def second_copy(at, side):
        bit = bits[1 - side]
        return pltpu.make_async_remote_copy(
            src_ref=second_out.at[at, side],
            dst_ref=second_in.at[at, side],
            send_sem=second_sem.at[0, at, side],
            recv_sem=second_sem.at[1, at, side],
            device_id=(2 * flipped(chip, bit) + core, tp_index),
            device_id_type=MESH,
        )

    def multiply_step(at):
        for side in range(2):
            for u in range(2):
                c = 2 * side + u
                block = chips * at + c
                twin_copy(block).wait_recv()
                normalize(x_out, block, 2 * c + core, (side, u, core))
                normalize(twin, block, 2 * c + 1 - core, (side, u, 1 - core))
            rows = normed[side].reshape(4 * half, quarter)

            def part(mask):
                target = flipped(chip, mask)
                return jnp.dot(
                    rows,
                    weight[:, lanes(2 * target, 2)],
                    preferred_element_type=jnp.float32,
                )

            first, second = bits[side], bits[1 - side]
            first_out[at, side, 0] = part(first).astype(jnp.bfloat16)
            first_out[at, side, 1] = part(3).astype(jnp.bfloat16)
            first_copy(at, side).start()
            kept[at, side, 0] = part(0)
            kept[at, side, 1] = part(second)

    def add_step(at):
        for side in range(2):
            first_copy(at, side).wait_recv()
            second_out[at, side] = (
                kept[at, side, 1] + first_in[at, side, 1].astype(jnp.float32)
            ).astype(jnp.bfloat16)
            second_copy(at, side).start()

    def kv_copy(kind, block):
        rows = pl.ds(pl.multiple_of(block * BLOCK, BLOCK), BLOCK)
        view = kv_buf.at[kind, rows, :]
        return remote(
            view, view, (kv_sem.at[0], kv_sem.at[1]), block, partner, tp_index
        )

    lane = lax.broadcasted_iota(jnp.int32, (BLOCK, HEAD), 1)

    def turned(values, rows):
        angles = angle_ref[rows, :]
        swapped = pltpu.roll(angles, HEAD // 2, 1)
        low = lane < HEAD // 2
        cosine = jnp.where(low, angles, swapped)
        sine = jnp.where(low, -swapped, angles)
        return values * cosine + pltpu.roll(values, HEAD // 2, 1) * sine

    def finish_step(at):
        for side in range(2):
            second_copy(at, side).wait_recv()
            for u in range(2):
                block = chips * at + 2 * side + u
                part = slice(u * BLOCK, (u + 1) * BLOCK)
                value = (
                    kept[at, side, 0, part]
                    + first_in[at, side, 0, part].astype(jnp.float32)
                    + second_in[at, side, part].astype(jnp.float32)
                )
                rows = pl.ds(pl.multiple_of(block * BLOCK, BLOCK), BLOCK)
                q_buf[rows, :] = (turned(value[:, :HEAD], rows) * scale).astype(jnp.bfloat16)

                @pl.when(core == 0)
                def _():
                    kv_buf[0, rows, :] = turned(value[:, HEAD:], rows).astype(jnp.bfloat16)

                @pl.when(core == 1)
                def _():
                    kv_buf[1, rows, :] = value[:, HEAD:].astype(jnp.bfloat16)

                kv_copy(core, block).start()

    span = chips * BLOCK
    sub = span // 2
    mask = lax.broadcasted_iota(jnp.int32, (sub, sub), 1) <= lax.broadcasted_iota(
        jnp.int32, (sub, sub), 0
    )

    def attend_step(at):
        for c in range(chips):
            kv_copy(1 - core, chips * at + c).wait_recv()

        def attend(query, start, count, carry, masked):
            keys = pl.ds(pl.multiple_of(start, sub), count)
            score = lax.dot_general(
                query,
                kv_buf[0, keys, :],
                (((1,), (1,)), ((), ())),
                preferred_element_type=jnp.float32,
            )
            part = jnp.exp2((50.0 / math.log(2.0)) * jnp.tanh(score * (1.0 / 50.0)))
            if masked:
                part = jnp.where(mask, part, 0.0)
            numer, denom = carry
            denom = denom + jnp.sum(part, axis=1, keepdims=True)
            numer = numer + jnp.dot(
                part.astype(jnp.bfloat16), kv_buf[1, keys, :], preferred_element_type=jnp.float32
            )
            return numer, denom

        for piece in range(2):
            begin = at * span + piece * sub
            rows = pl.ds(pl.multiple_of(begin, sub), sub)
            query = q_buf[rows, :]
            state = (jnp.zeros((sub, HEAD), jnp.float32), jnp.zeros((sub, 1), jnp.float32))
            state = lax.fori_loop(
                0, at, lambda n, carry: attend(query, n * span, span, carry, False), state
            )
            if piece:
                state = attend(query, at * span, sub, state, False)
            numer, denom = attend(query, begin, sub, state, True)
            context_out[rows, :] = (numer / denom).astype(jnp.bfloat16)

    def stat_copy(layer_from, layer_to):
        return pltpu.make_async_remote_copy(
            src_ref=scale_row.at[layer_from],
            dst_ref=scale_row.at[layer_from],
            send_sem=stat_sem.at[0, layer_to],
            recv_sem=stat_sem.at[1, layer_from],
            device_id=(seq_index, layer_to),
            device_id_type=MESH,
        )

    def factor_copy(holder, other):
        return pltpu.make_async_remote_copy(
            src_ref=scale_all.at[holder],
            dst_ref=scale_all.at[holder],
            send_sem=factor_sem.at[0, other],
            recv_sem=factor_sem.at[1, holder],
            device_id=(other, tp_index),
            device_id_type=MESH,
        )

    own_step(0)
    squares = []
    for at in range(each):
        values = line[tp_index, at].astype(jnp.float32)
        squares.append(jnp.sum(values * values, axis=1, keepdims=True))
    column = jnp.broadcast_to(jnp.concatenate(squares, axis=0), (each * half, HEAD))
    scale_row[tp_index] = jnp.transpose(column)[:8, :]
    for k in range(1, tp_count):
        stat_copy(tp_index, lax.rem(tp_index + k, tp_count)).start()
    for c in range(2 * chips):
        weight_copy(query_ref, 0, 0, c, 1 - core).wait_recv()
    for k in range(1, tp_count):
        other = lax.rem(tp_index + k, tp_count)
        stat_copy(other, tp_index).wait_recv()
    square = scale_row[0]
    for k in range(1, tp_count):
        square = square + scale_row[k]
    scale_all[seq_index] = lax.rsqrt(square * (1.0 / (quarter * tp_count)) + EPS)
    for k in range(1, seq_count):
        factor_copy(seq_index, lax.rem(seq_index + k, seq_count)).start()

    def steps(i, carry):
        for lag, action in (
            (0, lambda at: guarded(at > 0, lambda: own_step(at))),
            (1, lambda at: hop_step(at, 1)),
            (2, lambda at: hop_step(at, 2)),
            (3, lambda at: hop_step(at, 3)),
            (4, plane_step),
            (5, multiply_step),
            (6, add_step),
            (7, finish_step),
            (8, attend_step),
        ):
            at = i - lag

            @pl.when(jnp.logical_and(at >= 0, at < each))
            def _():
                action(at)

        return carry

    lax.fori_loop(0, 5, steps, 0)
    for k in range(1, seq_count):
        other = lax.rem(seq_index + k, seq_count)
        factor_copy(other, seq_index).wait_recv()
    for s in range(seq_count):
        scale_column[s] = jnp.transpose(
            jnp.broadcast_to(scale_all[s, :1, :], (HEAD, each * half))
        )
    lax.fori_loop(5, each + 8, steps, 0)

    swap_slots(core).wait_send()
    for c in range(2 * chips):
        weight_copy(query_ref, 0, 0, c, core).wait_send()
    for at in range(2 * each):
        remote(
            send_a.at[at], far.at[at], stage_sems, at, 2 * first_chip + core, tp_index
        ).wait_send()
    for at in range(each):
        remote(
            send_b.at[at],
            far.at[2 * each + at],
            stage_sems,
            2 * each + at,
            2 * second_chip + core,
            tp_index,
        ).wait_send()
    for k in range(1, tp_count):
        stat_copy(tp_index, lax.rem(tp_index + k, tp_count)).wait_send()
    for k in range(1, seq_count):
        factor_copy(seq_index, lax.rem(seq_index + k, seq_count)).wait_send()

    def drain(at, carry):
        for layer in range(tp_count):
            right = jnp.logical_and(tp_index >= layer, tp_index < tp_count - 1)
            guarded(right, lambda: line_copy(layer, at, 1).wait_send())
            left = jnp.logical_and(tp_index <= layer, tp_index > 0)
            guarded(left, lambda: line_copy(layer, at, -1).wait_send())
            guarded(chip != layer, lambda: plane_copy(layer, at, chip).wait_send())
        for side in range(2):
            first_copy(at, side).wait_send()
            second_copy(at, side).wait_send()
        for c in range(chips):
            twin_copy(chips * at + c).wait_send()
            kv_copy(core, chips * at + c).wait_send()
        return carry

    lax.fori_loop(0, each, drain, 0)


def front_fits(seq_count, tp_count, heads, kv_heads, capacity):
    return (
        heads == seq_count == 8
        and 2 * kv_heads == heads
        and tp_count == 4
        and capacity == 4 * BLOCK
    )


def front_phase(
    x_old, old_blocks, order, gains, w_query, w_key, w_value, seq_count, tp_count, scale
):
    capacity, quarter = x_old.shape
    depth = w_query.shape[0]
    slots = capacity // BLOCK
    half = BLOCK // 2
    tokens = seq_count * capacity // 2
    chips = seq_count // 2
    each = tokens // BLOCK // chips
    group = w_query.shape[1] // w_key.shape[1]
    angles = (
        np.arange(tokens, dtype=np.float32)[:, None]
        * np.exp(
            np.arange(HEAD // 2, dtype=np.float32) * np.float32(-2.0 * math.log(10000.0) / HEAD)
        )[None, :]
    )
    table = np.concatenate([np.cos(angles), np.sin(angles)], axis=1).astype(np.float32)
    bf16, f32 = jnp.bfloat16, jnp.float32
    piece = (half, quarter)
    dma = pltpu.SemaphoreType.DMA
    vmem = pl.BlockSpec(memory_space=pltpu.VMEM)
    smem = pl.BlockSpec(memory_space=pltpu.SMEM)
    square = (2 * BLOCK, 2 * HEAD)
    return pl.pallas_call(
        functools.partial(front_kernel, seq_count, tp_count, group, scale),
        out_shape=(
            jax.ShapeDtypeStruct((tokens, HEAD), bf16),
            jax.ShapeDtypeStruct((each * chips,) + piece, bf16),
        ),
        in_specs=[smem] * 2 + [vmem] * 6,
        out_specs=(vmem, vmem),
        scratch_shapes=[
            pltpu.VMEM((tokens, HEAD), bf16),
            pltpu.VMEM((2, tokens, HEAD), bf16),
            pltpu.VMEM((2 * slots + 4 * each,) + piece, bf16),
            pltpu.VMEM((2 * each,) + piece, bf16),
            pltpu.VMEM((each,) + piece, bf16),
            pltpu.VMEM((3 * each,) + piece, bf16),
            pltpu.VMEM((tp_count, each) + piece, bf16),
            pltpu.VMEM((each * chips,) + piece, bf16),
            pltpu.VMEM((2 * depth, 2 * chips * HEAD), bf16),
            pltpu.VMEM((2, 2, 2) + piece, bf16),
            pltpu.VMEM((tp_count, 8, each * half), f32),
            pltpu.VMEM((seq_count, 8, each * half), f32),
            pltpu.VMEM((seq_count, each * half, HEAD), f32),
            pltpu.VMEM((each, 2, 2) + square, bf16),
            pltpu.VMEM((each, 2, 2) + square, bf16),
            pltpu.VMEM((each, 2) + square, bf16),
            pltpu.VMEM((each, 2) + square, bf16),
            pltpu.VMEM((each, 2, 2) + square, f32),
            dma((2, 1)),
            dma((2, 2 * chips)),
            dma((2, 3 * each)),
            dma((2, tp_count, each)),
            dma((tp_count, each)),
            dma((tp_count, each)),
            dma((each * chips,)),
            dma((2, each * chips)),
            dma((2, tp_count)),
            dma((2, seq_count)),
            dma((2, each, 2)),
            dma((2, each, 2)),
            dma((2, each * chips)),
        ],
        compiler_params=pltpu.CompilerParams(
            collective_id=1, has_side_effects=True, vmem_limit_bytes=60 * 2**20
        ),
        cost_estimate=pl.CostEstimate(
            flops=60_000_000_000, bytes_accessed=8 * tokens * depth, transcendentals=0
        ),
    )(
        old_blocks,
        order,
        x_old.reshape(slots, 2, half, quarter),
        gains,
        w_query,
        w_key,
        w_value,
        jnp.asarray(table),
    )


def output_phase(context, w_out_t, residual, gains, new_blocks, seq_count, tp_count, heads):
    tokens = context.shape[0]
    depth = w_out_t.shape[0]
    width = depth * seq_count
    share = 2 * tokens // (seq_count * tp_count)
    scattered = residual.ndim == 3
    places = tokens // share
    per_block = BLOCK // share
    copies = seq_count // heads
    bits = heads.bit_length() - 1
    first, last = layer_windows(seq_count, tp_count, per_block)
    seq_index = lax.axis_index("seq")
    tp_index = lax.axis_index("tp")
    if scattered:
        perm = place = live = new_blocks
    else:
        blocks = new_blocks * per_block
        new_start = jnp.sum(
            jnp.where(
                jnp.arange(seq_count)[None, :] < jnp.arange(seq_count)[:, None], blocks[None, :], 0
            ),
            axis=1,
        )
        slots = jnp.arange(tp_count * seq_count, dtype=jnp.int32)
        layer = jnp.arange(tp_count, dtype=jnp.int32)[:, None]
        valid = (blocks[None, :] > layer).astype(jnp.int32).reshape(-1)
        source = (new_start[None, :] + layer).reshape(-1)
        rank = jnp.sum(jnp.where(slots[None, :] < slots[:, None], valid[None, :], 0), axis=1)
        perm = jnp.sum(
            jnp.where(
                (jnp.arange(places)[:, None] == rank[None, :]) & (valid[None, :] > 0),
                source[None, :],
                0,
            ),
            axis=1,
        ).astype(jnp.int32)
        in_layer = (jnp.arange(tp_count) == tp_index)[:, None]
        place = jnp.sum(jnp.where(in_layer, rank.reshape(tp_count, seq_count), 0), axis=0)
        place = jnp.minimum(place, places - 1).astype(jnp.int32)
        mine = jnp.sum(jnp.where(jnp.arange(seq_count) == seq_index, blocks, 0))
        live = (tp_index < mine).astype(jnp.int32).reshape(1)
    piece = residual.shape[1:] if scattered else (8, HEAD)
    old_block = pltpu.VMEM((seq_count,) + piece, jnp.bfloat16)
    chunks = 4
    rows = tokens // chunks // 2
    half = share // 2
    scratch_block = pltpu.VMEM((places, half, 2 * depth), jnp.bfloat16)
    swap_block = pltpu.VMEM((seq_count, half, 2 * depth), jnp.bfloat16)
    line_sem = pltpu.SemaphoreType.DMA((places,))
    gather_sem = pltpu.SemaphoreType.DMA((chunks, bits, heads))
    swap_sem = pltpu.SemaphoreType.DMA((seq_count,))
    return pl.pallas_call(
        functools.partial(
            output_kernel, heads, copies, seq_count, tp_count, share, first, last, scattered
        ),
        out_shape=jax.ShapeDtypeStruct((share, width), jnp.bfloat16),
        in_specs=[pl.BlockSpec(memory_space=pltpu.SMEM)] * 3
        + [pl.BlockSpec(memory_space=pltpu.VMEM)] * 4,
        out_specs=pl.BlockSpec(memory_space=pltpu.VMEM),
        scratch_shapes=[
            pltpu.VMEM((chunks, rows, heads * HEAD), jnp.bfloat16),
            scratch_block,
            scratch_block,
            scratch_block,
            scratch_block,
            scratch_block,
            scratch_block,
            swap_block,
            swap_block,
            gather_sem,
            gather_sem,
            line_sem,
            line_sem,
            line_sem,
            line_sem,
            swap_sem,
            swap_sem,
            old_block,
            old_block,
            swap_sem,
            swap_sem,
            pltpu.VMEM((2 * depth, heads * HEAD), jnp.bfloat16),
            pltpu.VMEM((chunks, rows, HEAD), jnp.bfloat16),
            pltpu.SemaphoreType.DMA((2,)),
            pltpu.SemaphoreType.DMA((2, chunks)),
        ],
        compiler_params=pltpu.CompilerParams(
            collective_id=0, has_side_effects=True, vmem_limit_bytes=56 * 2**20
        ),
        cost_estimate=pl.CostEstimate(
            flops=60_000_000_000, bytes_accessed=4 * tokens * depth, transcendentals=0
        ),
    )(perm, place, live, context.reshape(places, 2, half, HEAD), w_out_t, residual, gains)


def per_device(
    x_old, old_blocks, new_blocks, order, pre_gain, post_gain, w_query, w_key, w_value, w_out_t
):
    seq_count = lax.axis_size("seq")
    tp_count = lax.axis_size("tp")
    capacity, quarter = x_old.shape
    width = quarter * tp_count
    tokens = seq_count * capacity // 2
    own = tokens // seq_count
    share = capacity // tp_count
    seq_index = lax.axis_index("seq")
    tp_index = lax.axis_index("tp")
    heads = w_query.shape[1] // HEAD
    kv_heads = w_key.shape[1] // HEAD
    scale = (width // (heads * tp_count)) ** (-0.5)
    gains = jnp.stack([pre_gain, post_gain])
    if front_fits(seq_count, tp_count, heads, kv_heads, capacity):
        context, rows = front_phase(
            x_old, old_blocks, order, gains, w_query, w_key, w_value, seq_count, tp_count, scale
        )
        return output_phase(
            context, w_out_t, rows, gains, new_blocks, seq_count, tp_count, heads
        )
    old_start = offsets(old_blocks)
    new_start = offsets(new_blocks)
    device_ids = jnp.arange(seq_count, dtype=jnp.int32)

    gathered = lax.all_gather(x_old, "seq", axis=0, tiled=True)

    def stored(row, count):
        row = jnp.minimum(row, tokens - count)
        shard = jnp.sum((old_start <= row).astype(jnp.int32)) - 1
        holder = jnp.sum(jnp.where(order == shard, device_ids, 0))
        begin = jnp.sum(jnp.where(device_ids == shard, old_start, 0))
        return lax.dynamic_slice_in_dim(gathered, holder * capacity + row - begin, count, 0)

    def shift(k):
        return [(i, (i + k) % tp_count) for i in range(tp_count)]

    def by_source(received):
        stack = jnp.stack(received)
        pieces = [
            lax.dynamic_index_in_dim(stack, lax.rem(tp_index - u + tp_count, tp_count), 0, False)
            for u in range(tp_count)
        ]
        return jnp.concatenate(pieces, axis=1)

    mine = jnp.concatenate(
        [stored(seq_index * own + at, BLOCK) for at in range(0, own, BLOCK)], axis=0
    )
    full_rows = by_source(
        [mine] + [lax.ppermute(mine, "tp", shift(k)) for k in range(1, tp_count)]
    )
    my_start = jnp.sum(jnp.where(device_ids == seq_index, new_start, 0))

    def slot_rows(place):
        return stored(my_start + place * share, share)

    residual = by_source(
        [slot_rows(tp_index)]
        + [
            lax.ppermute(slot_rows(lax.rem(tp_index + k, tp_count)), "tp", shift(k))
            for k in range(1, tp_count)
        ]
    )

    weights = lax.all_gather(
        jnp.concatenate([w_query, w_key, w_value], axis=1), "seq", axis=0, tiled=True
    )

    normed = rms_scale(full_rows.astype(jnp.float32), pre_gain).astype(jnp.bfloat16)
    normed, residual = lax.optimization_barrier((normed, residual))
    group = heads // kv_heads
    copies = seq_count // heads
    raw = jnp.dot(normed, weights, preferred_element_type=jnp.float32)

    half = HEAD // 2
    inverse = jnp.exp(jnp.arange(half, dtype=jnp.float32) * (-2.0 * math.log(10000.0) / HEAD))
    places = seq_index * own + jnp.arange(own, dtype=jnp.int32)
    angles = places.astype(jnp.float32)[:, None] * inverse[None, :]
    cosine, sine = jnp.cos(angles), jnp.sin(angles)

    def rotate(at):
        first = raw[:, at * HEAD : at * HEAD + half]
        second = raw[:, at * HEAD + half : (at + 1) * HEAD]
        return jnp.concatenate(
            [first * cosine - second * sine, second * cosine + first * sine], axis=-1
        )

    queries = [(rotate(h) * scale).astype(jnp.bfloat16) for h in range(heads)]
    keys = [rotate(heads + g).astype(jnp.bfloat16) for g in range(kv_heads)]
    values = [
        raw[:, (heads + kv_heads + g) * HEAD : (heads + kv_heads + g + 1) * HEAD].astype(
            jnp.bfloat16
        )
        for g in range(kv_heads)
    ]
    sent = jnp.stack(
        [
            jnp.stack([queries[s // copies], keys[s // copies // group], values[s // copies // group]])
            for s in range(seq_count)
        ]
    )
    came = lax.all_to_all(sent, "seq", 0, 0, tiled=True)
    context = attention(
        came[:, 0].reshape(tokens, HEAD),
        came[:, 1].reshape(tokens, HEAD),
        came[:, 2].reshape(tokens, HEAD),
    )
    return output_phase(
        context, w_out_t, residual, gains, new_blocks, seq_count, tp_count, heads
    )


def solution(mesh):
    placed = (
        P("seq", "tp"),
        P(),
        P(),
        P(),
        P(),
        P(),
        P("seq", "tp"),
        P("seq", "tp"),
        P("seq", "tp"),
        P("seq", "tp"),
    )
    return jax.shard_map(
        per_device, mesh=mesh, in_specs=placed, out_specs=P(("seq", "tp"), None), check_vma=False
    )
```

```python
import functools
import math

import jax
import jax.numpy as jnp
import numpy as np
from jax import lax
from jax.experimental import pallas as pl
from jax.experimental.pallas import tpu as pltpu
from jax.sharding import PartitionSpec as P

HEAD = 128
BLOCK = 128
EPS = 1e-06
LAG = 4


def offsets(blocks):
    return (jnp.cumsum(blocks) - blocks) * BLOCK


def rms_scale(values, gain):
    return values * lax.rsqrt(jnp.mean(values * values, axis=-1, keepdims=True) + EPS) * gain


def attention_kernel(rows, span, q_ref, k_ref, v_ref, out_ref):
    first = pl.program_id(0) * rows
    query = q_ref[...]

    def step(at, carry, masked):
        numer, denom = carry
        start = pl.multiple_of(at * span, span)
        score = lax.dot_general(
            query,
            k_ref[pl.ds(start, span), :],
            (((1,), (1,)), ((), ())),
            preferred_element_type=jnp.float32,
        )
        weight = jnp.exp(50.0 * jnp.tanh(score * (1.0 / 50.0)))
        if masked:
            places = first + lax.broadcasted_iota(jnp.int32, weight.shape, 0)
            keys = start + lax.broadcasted_iota(jnp.int32, weight.shape, 1)
            weight = jnp.where(keys <= places, weight, 0.0)
        denom = denom + jnp.sum(weight, axis=1, keepdims=True)
        numer = numer + jnp.dot(
            weight.astype(jnp.bfloat16),
            v_ref[pl.ds(start, span), :],
            preferred_element_type=jnp.float32,
        )
        return numer, denom

    whole = first // span
    state = (jnp.zeros((rows, HEAD), jnp.float32), jnp.zeros((rows, 1), jnp.float32))
    state = lax.fori_loop(0, whole, lambda at, c: step(at, c, False), state)
    numer, denom = step(whole, state, True)
    out_ref[...] = (numer / denom).astype(out_ref.dtype)


def attention(query, key, value):
    tokens = query.shape[0]
    rows, span = 256, 512
    return pl.pallas_call(
        functools.partial(attention_kernel, rows, span),
        grid=(tokens // rows,),
        in_specs=[
            pl.BlockSpec((rows, HEAD), lambda i: (i, 0)),
            pl.BlockSpec((tokens, HEAD), lambda i: (0, 0)),
            pl.BlockSpec((tokens, HEAD), lambda i: (0, 0)),
        ],
        out_specs=pl.BlockSpec((rows, HEAD), lambda i: (i, 0)),
        out_shape=jax.ShapeDtypeStruct((tokens, HEAD), jnp.bfloat16),
        cost_estimate=pl.CostEstimate(
            flops=3 * tokens * tokens * HEAD,
            bytes_accessed=8 * tokens * HEAD,
            transcendentals=tokens * tokens,
        ),
    )(query, key, value)


MESH = pl.DeviceIdType.MESH


def arrangements(seq_count):
    found = []
    for second in range(1, seq_count + 1):
        for third in range(1, second + 1):
            fourth = seq_count - second - third
            if 1 <= fourth <= third:
                found.append((seq_count, second, third, fourth))
    return found


def layer_windows(seq_count, tp_count, per_block):
    first, last = [], []
    for layer in range(tp_count):
        starts, ends = [], []
        for counts in arrangements(seq_count):
            begin = sum(counts[u // per_block] for u in range(layer))
            starts.append(begin)
            ends.append(begin + counts[layer // per_block])
        first.append(min(starts))
        last.append(max(ends))
    return first, last


def pick(index, values):
    result = jnp.int32(values[0])
    for k in range(1, len(values)):
        result = jnp.where(index == k, jnp.int32(values[k]), result)
    return result


def flipped(index, mask):
    result = index
    bit = 1
    while bit <= mask:
        if mask & bit:
            result = result + bit - 2 * bit * lax.rem(index // bit, 2)
        bit *= 2
    return result


def output_kernel(
    heads,
    copies,
    seq_count,
    tp_count,
    share,
    first,
    last,
    scattered,
    perm_ref,
    place_ref,
    block_ref,
    context_ref,
    weight_ref,
    residual_ref,
    gain_ref,
    out_ref,
    full,
    partial,
    left_in,
    right_in,
    left_out,
    right_out,
    total,
    sent,
    came,
    gather_send,
    gather_recv,
    left_send,
    left_recv,
    right_send,
    right_recv,
    swap_send,
    swap_recv,
    old_sent,
    old_came,
    old_send,
    old_recv,
    weight,
    staged,
    weight_sem,
    staged_sem,
):
    seq_index = lax.axis_index("seq")
    tp_index = lax.axis_index("tp")
    places = partial.shape[0]
    depth = weight_ref.shape[0]
    half = partial.shape[1]
    core = lax.rem(seq_index, 2)
    partner = seq_index + 1 - 2 * core
    shared = copies == 1
    unit = 2 if shared else copies
    span = 2 * HEAD if shared else HEAD
    slot_index = seq_index // unit
    chunks = full.shape[0]
    per_chunk = places // chunks

    barrier = pltpu.get_barrier_semaphore()
    for k in range(1, seq_count):
        pl.semaphore_signal(
            barrier,
            inc=1,
            device_id=(lax.rem(seq_index + k, seq_count), tp_index),
            device_id_type=MESH,
        )

    @pl.when(tp_index > 0)
    def _():
        pl.semaphore_signal(
            barrier, inc=1, device_id=(seq_index, tp_index - 1), device_id_type=MESH
        )

    @pl.when(tp_index < tp_count - 1)
    def _():
        pl.semaphore_signal(
            barrier, inc=1, device_id=(seq_index, tp_index + 1), device_id_type=MESH
        )

    if scattered:
        per_block = BLOCK // share
        counts = [perm_ref[j] * per_block for j in range(seq_count)]
        begins, begin = [], jnp.int32(0)
        for j in range(seq_count):
            begins.append(begin)
            begin = begin + counts[j]
        perm = [jnp.int32(0)] * places
        place_of = [jnp.int32(0)] * seq_count
        rank = jnp.int32(0)
        for layer in range(tp_count):
            for j in range(seq_count):
                valid = jnp.minimum(jnp.maximum(counts[j] - layer, 0), 1)
                for q in range(first[layer], last[layer]):
                    here = jnp.where(rank == q, valid, 0)
                    perm[q] = perm[q] + here * (begins[j] + layer)
                place_of[j] = place_of[j] + jnp.where(tp_index == layer, rank, 0)
                rank = rank + valid
        place_of = [jnp.minimum(place, places - 1) for place in place_of]
        block_of = [
            jnp.minimum((begins[j] + tp_index) // per_block, places // per_block - 1)
            for j in range(seq_count)
        ]
        mine = jnp.int32(0)
        for j in range(seq_count):
            mine = mine + jnp.where(seq_index == j, counts[j], 0)
        live = jnp.minimum(jnp.maximum(mine - tp_index, 0), 1)
    else:
        perm = [perm_ref[q] for q in range(places)]
        place_of = [place_ref[j] for j in range(seq_count)]
        live = block_ref[0]
    live = live.astype(jnp.float32)

    neighbours = jnp.where(tp_index > 0, 1, 0) + jnp.where(tp_index < tp_count - 1, 1, 0)
    pl.semaphore_wait(barrier, seq_count - 1 + neighbours)

    bits = (seq_count // unit).bit_length() - 1
    order = list(range(chunks))[::-1]
    head = seq_index // copies
    own_columns = pl.ds(pl.multiple_of(head * HEAD, HEAD), HEAD)

    def staged_copy(chunk):
        return pltpu.make_async_remote_copy(
            src_ref=staged.at[chunk],
            dst_ref=full.at[chunk, :, own_columns],
            send_sem=staged_sem.at[0, chunk],
            recv_sem=staged_sem.at[1, chunk],
            device_id=(partner, tp_index),
            device_id_type=MESH,
        )

    own_rows = pl.ds(pl.multiple_of(core * depth, depth), depth)
    weight_copy = pltpu.make_async_remote_copy(
        src_ref=weight_ref,
        dst_ref=weight.at[own_rows],
        send_sem=weight_sem.at[0],
        recv_sem=weight_sem.at[1],
        device_id=(partner, tp_index),
        device_id_type=MESH,
    )

    for chunk in order:
        for at in range(per_chunk):
            source = perm[chunk * per_chunk + at]
            rows = slice(at * half, (at + 1) * half)
            full[chunk, rows, own_columns] = context_ref[source, core]
            if shared:
                staged[chunk, rows] = context_ref[source, 1 - core]
        if shared:
            staged_copy(chunk).start()
    weight_copy.start()

    def dims(chunk):
        outer = list(range(bits))
        return outer[::-1] if chunk % 2 else outer

    def gather_copy(chunk, bit, combo, to_me):
        slot = flipped(slot_index, (combo ^ (1 << bit)) if to_me else combo)
        view = full.at[chunk, :, pl.ds(pl.multiple_of(slot * span, span), span)]
        return pltpu.make_async_remote_copy(
            src_ref=view,
            dst_ref=view,
            send_sem=gather_send.at[chunk, bit, combo],
            recv_sem=gather_recv.at[chunk, bit, combo],
            device_id=(flipped(seq_index, unit << bit), tp_index),
            device_id_type=MESH,
        )

    def steps(chunk):
        held = [0]
        for bit in dims(chunk):
            yield bit, list(held)
            held = held + [c ^ (1 << bit) for c in held]

    def offer(at):
        if at < chunks:
            if shared:
                staged_copy(order[at]).wait_recv()
            for bit, _ in steps(order[at]):
                gather_copy(order[at], bit, 0, False).start()

    offer(0)
    weight[own_rows] = weight_ref[...]
    total[...] = jnp.zeros_like(total)

    def relay(at):
        chunk = order[at]
        stages = list(steps(chunk))
        for level, (bit, held) in enumerate(stages):
            for combo in held:
                gather_copy(chunk, bit, combo, True).wait_recv()
                for later, _ in stages[level + 1 :]:
                    gather_copy(chunk, later, combo ^ (1 << bit), False).start()
            if level == 0:
                offer(at + 1)

    def multiply(chunk):
        product = lax.dot_general(
            full[chunk],
            weight[...],
            (((1,), (1,)), ((), ())),
            preferred_element_type=jnp.float32,
        ).astype(jnp.bfloat16)
        for at in range(per_chunk):
            partial[chunk * per_chunk + at] = product[at * half : (at + 1) * half]

    left_has = jnp.where(tp_index < tp_count - 1, pick(tp_index, last), 0)
    left_gives = pick(tp_index, [0] + last[:-1])
    right_has = jnp.where(tp_index > 0, pick(tp_index, first), places)
    right_gives = pick(tp_index, first[1:] + [places])

    def line_copy(place, source, landing, send, recv, step):
        return pltpu.make_async_remote_copy(
            src_ref=source.at[place],
            dst_ref=landing.at[place],
            send_sem=send.at[place],
            recv_sem=recv.at[place],
            device_id=(seq_index, tp_index + step),
            device_id_type=MESH,
        )

    def flow(place, has, gives, source, landing, send, recv, step):
        @pl.when(has)
        def _():
            line_copy(place, source, landing, send, recv, step).wait_recv()

        @pl.when(jnp.logical_and(has, gives))
        def _():
            source[place] = (
                partial[place].astype(jnp.float32) + landing[place].astype(jnp.float32)
            ).astype(jnp.bfloat16)

        @pl.when(jnp.logical_and(jnp.logical_not(has), gives))
        def _():
            source[place] = partial[place]

        @pl.when(gives)
        def _():
            line_copy(place, source, landing, send, recv, step).start()

    def swap_copy(other, mine, at):
        return pltpu.make_async_remote_copy(
            src_ref=sent.at[other],
            dst_ref=came.at[mine],
            send_sem=swap_send.at[at],
            recv_sem=swap_recv.at[at],
            device_id=(other, tp_index),
            device_id_type=MESH,
        )

    def line_step(at, carry):
        passed = at - LAG * (tp_count - 1 - tp_index)
        place = places - 1 - passed
        valid = jnp.logical_and(passed >= 0, passed < places)
        has = jnp.logical_and(valid, place < left_has)
        gives = jnp.logical_and(valid, place < left_gives)
        flow(place, has, gives, left_out, left_in, left_send, left_recv, -1)
        ends = jnp.logical_and(
            jnp.logical_and(valid, tp_index == 0), place < seq_count
        )

        @pl.when(ends)
        def _():
            sent[place] = (
                partial[place].astype(jnp.float32) + left_in[place].astype(jnp.float32)
            ).astype(jnp.bfloat16)

            @pl.when(place == seq_index)
            def _():
                came[place] = sent[place]

            @pl.when(place != seq_index)
            def _():
                swap_copy(
                    place, seq_index, lax.rem(place + seq_count - seq_index, seq_count)
                ).start()

        passed = at - LAG * tp_index
        place = places - 1 - passed
        valid = jnp.logical_and(passed >= 0, passed < places)
        has = jnp.logical_and(valid, place >= right_has)
        gives = jnp.logical_and(valid, place >= right_gives)
        flow(place, has, gives, right_out, right_in, right_send, right_recv, 1)
        return carry

    def old_copy(other, mine, at):
        return pltpu.make_async_remote_copy(
            src_ref=old_sent.at[other],
            dst_ref=old_came.at[mine],
            send_sem=old_send.at[at],
            recv_sem=old_recv.at[at],
            device_id=(other, tp_index),
            device_id_type=MESH,
        )

    for at, chunk in enumerate(order):
        relay(at)
        if at == 0:
            weight_from = pltpu.make_async_remote_copy(
                src_ref=weight_ref,
                dst_ref=weight.at[pl.ds(pl.multiple_of((1 - core) * depth, depth), depth)],
                send_sem=weight_sem.at[0],
                recv_sem=weight_sem.at[1],
                device_id=(partner, tp_index),
                device_id_type=MESH,
            )
            weight_from.wait_recv()
        multiply(chunk)
        if scattered and at == chunks - 1:
            for j in range(seq_count):
                old_sent[j] = residual_ref[block_of[j]]
            for k in range(1, seq_count):
                old_copy(lax.rem(seq_index + k, seq_count), seq_index, k).start()
            old_came[seq_index] = old_sent[seq_index]
        lax.fori_loop(at * per_chunk, (at + 1) * per_chunk, line_step, 0)
    lax.fori_loop(places, places + LAG * (tp_count - 1), line_step, 0)

    def sum_step(place, carry):
        value = partial[place].astype(jnp.float32) + right_in[place].astype(jnp.float32)

        @pl.when(place < left_has)
        def _():
            total[place] = (value + left_in[place].astype(jnp.float32)).astype(jnp.bfloat16)

        @pl.when(place >= left_has)
        def _():
            total[place] = value.astype(jnp.bfloat16)

        return carry

    @pl.when(tp_index > 0)
    def _():
        lax.fori_loop(pick(tp_index, first), pick(tp_index, last), sum_step, 0)
        for j in range(seq_count):
            sent[j] = total[place_of[j]]
        for k in range(1, seq_count):
            swap_copy(lax.rem(seq_index + k, seq_count), seq_index, k).start()
        came[seq_index] = sent[seq_index]

    for k in range(1, seq_count):
        swap_copy(
            lax.rem(seq_index + k, seq_count),
            lax.rem(seq_index + seq_count - k, seq_count),
            k,
        ).wait_recv()

    if scattered:
        for k in range(1, seq_count):
            old_copy(
                lax.rem(seq_index + k, seq_count),
                lax.rem(seq_index + seq_count - k, seq_count),
                k,
            ).wait_recv()
    wide = 2 * depth
    for side in range(2):
        square = jnp.zeros((half, 1), jnp.float32)
        for c in range(seq_count // 2):
            piece = came[2 * c + side].astype(jnp.float32)
            square = square + jnp.sum(piece * piece, axis=1, keepdims=True)
        factor = lax.rsqrt(square * (1.0 / (depth * seq_count)) + EPS)
        rows = slice(side * half, (side + 1) * half)
        width = HEAD if scattered else wide
        for c in range(seq_count // 2):
            for begin in range(0, wide, width):
                part = slice(begin, begin + width)
                columns = slice(c * wide + begin, c * wide + begin + width)
                row = (c * wide + begin) // HEAD
                if scattered:
                    old, gain = old_came[2 * c + side, :, part], gain_ref[row : row + 1, :]
                else:
                    old, gain = residual_ref[rows, columns], gain_ref[:, columns]
                value = old.astype(jnp.float32) + (
                    came[2 * c + side, :, part].astype(jnp.float32) * factor * gain
                )
                out_ref[rows, columns] = (value * live).astype(jnp.bfloat16)

    for k in range(1, seq_count):
        swap_copy(lax.rem(seq_index + k, seq_count), seq_index, k).wait_send()
    if scattered:
        for k in range(1, seq_count):
            old_copy(lax.rem(seq_index + k, seq_count), seq_index, k).wait_send()
    weight_copy.wait_send()
    for chunk in range(chunks):
        if shared:
            staged_copy(chunk).wait_send()
        for bit, held in steps(chunk):
            for combo in held:
                gather_copy(chunk, bit, combo, False).wait_send()

    def drain(place, carry):
        @pl.when(place < left_gives)
        def _():
            line_copy(place, left_out, left_in, left_send, left_recv, -1).wait_send()

        @pl.when(place >= right_gives)
        def _():
            line_copy(place, right_out, right_in, right_send, right_recv, 1).wait_send()

        return carry

    lax.fori_loop(0, places, drain, 0)


def front_kernel(
    seq_count,
    tp_count,
    group,
    scale,
    blocks_ref,
    order_ref,
    x_ref,
    gain_ref,
    query_ref,
    key_ref,
    value_ref,
    angle_ref,
    context_out,
    x_out,
    q_buf,
    kv_buf,
    near,
    send_a,
    send_b,
    far,
    line,
    twin,
    weight,
    normed,
    scale_row,
    scale_all,
    scale_column,
    first_out,
    first_in,
    second_out,
    second_in,
    kept,
    core_sem,
    weight_sem,
    stage_sem,
    line_send,
    line_recv,
    plane_send,
    plane_recv,
    twin_sem,
    stat_sem,
    factor_sem,
    first_sem,
    second_sem,
    kv_sem,
):
    seq_index = lax.axis_index("seq")
    tp_index = lax.axis_index("tp")
    chip = seq_index // 2
    core = lax.rem(seq_index, 2)
    partner = seq_index + 1 - 2 * core
    slots = x_ref.shape[0]
    chips = seq_count // 2
    each = line.shape[1]
    half = line.shape[2]
    quarter = line.shape[3]
    depth = query_ref.shape[0]
    pair = 2 * HEAD

    barrier = pltpu.get_barrier_semaphore()
    for k in range(1, seq_count):
        other = lax.rem(seq_index + k, seq_count)
        pl.semaphore_signal(barrier, inc=1, device_id=(other, tp_index), device_id_type=MESH)
    for k in range(1, tp_count):
        other = lax.rem(tp_index + k, tp_count)
        pl.semaphore_signal(barrier, inc=1, device_id=(seq_index, other), device_id_type=MESH)

    def remote(source, target, sems, at, seq, tp):
        return pltpu.make_async_remote_copy(
            src_ref=source,
            dst_ref=target,
            send_sem=sems[0].at[at],
            recv_sem=sems[1].at[at],
            device_id=(seq, tp),
            device_id_type=MESH,
        )

    core_sems = (core_sem.at[0], core_sem.at[1])

    def swap_slots(holder):
        return remote(
            x_ref.at[:, 1 - core],
            near.at[pl.ds(slots * holder, slots)],
            core_sems,
            0,
            partner,
            tp_index,
        )

    def lanes(head, count=1):
        return pl.ds(pl.multiple_of(head * HEAD, HEAD), count * HEAD)

    def weight_copy(source, column, target, at, holder):
        return remote(
            source.at[:, lanes(column)],
            weight.at[pl.ds(pl.multiple_of(holder * depth, depth), depth), lanes(target)],
            (weight_sem.at[0], weight_sem.at[1]),
            at,
            partner,
            tp_index,
        )

    pl.semaphore_wait(barrier, seq_count - 1 + tp_count - 1)
    swap_slots(core).start()
    for slot in range(slots):
        near[slots * core + slot] = x_ref[slot, core]

    starts, counts, holders = [], [], []
    begin = jnp.int32(0)
    for k in range(seq_count):
        starts.append(begin)
        counts.append(blocks_ref[k])
        begin = begin + blocks_ref[k]
        holder = jnp.int32(0)
        for place in range(1, seq_count):
            holder = holder + jnp.where(order_ref[place] == k, jnp.int32(place), jnp.int32(0))
        holders.append(holder)

    def found(block):
        at = jnp.int32(0)
        for k in range(seq_count):
            inside = jnp.logical_and(starts[k] <= block, block < starts[k] + counts[k])
            at = at + jnp.where(inside, holders[k] * slots + block - starts[k], jnp.int32(0))
        return at // (2 * slots), lax.rem(at, 2 * slots)

    first_chip = jnp.where(core == 0, flipped(chip, 1), flipped(chip, 2))
    second_chip = jnp.where(core == 0, flipped(chip, 2), flipped(chip, 1))
    cross_chip = flipped(chip, 3)
    stage_sems = (stage_sem.at[0], stage_sem.at[1])
    table_a = []
    for at in range(2 * each):
        target = first_chip if at < each else cross_chip
        owner, index = found(chips * (at % each) + target)
        table_a.append(jnp.where(owner == chip, index, 0))
    swap_slots(1 - core).wait_recv()
    across_first = list(range(each, 2 * each)) + list(range(each))
    for at in across_first:
        send_a[at] = near[table_a[at]]
        remote(
            send_a.at[at], far.at[at], stage_sems, at, 2 * first_chip + core, tp_index
        ).start()

    for c in range(chips):
        weight_copy(query_ref, 2 * c + 1 - core, 2 * c, 2 * c, core).start()

        @pl.when(core == 0)
        def _():
            weight_copy(value_ref, c, 2 * c + 1, 2 * c + 1, core).start()

        @pl.when(core == 1)
        def _():
            weight_copy(key_ref, c, 2 * c + 1, 2 * c + 1, core).start()

    own_rows = pl.ds(pl.multiple_of(core * depth, depth), depth)
    for c in range(chips):
        weight[own_rows, pl.ds(2 * c * HEAD, HEAD)] = query_ref[:, lanes(2 * c + core)]

        @pl.when(core == 0)
        def _():
            weight[own_rows, pl.ds((2 * c + 1) * HEAD, HEAD)] = key_ref[
                :, pl.ds(c * HEAD, HEAD)
            ]

        @pl.when(core == 1)
        def _():
            weight[own_rows, pl.ds((2 * c + 1) * HEAD, HEAD)] = value_ref[
                :, pl.ds(c * HEAD, HEAD)
            ]

    def arrive_a(at):
        remote(
            send_a.at[at], far.at[at], stage_sems, at, 2 * first_chip + core, tp_index
        ).wait_recv()

    both = 2 * slots
    for at in range(each, 2 * each):
        arrive_a(at)
        near[both + at] = far[at]
    for at in range(each):
        owner, index = found(chips * at + second_chip)
        send_b[at] = near[jnp.where(owner == chip, index, both + each + at)]
        remote(
            send_b.at[at],
            far.at[2 * each + at],
            stage_sems,
            2 * each + at,
            2 * second_chip + core,
            tp_index,
        ).start()
    for at in range(each):
        arrive_a(at)
        near[both + at] = far[at]
    for at in range(each):
        owner, index = found(chips * at + chip)
        near[both + 2 * each + at] = near[jnp.where(owner == chip, index, both + at)]
    for at in range(each):
        remote(
            send_b.at[at],
            far.at[2 * each + at],
            stage_sems,
            2 * each + at,
            2 * second_chip + core,
            tp_index,
        ).wait_recv()
        near[both + 3 * each + at] = far[2 * each + at]
    for at in range(each):
        owner, _ = found(chips * at + chip)
        local = jnp.logical_or(owner == chip, owner == first_chip)
        line[tp_index, at] = near[
            jnp.where(local, both + 2 * each + at, both + 3 * each + at)
        ]

    def line_copy(layer, at, step):
        view = line.at[layer, at]
        return pltpu.make_async_remote_copy(
            src_ref=view,
            dst_ref=view,
            send_sem=line_send.at[(step + 1) // 2, layer, at],
            recv_sem=line_recv.at[layer, at],
            device_id=(seq_index, tp_index + step),
            device_id_type=MESH,
        )

    def plane_copy(layer, at, holder):
        return pltpu.make_async_remote_copy(
            src_ref=line.at[layer, at],
            dst_ref=x_out.at[chips * at + holder],
            send_sem=plane_send.at[layer, at],
            recv_sem=plane_recv.at[chips * at + holder],
            device_id=(2 * layer + core, tp_index),
            device_id_type=MESH,
        )

    def twin_copy(block):
        return remote(
            x_out.at[block],
            twin.at[block],
            (twin_sem.at[0], twin_sem.at[1]),
            block,
            partner,
            tp_index,
        )

    def guarded(condition, action):
        @pl.when(condition)
        def _():
            action()

    def forward(layer, at):
        @pl.when(layer == chip)
        def _():
            x_out[chips * at + chip] = line[layer, at]

        @pl.when(layer != chip)
        def _():
            plane_copy(layer, at, chip).start()

    def own_step(at):
        guarded(tp_index > 0, lambda: line_copy(tp_index, at, -1).start())
        guarded(tp_index < tp_count - 1, lambda: line_copy(tp_index, at, 1).start())
        forward(tp_index, at)

    def hop_step(at, distance):
        @pl.when(tp_index >= distance)
        def _():
            layer = tp_index - distance
            line_copy(layer, at, 1).wait_recv()
            guarded(tp_index < tp_count - 1, lambda: line_copy(layer, at, 1).start())
            forward(layer, at)

        @pl.when(tp_index + distance < tp_count)
        def _():
            layer = tp_index + distance
            line_copy(layer, at, -1).wait_recv()
            guarded(tp_index > 0, lambda: line_copy(layer, at, -1).start())
            forward(layer, at)

    def plane_step(at):
        for c in range(chips):

            @pl.when(chip != c)
            def _():
                plane_copy(chip, at, c).wait_recv()

        for c in range(chips):
            twin_copy(chips * at + c).start()

    tiles = quarter // HEAD

    def normalize(source, block, holder, target):
        rows = pl.ds(pl.multiple_of((block // chips) * half, half), half)
        factor = scale_column[holder, rows, :]
        for tile in range(tiles):
            columns = slice(tile * HEAD, (tile + 1) * HEAD)
            values = source[block, :, columns].astype(jnp.float32)
            gains = gain_ref[pl.ds(chip * tiles + tile, 1), :]
            normed[target[0], target[1], target[2], :, columns] = (
                values * factor * gains
            ).astype(jnp.bfloat16)

    bits = (1, 2)

    def first_copy(at, side):
        bit = bits[side]
        return pltpu.make_async_remote_copy(
            src_ref=first_out.at[at, side],
            dst_ref=first_in.at[at, side],
            send_sem=first_sem.at[0, at, side],
            recv_sem=first_sem.at[1, at, side],
            device_id=(2 * flipped(chip, bit) + core, tp_index),
            device_id_type=MESH,
        )

    def second_copy(at, side):
        bit = bits[1 - side]
        return pltpu.make_async_remote_copy(
            src_ref=second_out.at[at, side],
            dst_ref=second_in.at[at, side],
            send_sem=second_sem.at[0, at, side],
            recv_sem=second_sem.at[1, at, side],
            device_id=(2 * flipped(chip, bit) + core, tp_index),
            device_id_type=MESH,
        )

    def multiply_step(at):
        for side in range(2):
            for u in range(2):
                c = 2 * side + u
                block = chips * at + c
                twin_copy(block).wait_recv()
                normalize(x_out, block, 2 * c + core, (side, u, core))
                normalize(twin, block, 2 * c + 1 - core, (side, u, 1 - core))
            rows = normed[side].reshape(4 * half, quarter)

            def part(mask):
                target = flipped(chip, mask)
                return jnp.dot(
                    rows,
                    weight[:, lanes(2 * target, 2)],
                    preferred_element_type=jnp.float32,
                )

            first, second = bits[side], bits[1 - side]
            first_out[at, side, 0] = part(first).astype(jnp.bfloat16)
            first_out[at, side, 1] = part(3).astype(jnp.bfloat16)
            first_copy(at, side).start()
            kept[at, side, 0] = part(0)
            kept[at, side, 1] = part(second)

    def add_step(at):
        for side in range(2):
            first_copy(at, side).wait_recv()
            second_out[at, side] = (
                kept[at, side, 1] + first_in[at, side, 1].astype(jnp.float32)
            ).astype(jnp.bfloat16)
            second_copy(at, side).start()

    def kv_copy(kind, block):
        rows = pl.ds(pl.multiple_of(block * BLOCK, BLOCK), BLOCK)
        view = kv_buf.at[kind, rows, :]
        return remote(
            view, view, (kv_sem.at[0], kv_sem.at[1]), block, partner, tp_index
        )

    lane = lax.broadcasted_iota(jnp.int32, (BLOCK, HEAD), 1)

    def turned(values, rows):
        angles = angle_ref[rows, :]
        swapped = pltpu.roll(angles, HEAD // 2, 1)
        low = lane < HEAD // 2
        cosine = jnp.where(low, angles, swapped)
        sine = jnp.where(low, -swapped, angles)
        return values * cosine + pltpu.roll(values, HEAD // 2, 1) * sine

    def finish_step(at):
        for side in range(2):
            second_copy(at, side).wait_recv()
            for u in range(2):
                block = chips * at + 2 * side + u
                part = slice(u * BLOCK, (u + 1) * BLOCK)
                value = (
                    kept[at, side, 0, part]
                    + first_in[at, side, 0, part].astype(jnp.float32)
                    + second_in[at, side, part].astype(jnp.float32)
                )
                rows = pl.ds(pl.multiple_of(block * BLOCK, BLOCK), BLOCK)
                q_buf[rows, :] = (turned(value[:, :HEAD], rows) * scale).astype(jnp.bfloat16)

                @pl.when(core == 0)
                def _():
                    kv_buf[0, rows, :] = turned(value[:, HEAD:], rows).astype(jnp.bfloat16)

                @pl.when(core == 1)
                def _():
                    kv_buf[1, rows, :] = value[:, HEAD:].astype(jnp.bfloat16)

                kv_copy(core, block).start()

    span = chips * BLOCK
    sub = span // 2
    mask = lax.broadcasted_iota(jnp.int32, (sub, sub), 1) <= lax.broadcasted_iota(
        jnp.int32, (sub, sub), 0
    )

    def attend_step(at):
        for c in range(chips):
            kv_copy(1 - core, chips * at + c).wait_recv()

        def attend(query, start, count, carry, masked):
            keys = pl.ds(pl.multiple_of(start, sub), count)
            score = lax.dot_general(
                query,
                kv_buf[0, keys, :],
                (((1,), (1,)), ((), ())),
                preferred_element_type=jnp.float32,
            )
            part = jnp.exp2((50.0 / math.log(2.0)) * jnp.tanh(score * (1.0 / 50.0)))
            if masked:
                part = jnp.where(mask, part, 0.0)
            numer, denom = carry
            denom = denom + jnp.sum(part, axis=1, keepdims=True)
            numer = numer + jnp.dot(
                part.astype(jnp.bfloat16), kv_buf[1, keys, :], preferred_element_type=jnp.float32
            )
            return numer, denom

        every = q_buf[pl.ds(pl.multiple_of(at * span, span), span), :]
        numers, denoms = lax.fori_loop(
            0,
            2 * at,
            lambda n, carry: attend(every, n * sub, sub, carry, False),
            (jnp.zeros((span, HEAD), jnp.float32), jnp.zeros((span, 1), jnp.float32)),
        )
        for piece in range(2):
            begin = at * span + piece * sub
            rows = pl.ds(pl.multiple_of(begin, sub), sub)
            query = q_buf[rows, :]
            part = slice(piece * sub, (piece + 1) * sub)
            state = (numers[part], denoms[part])
            if piece:
                state = attend(query, at * span, sub, state, False)
            numer, denom = attend(query, begin, sub, state, True)
            context_out[rows, :] = (numer / denom).astype(jnp.bfloat16)

    def stat_copy(layer_from, layer_to):
        return pltpu.make_async_remote_copy(
            src_ref=scale_row.at[layer_from],
            dst_ref=scale_row.at[layer_from],
            send_sem=stat_sem.at[0, layer_to],
            recv_sem=stat_sem.at[1, layer_from],
            device_id=(seq_index, layer_to),
            device_id_type=MESH,
        )

    def factor_copy(holder, other):
        return pltpu.make_async_remote_copy(
            src_ref=scale_all.at[holder],
            dst_ref=scale_all.at[holder],
            send_sem=factor_sem.at[0, other],
            recv_sem=factor_sem.at[1, holder],
            device_id=(other, tp_index),
            device_id_type=MESH,
        )

    own_step(0)
    squares = []
    for at in range(each):
        values = line[tp_index, at].astype(jnp.float32)
        squares.append(jnp.sum(values * values, axis=1, keepdims=True))
    column = jnp.broadcast_to(jnp.concatenate(squares, axis=0), (each * half, HEAD))
    scale_row[tp_index] = jnp.transpose(column)[:8, :]
    for k in range(1, tp_count):
        stat_copy(tp_index, lax.rem(tp_index + k, tp_count)).start()
    for c in range(2 * chips):
        weight_copy(query_ref, 0, 0, c, 1 - core).wait_recv()
    for k in range(1, tp_count):
        other = lax.rem(tp_index + k, tp_count)
        stat_copy(other, tp_index).wait_recv()
    square = scale_row[0]
    for k in range(1, tp_count):
        square = square + scale_row[k]
    scale_all[seq_index] = lax.rsqrt(square * (1.0 / (quarter * tp_count)) + EPS)
    for k in range(1, seq_count):
        factor_copy(seq_index, lax.rem(seq_index + k, seq_count)).start()

    def steps(i, carry):
        for lag, action in (
            (0, lambda at: guarded(at > 0, lambda: own_step(at))),
            (1, lambda at: hop_step(at, 1)),
            (2, lambda at: hop_step(at, 2)),
            (3, lambda at: hop_step(at, 3)),
            (4, plane_step),
            (5, multiply_step),
            (6, add_step),
            (7, finish_step),
            (8, attend_step),
        ):
            at = i - lag

            @pl.when(jnp.logical_and(at >= 0, at < each))
            def _():
                action(at)

        return carry

    lax.fori_loop(0, 5, steps, 0)
    for k in range(1, seq_count):
        other = lax.rem(seq_index + k, seq_count)
        factor_copy(other, seq_index).wait_recv()
    for s in range(seq_count):
        scale_column[s] = jnp.transpose(
            jnp.broadcast_to(scale_all[s, :1, :], (HEAD, each * half))
        )
    lax.fori_loop(5, each + 8, steps, 0)

    swap_slots(core).wait_send()
    for c in range(2 * chips):
        weight_copy(query_ref, 0, 0, c, core).wait_send()
    for at in range(2 * each):
        remote(
            send_a.at[at], far.at[at], stage_sems, at, 2 * first_chip + core, tp_index
        ).wait_send()
    for at in range(each):
        remote(
            send_b.at[at],
            far.at[2 * each + at],
            stage_sems,
            2 * each + at,
            2 * second_chip + core,
            tp_index,
        ).wait_send()
    for k in range(1, tp_count):
        stat_copy(tp_index, lax.rem(tp_index + k, tp_count)).wait_send()
    for k in range(1, seq_count):
        factor_copy(seq_index, lax.rem(seq_index + k, seq_count)).wait_send()

    def drain(at, carry):
        for layer in range(tp_count):
            right = jnp.logical_and(tp_index >= layer, tp_index < tp_count - 1)
            guarded(right, lambda: line_copy(layer, at, 1).wait_send())
            left = jnp.logical_and(tp_index <= layer, tp_index > 0)
            guarded(left, lambda: line_copy(layer, at, -1).wait_send())
            guarded(chip != layer, lambda: plane_copy(layer, at, chip).wait_send())
        for side in range(2):
            first_copy(at, side).wait_send()
            second_copy(at, side).wait_send()
        for c in range(chips):
            twin_copy(chips * at + c).wait_send()
            kv_copy(core, chips * at + c).wait_send()
        return carry

    lax.fori_loop(0, each, drain, 0)


def front_fits(seq_count, tp_count, heads, kv_heads, capacity):
    return (
        heads == seq_count == 8
        and 2 * kv_heads == heads
        and tp_count == 4
        and capacity == 4 * BLOCK
    )


def front_phase(
    x_old, old_blocks, order, gains, w_query, w_key, w_value, seq_count, tp_count, scale
):
    capacity, quarter = x_old.shape
    depth = w_query.shape[0]
    slots = capacity // BLOCK
    half = BLOCK // 2
    tokens = seq_count * capacity // 2
    chips = seq_count // 2
    each = tokens // BLOCK // chips
    group = w_query.shape[1] // w_key.shape[1]
    angles = (
        np.arange(tokens, dtype=np.float32)[:, None]
        * np.exp(
            np.arange(HEAD // 2, dtype=np.float32) * np.float32(-2.0 * math.log(10000.0) / HEAD)
        )[None, :]
    )
    table = np.concatenate([np.cos(angles), np.sin(angles)], axis=1).astype(np.float32)
    bf16, f32 = jnp.bfloat16, jnp.float32
    piece = (half, quarter)
    dma = pltpu.SemaphoreType.DMA
    vmem = pl.BlockSpec(memory_space=pltpu.VMEM)
    smem = pl.BlockSpec(memory_space=pltpu.SMEM)
    square = (2 * BLOCK, 2 * HEAD)
    return pl.pallas_call(
        functools.partial(front_kernel, seq_count, tp_count, group, scale),
        out_shape=(
            jax.ShapeDtypeStruct((tokens, HEAD), bf16),
            jax.ShapeDtypeStruct((each * chips,) + piece, bf16),
        ),
        in_specs=[smem] * 2 + [vmem] * 6,
        out_specs=(vmem, vmem),
        scratch_shapes=[
            pltpu.VMEM((tokens, HEAD), bf16),
            pltpu.VMEM((2, tokens, HEAD), bf16),
            pltpu.VMEM((2 * slots + 4 * each,) + piece, bf16),
            pltpu.VMEM((2 * each,) + piece, bf16),
            pltpu.VMEM((each,) + piece, bf16),
            pltpu.VMEM((3 * each,) + piece, bf16),
            pltpu.VMEM((tp_count, each) + piece, bf16),
            pltpu.VMEM((each * chips,) + piece, bf16),
            pltpu.VMEM((2 * depth, 2 * chips * HEAD), bf16),
            pltpu.VMEM((2, 2, 2) + piece, bf16),
            pltpu.VMEM((tp_count, 8, each * half), f32),
            pltpu.VMEM((seq_count, 8, each * half), f32),
            pltpu.VMEM((seq_count, each * half, HEAD), f32),
            pltpu.VMEM((each, 2, 2) + square, bf16),
            pltpu.VMEM((each, 2, 2) + square, bf16),
            pltpu.VMEM((each, 2) + square, bf16),
            pltpu.VMEM((each, 2) + square, bf16),
            pltpu.VMEM((each, 2, 2) + square, f32),
            dma((2, 1)),
            dma((2, 2 * chips)),
            dma((2, 3 * each)),
            dma((2, tp_count, each)),
            dma((tp_count, each)),
            dma((tp_count, each)),
            dma((each * chips,)),
            dma((2, each * chips)),
            dma((2, tp_count)),
            dma((2, seq_count)),
            dma((2, each, 2)),
            dma((2, each, 2)),
            dma((2, each * chips)),
        ],
        compiler_params=pltpu.CompilerParams(
            collective_id=1, has_side_effects=True, vmem_limit_bytes=60 * 2**20
        ),
        cost_estimate=pl.CostEstimate(
            flops=60_000_000_000, bytes_accessed=8 * tokens * depth, transcendentals=0
        ),
    )(
        old_blocks,
        order,
        x_old.reshape(slots, 2, half, quarter),
        gains,
        w_query,
        w_key,
        w_value,
        jnp.asarray(table),
    )


def output_phase(context, w_out_t, residual, gains, new_blocks, seq_count, tp_count, heads):
    tokens = context.shape[0]
    depth = w_out_t.shape[0]
    width = depth * seq_count
    share = 2 * tokens // (seq_count * tp_count)
    scattered = residual.ndim == 3
    places = tokens // share
    per_block = BLOCK // share
    copies = seq_count // heads
    bits = heads.bit_length() - 1
    first, last = layer_windows(seq_count, tp_count, per_block)
    seq_index = lax.axis_index("seq")
    tp_index = lax.axis_index("tp")
    if scattered:
        perm = place = live = new_blocks
    else:
        blocks = new_blocks * per_block
        new_start = jnp.sum(
            jnp.where(
                jnp.arange(seq_count)[None, :] < jnp.arange(seq_count)[:, None], blocks[None, :], 0
            ),
            axis=1,
        )
        slots = jnp.arange(tp_count * seq_count, dtype=jnp.int32)
        layer = jnp.arange(tp_count, dtype=jnp.int32)[:, None]
        valid = (blocks[None, :] > layer).astype(jnp.int32).reshape(-1)
        source = (new_start[None, :] + layer).reshape(-1)
        rank = jnp.sum(jnp.where(slots[None, :] < slots[:, None], valid[None, :], 0), axis=1)
        perm = jnp.sum(
            jnp.where(
                (jnp.arange(places)[:, None] == rank[None, :]) & (valid[None, :] > 0),
                source[None, :],
                0,
            ),
            axis=1,
        ).astype(jnp.int32)
        in_layer = (jnp.arange(tp_count) == tp_index)[:, None]
        place = jnp.sum(jnp.where(in_layer, rank.reshape(tp_count, seq_count), 0), axis=0)
        place = jnp.minimum(place, places - 1).astype(jnp.int32)
        mine = jnp.sum(jnp.where(jnp.arange(seq_count) == seq_index, blocks, 0))
        live = (tp_index < mine).astype(jnp.int32).reshape(1)
    piece = residual.shape[1:] if scattered else (8, HEAD)
    old_block = pltpu.VMEM((seq_count,) + piece, jnp.bfloat16)
    chunks = 4
    rows = tokens // chunks // 2
    half = share // 2
    scratch_block = pltpu.VMEM((places, half, 2 * depth), jnp.bfloat16)
    swap_block = pltpu.VMEM((seq_count, half, 2 * depth), jnp.bfloat16)
    line_sem = pltpu.SemaphoreType.DMA((places,))
    gather_sem = pltpu.SemaphoreType.DMA((chunks, bits, heads))
    swap_sem = pltpu.SemaphoreType.DMA((seq_count,))
    return pl.pallas_call(
        functools.partial(
            output_kernel, heads, copies, seq_count, tp_count, share, first, last, scattered
        ),
        out_shape=jax.ShapeDtypeStruct((share, width), jnp.bfloat16),
        in_specs=[pl.BlockSpec(memory_space=pltpu.SMEM)] * 3
        + [pl.BlockSpec(memory_space=pltpu.VMEM)] * 4,
        out_specs=pl.BlockSpec(memory_space=pltpu.VMEM),
        scratch_shapes=[
            pltpu.VMEM((chunks, rows, heads * HEAD), jnp.bfloat16),
            scratch_block,
            scratch_block,
            scratch_block,
            scratch_block,
            scratch_block,
            scratch_block,
            swap_block,
            swap_block,
            gather_sem,
            gather_sem,
            line_sem,
            line_sem,
            line_sem,
            line_sem,
            swap_sem,
            swap_sem,
            old_block,
            old_block,
            swap_sem,
            swap_sem,
            pltpu.VMEM((2 * depth, heads * HEAD), jnp.bfloat16),
            pltpu.VMEM((chunks, rows, HEAD), jnp.bfloat16),
            pltpu.SemaphoreType.DMA((2,)),
            pltpu.SemaphoreType.DMA((2, chunks)),
        ],
        compiler_params=pltpu.CompilerParams(
            collective_id=0, has_side_effects=True, vmem_limit_bytes=56 * 2**20
        ),
        cost_estimate=pl.CostEstimate(
            flops=60_000_000_000, bytes_accessed=4 * tokens * depth, transcendentals=0
        ),
    )(perm, place, live, context.reshape(places, 2, half, HEAD), w_out_t, residual, gains)


def per_device(
    x_old, old_blocks, new_blocks, order, pre_gain, post_gain, w_query, w_key, w_value, w_out_t
):
    seq_count = lax.axis_size("seq")
    tp_count = lax.axis_size("tp")
    capacity, quarter = x_old.shape
    width = quarter * tp_count
    tokens = seq_count * capacity // 2
    own = tokens // seq_count
    share = capacity // tp_count
    seq_index = lax.axis_index("seq")
    tp_index = lax.axis_index("tp")
    heads = w_query.shape[1] // HEAD
    kv_heads = w_key.shape[1] // HEAD
    scale = (width // (heads * tp_count)) ** (-0.5)
    if front_fits(seq_count, tp_count, heads, kv_heads, capacity):
        context, rows = front_phase(
            x_old,
            old_blocks,
            order,
            pre_gain.reshape(-1, HEAD),
            w_query,
            w_key,
            w_value,
            seq_count,
            tp_count,
            scale,
        )
        return output_phase(
            context, w_out_t, rows, post_gain.reshape(-1, HEAD), new_blocks, seq_count, tp_count, heads
        )
    old_start = offsets(old_blocks)
    new_start = offsets(new_blocks)
    device_ids = jnp.arange(seq_count, dtype=jnp.int32)

    gathered = lax.all_gather(x_old, "seq", axis=0, tiled=True)

    def stored(row, count):
        row = jnp.minimum(row, tokens - count)
        shard = jnp.sum((old_start <= row).astype(jnp.int32)) - 1
        holder = jnp.sum(jnp.where(order == shard, device_ids, 0))
        begin = jnp.sum(jnp.where(device_ids == shard, old_start, 0))
        return lax.dynamic_slice_in_dim(gathered, holder * capacity + row - begin, count, 0)

    def shift(k):
        return [(i, (i + k) % tp_count) for i in range(tp_count)]

    def by_source(received):
        stack = jnp.stack(received)
        pieces = [
            lax.dynamic_index_in_dim(stack, lax.rem(tp_index - u + tp_count, tp_count), 0, False)
            for u in range(tp_count)
        ]
        return jnp.concatenate(pieces, axis=1)

    mine = jnp.concatenate(
        [stored(seq_index * own + at, BLOCK) for at in range(0, own, BLOCK)], axis=0
    )
    full_rows = by_source(
        [mine] + [lax.ppermute(mine, "tp", shift(k)) for k in range(1, tp_count)]
    )
    my_start = jnp.sum(jnp.where(device_ids == seq_index, new_start, 0))

    def slot_rows(place):
        return stored(my_start + place * share, share)

    residual = by_source(
        [slot_rows(tp_index)]
        + [
            lax.ppermute(slot_rows(lax.rem(tp_index + k, tp_count)), "tp", shift(k))
            for k in range(1, tp_count)
        ]
    )

    weights = lax.all_gather(
        jnp.concatenate([w_query, w_key, w_value], axis=1), "seq", axis=0, tiled=True
    )

    normed = rms_scale(full_rows.astype(jnp.float32), pre_gain).astype(jnp.bfloat16)
    normed, residual = lax.optimization_barrier((normed, residual))
    group = heads // kv_heads
    copies = seq_count // heads
    raw = jnp.dot(normed, weights, preferred_element_type=jnp.float32)

    half = HEAD // 2
    inverse = jnp.exp(jnp.arange(half, dtype=jnp.float32) * (-2.0 * math.log(10000.0) / HEAD))
    places = seq_index * own + jnp.arange(own, dtype=jnp.int32)
    angles = places.astype(jnp.float32)[:, None] * inverse[None, :]
    cosine, sine = jnp.cos(angles), jnp.sin(angles)

    def rotate(at):
        first = raw[:, at * HEAD : at * HEAD + half]
        second = raw[:, at * HEAD + half : (at + 1) * HEAD]
        return jnp.concatenate(
            [first * cosine - second * sine, second * cosine + first * sine], axis=-1
        )

    queries = [(rotate(h) * scale).astype(jnp.bfloat16) for h in range(heads)]
    keys = [rotate(heads + g).astype(jnp.bfloat16) for g in range(kv_heads)]
    values = [
        raw[:, (heads + kv_heads + g) * HEAD : (heads + kv_heads + g + 1) * HEAD].astype(
            jnp.bfloat16
        )
        for g in range(kv_heads)
    ]
    sent = jnp.stack(
        [
            jnp.stack([queries[s // copies], keys[s // copies // group], values[s // copies // group]])
            for s in range(seq_count)
        ]
    )
    came = lax.all_to_all(sent, "seq", 0, 0, tiled=True)
    context = attention(
        came[:, 0].reshape(tokens, HEAD),
        came[:, 1].reshape(tokens, HEAD),
        came[:, 2].reshape(tokens, HEAD),
    )
    return output_phase(
        context, w_out_t, residual, post_gain.reshape(1, -1), new_blocks, seq_count, tp_count, heads
    )


def solution(mesh):
    placed = (
        P("seq", "tp"),
        P(),
        P(),
        P(),
        P(),
        P(),
        P("seq", "tp"),
        P("seq", "tp"),
        P("seq", "tp"),
        P("seq", "tp"),
    )
    return jax.shard_map(
        per_device, mesh=mesh, in_specs=placed, out_specs=P(("seq", "tp"), None), check_vma=False
    )
```
